256 devices in a mesh: shots: 2 (over z), mx: 128 (over x, y, core).
Axes of the slice: x: 8, y: 8, z: 2, core: 2. Of those that a mesh axis runs over, the one named last changes fastest.
The devices are a block of a 8x8x16 slice.
Arguments:
- initial: float32 [18, 125, 16384], P('shots', None, 'mx'), parts along dimension 0, may hold values from -6 to 6
- derivative: float32 [3, 125, 125], replicated, may hold values from -0.5 to 0.5
- coupling: float32 [3, 9, 9], replicated, may hold values from -2 to 2
- face_lift: float32 [2, 125, 125], replicated, may hold values from -0.5 to 0.5
- metric: float32 [3, 16384], P(None, 'mx'), may hold values from 0.3 to 3
- rec_element: int32 [32768], P('mx'), may hold values from 0 to 127
- rec_weight: float32 [125, 32768], P(None, 'mx'), may hold values from -0.5 to 0.5
- live_counts: int32 [128], replicated, may hold values from 1 to 256, 16384 in all
- shot_order: int32 [32768], replicated, may hold values from 0 to 32767, as said below
- observed: float32 [65536, 48], P(('shots', 'mx')), parts along dimension 0, may hold values from -6 to 6
Outputs:
- residual: float32 [65536, 48], P(('shots', 'mx')), parts along dimension 0
- misfit: float32 [65536], P(('shots', 'mx')), parts along dimension 0
- adjoint: float32 [65536, 48], P(('shots', 'mx')), parts along dimension 0
The draws below stay inside these ranges and needn't reach their ends.
There are 2 independent parts, one for each index of `shots`. The reference program is written for one: setup_inputs(seed, part) draws one part's arguments, and reference() takes and returns one part's arrays. A program takes and returns all parts, laid end to end along the dimension named above; an argument that names none is the same for every part. Nothing has to cross between parts.
Inputs may be any that keep to these rules, and one draw needn't show every extreme that they name: `rec_element`: local element index of the slot within its block of 128 elements. The live receivers of block b are its first live_counts[b] slots. `shot_order`: a permutation of the slots; of the 256 positions of each block of shot-receiver order, exactly 2 come from the slots of each block.
All inputs are finite; a program needn't handle non-finite values.
Results may differ from the reference program's by a relative error of at most 0.00018.
Values sent between devices are 32-bit elements; how exact they have to be, the bound alone decides.
No kernel may reach another device: no remote copies, remote signals or barrier semaphores. Data moves between devices by JAX's collectives and lax.ppermute only.
A program may use at most 64 MiB of HBM per device.

```python
import math
import jax
import jax.numpy as jnp
import numpy as np
from jax import lax

FIELDS = 9
NODE = 125
STEPS = 12
E_DEV = 128
R_DEV = 256
TW = 48
BLOCKS = 128
PAIR = 2
ELEMS = 16384
R_TOTAL = 32768


def draw_shot_order(key, part):
    key_a, key_b = jax.random.split(key)
    slot_perm = jax.vmap(lambda sub: jax.random.permutation(sub, R_DEV))(jax.random.split(key_a, BLOCKS))
    grouped = slot_perm.reshape(BLOCKS, BLOCKS, PAIR)
    source_ids = jnp.arange(BLOCKS, dtype=jnp.int32)[:, None, None] * R_DEV + grouped.astype(jnp.int32)
    per_dest = source_ids.transpose(1, 0, 2).reshape(BLOCKS, R_DEV)
    dest_order = jax.vmap(lambda sub: jax.random.permutation(sub, R_DEV))(jax.random.split(key_b, BLOCKS))
    placed = jnp.take_along_axis(per_dest, dest_order.astype(jnp.int32), axis=1)
    return placed.reshape(-1).astype(jnp.int32)


def with_ends(drawn, rng, least, largest):
    longest = drawn.shape.index(max(drawn.shape))
    spots = []
    for shift in (0, 1):
        where = [jax.random.randint(jax.random.fold_in(rng, axis), (), 0, length) for axis, length in enumerate(drawn.shape)]
        where[longest] = (where[longest] + shift) % drawn.shape[longest]
        spots.append(tuple(where))
    return drawn.at[spots[0]].set(least).at[spots[1]].set(largest)


def level_of(key, extent, pieces, low, high):
    loudness = 1.0
    for position, shards_of in pieces:
        heights = jax.random.uniform(jax.random.fold_in(jax.random.fold_in(key, 6), position), (shards_of,), jnp.float32, low / len(pieces), high / len(pieces))
        loudness = loudness * jnp.repeat(jnp.exp(heights), extent[position] // shards_of).reshape((-1,) + (1,) * (len(extent) - 1 - position))
    return loudness


def split_up(count, total, most, slope):
    loads = [(1 << 20) // math.isqrt(standing ** slope) + 1 for standing in range(2, count + 1)]
    spare, counts = total - most - (count - 1), [1] * (count - 1)
    while spare > 0:
        free = [i for i in range(count - 1) if counts[i] < most]
        pool, left = sum([loads[i] for i in free]), spare
        for i in free:
            extra = min(most - counts[i], max(1, left * loads[i] // pool), spare)
            counts[i] = counts[i] + extra
            spare = spare - extra
    return np.array([most] + counts)


def ragged_sizes(stream_key, number_of, total, limit, lean):
    if number_of == 2:
        one = jax.random.randint(stream_key, (), max(1, total - limit), min(limit, total - 1) + 1)
        return jnp.stack([one, total - one])
    tallies = jnp.asarray(split_up(number_of, total, limit, lean), jnp.int32)
    pairs = (number_of - 1) // 2
    donor, receiver = tallies[1:1 + 2 * pairs:2], tallies[2:2 + 2 * pairs:2]
    margin = jnp.minimum(donor - 1, limit - receiver)
    passed = jax.random.randint(jax.random.fold_in(stream_key, 1), (pairs,), 0, 1 << 20) % (margin + 1)
    tallies = tallies.at[1:1 + 2 * pairs:2].set(donor - passed).at[2:2 + 2 * pairs:2].set(receiver + passed)
    return tallies[jax.random.permutation(jax.random.fold_in(stream_key, 2), number_of)]


def normal_values(own_key, extent, spread, most, pieces=(), kind=jnp.bfloat16):
    result = spread * jax.random.normal(own_key, extent, jnp.float32)
    if pieces:
        result = result * level_of(own_key, extent, pieces, -0.22, 0.18)
    return jnp.clip(result, -most, most).astype(kind)


def setup_inputs(seed: int = 0, part: int = 0) -> dict:
    key_list = jax.random.split(jax.random.key(seed), 11)
    part_splits = jax.random.split(jax.random.fold_in(key_list[10], part), 11)
    initial = normal_values(part_splits[0], (FIELDS, NODE, ELEMS), 1.0, 6.0, ((2, 128),), jnp.float32)
    derivative = normal_values(key_list[1], (3, NODE, NODE), NODE ** -0.5, 0.5, (), jnp.float32)
    coupling = normal_values(key_list[2], (3, FIELDS, FIELDS), FIELDS ** -0.5, 2.0, (), jnp.float32)
    face_lift = normal_values(key_list[3], (2, NODE, NODE), NODE ** -0.5, 0.5, (), jnp.float32)
    metric = jnp.clip(jnp.exp(math.log(3.0) - 2.3025851 * jax.random.uniform(key_list[4], (3, ELEMS), jnp.float32) ** level_of(key_list[4], (3, ELEMS), ((1, 128),), -0.2, 0.2)), 0.3, 3.0)
    rec_element = with_ends(jax.random.randint(key_list[5], (R_TOTAL,), 0, E_DEV), jax.random.fold_in(key_list[5], 1), 0, E_DEV - 1).astype(jnp.int32)
    rec_weight = normal_values(key_list[6], (NODE, R_TOTAL), NODE ** -0.5, 0.5, ((1, 128),), jnp.float32)
    live_counts = ragged_sizes(key_list[7], BLOCKS, BLOCKS * R_DEV // 2, R_DEV, 2).astype(jnp.int32)
    shot_order = draw_shot_order(jax.random.fold_in(key_list[10], 71), part)
    observed = normal_values(part_splits[9], (R_TOTAL, TW), 1.0, 6.0, ((0, 128),), jnp.float32)
    return dict(initial=initial, derivative=derivative, coupling=coupling, face_lift=face_lift, metric=metric, rec_element=rec_element, rec_weight=rec_weight, live_counts=live_counts, shot_order=shot_order, observed=observed)


HIGH = lax.Precision.HIGHEST


def advance(extended, metric_cols, derivative, coupling, face_lift, time_step):
    middle = extended[:, :, 1:-1]
    summed = jnp.einsum('pq,fqe->fpe', face_lift[0], extended[:, :, :-2] - middle, precision=HIGH)
    summed = summed + jnp.einsum('pq,fqe->fpe', face_lift[1], extended[:, :, 2:] - middle, precision=HIGH)
    for k in range(3):
        gradient = jnp.einsum('pq,fqe->fpe', derivative[k], middle, precision=HIGH)
        summed = summed + jnp.einsum('gf,fpe->gpe', coupling[k], gradient, precision=HIGH) * metric_cols[k][None, None, :]
    return middle + time_step * summed


def sample(wavefield, elements, rec_weight, live_slot):
    components = jnp.stack([wavefield[0], wavefield[1], wavefield[2], (wavefield[3] + wavefield[4] + wavefield[5]) / 3.0])
    columns = jnp.take(components, elements, axis=2)
    return jnp.sum(columns * rec_weight[None], axis=1) * live_slot[None]


def reference(initial, derivative, coupling, face_lift, metric, rec_element, rec_weight, live_counts, shot_order, observed):
    time_step = 0.5 / STEPS
    slot_ids = jnp.arange(R_TOTAL, dtype=jnp.int32)
    block_of = slot_ids // R_DEV
    global_elem = (block_of * E_DEV + rec_element).astype(jnp.int32)
    live_slot = ((slot_ids % R_DEV) < live_counts[block_of]).astype(jnp.float32)

    def one_step(t, carry):
        wavefield, trace_buffer = carry
        extended = jnp.pad(wavefield, ((0, 0), (0, 0), (1, 1)))
        wavefield = advance(extended, metric, derivative, coupling, face_lift, time_step)
        sampled = sample(wavefield, global_elem, rec_weight, live_slot)
        trace_buffer = lax.dynamic_update_slice(trace_buffer, sampled[:, None, :], (0, t, 0))
        return wavefield, trace_buffer

    trace_buffer = jnp.zeros((4, STEPS, R_TOTAL), jnp.float32)
    final_field, trace_buffer = lax.fori_loop(0, STEPS, one_step, (initial, trace_buffer))
    synthetic = trace_buffer.transpose(2, 0, 1).reshape(R_TOTAL, 4 * STEPS)
    ordered = synthetic[shot_order]
    live_out = live_slot[shot_order]
    residual = live_out[:, None] * (ordered - observed)
    misfit = 0.5 * jnp.sum(residual * residual, axis=1)
    flipped = residual.reshape(R_TOTAL, 4, STEPS)[:, :, ::-1].reshape(R_TOTAL, 4 * STEPS)
    adjoint = jnp.zeros_like(flipped).at[shot_order].set(flipped)
    return residual, misfit, adjoint
```

```python
import jax
import jax.numpy as jnp
from jax import lax
from jax.experimental import pallas as pl
from jax.experimental.pallas import tpu as pltpu
from jax.sharding import Mesh
from jax.sharding import PartitionSpec as P

STEPS = 12
COMPS = 4
MX = ("mx_0", "mx_1", "mx_2")
SHOTS_MX = ("shots", "mx_0", "mx_1", "mx_2")
F32 = jnp.float32
BF16 = jnp.bfloat16
I32 = jnp.int32
LANES = 128
GROUP = 8
PAIR_ROWS = 2 * GROUP
HALO = 16
OBS_LANE = 64
VMEM = pltpu.VMEM


def iota(shape, dim):
    return lax.broadcasted_iota(I32, shape, dim)


def split2(x):
    hi = x.astype(BF16)
    return hi, (x - hi.astype(F32)).astype(BF16)


def split3(x):
    hi = x.astype(BF16)
    rest = x - hi.astype(F32)
    mid = rest.astype(BF16)
    return hi, mid, (rest - mid.astype(F32)).astype(BF16)


def dot(a, b):
    return jnp.dot(a, b, preferred_element_type=F32)


def pick(onehot, x):
    parts = split3(x)
    return dot(onehot, parts[0]) + (dot(onehot, parts[1]) + dot(onehot, parts[2]))


def padded(x, rows, cols):
    if x.shape[1] < cols:
        x = jnp.concatenate([x, jnp.zeros((x.shape[0], cols - x.shape[1]), x.dtype)], axis=1)
    if x.shape[0] < rows:
        x = jnp.concatenate([x, jnp.zeros((rows - x.shape[0], cols), x.dtype)], axis=0)
    return x


def turn_kernel(initial_ref, metric_ref, own_ref, low_ref, high_ref):
    fields, _, elems = initial_ref.shape
    for f in range(fields):
        own_ref[f] = padded(initial_ref[f], LANES, elems).T
    for k in range(metric_ref.shape[0]):
        own_ref[fields + k] = jnp.broadcast_to(metric_ref[k : k + 1, :], (LANES, elems)).T
    low_ref[...] = own_ref[:, :HALO, :]
    high_ref[...] = own_ref[:, elems - HALO :, :]


def turn(initial, metric):
    fields, _, elems = initial.shape
    planes = fields + metric.shape[0]
    return pl.pallas_call(
        turn_kernel,
        out_shape=(
            jax.ShapeDtypeStruct((planes, elems, LANES), F32),
            jax.ShapeDtypeStruct((planes, HALO, LANES), F32),
            jax.ShapeDtypeStruct((planes, HALO, LANES), F32),
        ),
        compiler_params=pltpu.CompilerParams(vmem_limit_bytes=8 << 20),
        name="turn",
    )(initial, metric)


def plan_kernel(
    me_ref,
    live_ref,
    lives_ref,
    derivative_ref,
    coupling_ref,
    lift_ref,
    element_ref,
    weight_ref,
    order_ref,
    observed_ref,
    wt_ref,
    wl_ref,
    ck_ref,
    eh_ref,
    wp_ref,
    acc_ref,
    back_slot_ref,
    back_pos_ref,
    seen_ref,
):
    slots, width = observed_ref.shape
    blocks = slots // 2
    me = me_ref[0]
    axes = derivative_ref.shape[0]
    fields = coupling_ref.shape[1]
    dh, dl = [], []
    for k in range(axes):
        hi, lo = split2(padded(derivative_ref[k], LANES, LANES).T)
        dh.append(hi)
        dl.append(lo)
    zero = jnp.zeros((LANES, LANES), BF16)
    for row, (left, right) in enumerate(
        [(dh[0], dl[0]), (dh[1], dl[1]), (dh[2], dl[2]), (dh[2], zero), (dh[0], zero), (dh[1], zero)]
    ):
        wt_ref[row * LANES : (row + 1) * LANES, :] = jnp.concatenate([left, right], axis=1)
    l0h, l0l = split2(padded(lift_ref[0], LANES, LANES).T)
    l1h, l1l = split2(padded(lift_ref[1], LANES, LANES).T)
    for row, (left, right) in enumerate([(l0h, l1h), (l0h, l1h), (l0l, l1l)]):
        wl_ref[row * LANES : (row + 1) * LANES, :] = jnp.concatenate([left, right], axis=1)
    rows, cols = axes * fields * GROUP, fields * GROUP
    spread_rows = (iota((rows, axes * fields), 0) // GROUP == iota((rows, axes * fields), 1)).astype(BF16)
    spread_cols = (iota((fields, cols), 0) == iota((fields, cols), 1) // GROUP).astype(BF16)
    stacked = jnp.concatenate([coupling_ref[k] for k in range(axes)], axis=0)
    by_row = pick(spread_rows, stacked)
    by_hi, by_mid, by_lo = split3(by_row)
    full = dot(by_hi, spread_cols) + (dot(by_mid, spread_cols) + dot(by_lo, spread_cols))
    diagonal = iota((rows, cols), 0) % GROUP == iota((rows, cols), 1) % GROUP
    full = jnp.where(diagonal, full, 0.0)
    full_hi = full.astype(BF16).astype(F32)
    ck_ref[...] = jnp.concatenate([full_hi, full_hi, full - full_hi], axis=1).astype(BF16)
    order = order_ref[...]
    half = iota((slots, LANES), 0) % 2
    position = half * LANES + iota((slots, LANES), 1)
    slot_of = order % slots
    key = (position * slots + slot_of).astype(F32)
    mine = (order // slots) == me
    big = float(slots * slots)
    first = jnp.min(jnp.where(mine, key, big), axis=1, keepdims=True)
    last = jnp.max(jnp.where(mine, key, -1.0), axis=1, keepdims=True)
    first = jnp.broadcast_to(first, (slots, LANES))
    last = jnp.broadcast_to(last, (slots, LANES))
    up = lambda x: pltpu.roll(x, slots - 1, 0)
    down = lambda x: pltpu.roll(x, 1, 0)
    chosen = jnp.where(half == 0, jnp.minimum(first, up(first)), jnp.maximum(last, down(last)))
    chosen = chosen.astype(I32) % slots
    chosen = jnp.concatenate([chosen, chosen], axis=1)
    send_slot = chosen == iota((slots, slots), 1)
    send_slot_f = send_slot.astype(F32)
    send_slot_b = send_slot_f.astype(BF16)
    my_rows = order_ref[pl.ds(2 * me, 2), :]
    my_row = jnp.concatenate([my_rows[0:1], my_rows[1:2]], axis=1)
    my_block = my_row // slots
    my_slot = (my_row % slots).astype(F32)
    row_id = iota((slots, slots), 0)
    col_id = iota((slots, slots), 1).astype(F32)
    from_block = my_block == row_id // 2
    jmin = jnp.min(jnp.where(from_block, col_id, big), axis=1, keepdims=True)
    jmax = jnp.max(jnp.where(from_block, col_id, -1.0), axis=1, keepdims=True)
    picked = jnp.where(row_id % 2 == 0, jmin, jmax)
    at_pos = (picked == col_id).astype(F32)
    lives = jnp.broadcast_to(lives_ref[...].astype(F32), (slots, blocks))
    live_of = jnp.sum(
        jnp.where(iota((slots, blocks), 0) // 2 == iota((slots, blocks), 1), lives, 0.0), axis=1, keepdims=True
    )
    slot_there = jnp.sum(at_pos * my_slot, axis=1, keepdims=True)
    alive = (slot_there < live_of).astype(F32)
    at_pos_live = (at_pos * alive).T
    back_pos_ref[...] = at_pos_live.astype(BF16)
    live_pos = jnp.sum(at_pos_live, axis=1, keepdims=True)
    observed = observed_ref[...]
    seen_ref[...] = observed * live_pos
    back_slot_ref[...] = send_slot_f.T.astype(BF16)
    my_live = live_ref[me]
    element = element_ref[...].astype(F32)
    element_sent = jnp.sum(send_slot_f * element, axis=1, keepdims=True)
    hit = (element_sent.astype(I32) == iota((slots, LANES), 1)).astype(BF16)
    eh_ref[...] = jnp.concatenate([hit, hit], axis=1)
    weight = jnp.where(iota(weight_ref.shape, 1) < my_live, weight_ref[...], 0.0)
    weight = padded(weight, LANES, slots).T
    wp_ref[...] = pick(send_slot_b, weight)
    lane, time = iota((width, LANES), 1) - OBS_LANE, iota((width, LANES), 0)
    comp = time // STEPS
    flipped = comp * STEPS + (STEPS - 1 - (time - comp * STEPS))
    turn_time = (lane == flipped).astype(BF16)
    hi, mid, lo = split3(observed)
    reversed_rows = dot(hi, turn_time) + (dot(mid, turn_time) + dot(lo, turn_time))
    acc_ref[...] = pick(at_pos.astype(BF16), reversed_rows)


def plan(me, live_counts, derivative, coupling, face_lift, rec_element, rec_weight, order, observed):
    slots, width = observed.shape
    axes, fields = coupling.shape[0], coupling.shape[1]
    block = axes * fields * GROUP
    smem = pl.BlockSpec(memory_space=pltpu.SMEM)
    vmem = pl.BlockSpec(memory_space=VMEM)
    return pl.pallas_call(
        plan_kernel,
        in_specs=[smem, smem] + [vmem] * 8,
        out_shape=(
            jax.ShapeDtypeStruct((6 * LANES, 2 * LANES), BF16),
            jax.ShapeDtypeStruct((3 * LANES, 2 * LANES), BF16),
            jax.ShapeDtypeStruct((block, 3 * fields * GROUP), BF16),
            jax.ShapeDtypeStruct((slots, 2 * LANES), BF16),
            jax.ShapeDtypeStruct((slots, LANES), F32),
            jax.ShapeDtypeStruct((slots, LANES), F32),
            jax.ShapeDtypeStruct((slots, slots), BF16),
            jax.ShapeDtypeStruct((slots, slots), BF16),
            jax.ShapeDtypeStruct((slots, width), F32),
        ),
        compiler_params=pltpu.CompilerParams(vmem_limit_bytes=16 << 20),
        cost_estimate=pl.CostEstimate(flops=4_000_000_000, bytes_accessed=2_000_000, transcendentals=0),
        name="plan",
    )(
        me,
        live_counts,
        live_counts.reshape(1, -1),
        derivative,
        coupling,
        face_lift,
        rec_element.reshape(1, -1),
        rec_weight,
        order,
        observed,
    )


def march_kernel(
    me_ref,
    own_ref,
    low_ref,
    high_ref,
    wt_ref,
    wl_ref,
    ck_ref,
    eh_ref,
    wp_ref,
    acc0_ref,
    send_ref,
    rev_ref,
    u_ref,
    m_ref,
    h_ref,
    t_ref,
    lt_ref,
    lu_ref,
    *,
    last_block,
):
    planes, elems, _ = own_ref.shape
    axes = 3
    fields = planes - axes
    rows = elems + 2 * HALO
    pairs = rows // PAIR_ROWS
    slots = eh_ref.shape[0]
    dt = 0.5 / STEPS
    me = me_ref[0]
    dt_low = jnp.where(me == 0, 0.0, dt).astype(F32)
    dt_high = jnp.where(me == last_block, 0.0, dt).astype(F32)
    u_ref[:, :HALO, :] = low_ref[:fields]
    u_ref[:, HALO : HALO + elems, :] = own_ref[:fields]
    u_ref[:, HALO + elems :, :] = high_ref[:fields]
    m_ref[:, :HALO, :] = low_ref[fields:]
    m_ref[:, HALO : HALO + elems, :] = own_ref[fields:]
    m_ref[:, HALO + elems :, :] = high_ref[fields:]
    send_ref[...] = acc0_ref[...]
    rev_ref[...] = jnp.zeros(rev_ref.shape, F32)
    tile = fields * PAIR_ROWS

    def load_pair(j):
        r = j * PAIR_ROWS
        halves = ([], [])
        for f in range(fields):
            x = u_ref[f, r : r + PAIR_ROWS, :]
            hi, lo = split2(x)
            lu_ref[j, f * PAIR_ROWS : (f + 1) * PAIR_ROWS, :LANES] = hi
            lu_ref[j, f * PAIR_ROWS : (f + 1) * PAIR_ROWS, LANES:] = lo
            hi32 = hi.astype(F32)
            lo32 = x - hi32
            for side in range(2):
                halves[side].append((hi32[side * GROUP : (side + 1) * GROUP], lo32[side * GROUP : (side + 1) * GROUP]))
        columns = []
        for side in range(2):
            his = [p[0] for p in halves[side]]
            los = [p[1] for p in halves[side]]
            columns.append(jnp.concatenate(his + los + his, axis=0).astype(BF16))
        return jnp.concatenate(columns, axis=1)

    def couple(j):
        v = dot(ck_ref[...], load_pair(j))
        r = j * PAIR_ROWS
        for k in range(axes):
            ma = m_ref[k, r : r + GROUP, :]
            mb = m_ref[k, r + GROUP : r + PAIR_ROWS, :]
            parts = []
            for g in range(fields):
                base = (k * fields + g) * GROUP
                parts.append(v[base : base + GROUP, :LANES] * ma)
                parts.append(v[base : base + GROUP, LANES:] * mb)
            hi, lo = split2(jnp.concatenate(parts, axis=0))
            lanes = ((0, 4), (1, 5), (2, 3))[k]
            lt_ref[j, :, lanes[0] * LANES : (lanes[0] + 1) * LANES] = hi
            lt_ref[j, :, lanes[1] * LANES : (lanes[1] + 1) * LANES] = lo

    def apply(j):
        r = j * PAIR_ROWS
        both = dot(lt_ref[j], wt_ref[...])
        both = both[:, :LANES] + both[:, LANES:]
        lifted = dot(lu_ref[j], wl_ref[: 2 * LANES, :]) + dot(lu_ref[j, :, :LANES], wl_ref[2 * LANES :, :])
        for g in range(fields):
            t_ref[g, r : r + PAIR_ROWS, :] = both[g * PAIR_ROWS : (g + 1) * PAIR_ROWS]
            for side in range(2):
                h_ref[side, g, GROUP + r : GROUP + r + PAIR_ROWS, :] = lifted[
                    g * PAIR_ROWS : (g + 1) * PAIR_ROWS, side * LANES : (side + 1) * LANES
                ]

    def update(j):
        r = j * PAIR_ROWS
        a = GROUP + r
        factor = dt_low if r < HALO else (dt_high if r >= HALO + elems else dt)
        for g in range(fields):
            lift = (h_ref[0, g, a - 1 : a - 1 + PAIR_ROWS, :] - h_ref[0, g, a : a + PAIR_ROWS, :]) + (
                h_ref[1, g, a + 1 : a + 1 + PAIR_ROWS, :] - h_ref[1, g, a : a + PAIR_ROWS, :]
            )
            u_ref[g, r : r + PAIR_ROWS, :] = u_ref[g, r : r + PAIR_ROWS, :] + factor * (
                t_ref[g, r : r + PAIR_ROWS, :] + lift
            )

    def sample(t, have_parts):
        lo_pair, hi_pair = HALO // PAIR_ROWS, (HALO + elems) // PAIR_ROWS
        columns = []
        own = slice(HALO, HALO + elems)
        for c in range(COMPS):
            if c < 3 and have_parts:
                part = lambda lanes: jnp.concatenate(
                    [lu_ref[j, c * PAIR_ROWS : (c + 1) * PAIR_ROWS, lanes] for j in range(lo_pair, hi_pair)], axis=0
                )
                hi, lo = part(slice(0, LANES)), part(slice(LANES, 2 * LANES))
            else:
                if c < 3:
                    x = u_ref[c, own, :]
                else:
                    x = (u_ref[3, own, :] + u_ref[4, own, :] + u_ref[5, own, :]) / 3.0
                hi, lo = split2(x)
            columns.append(jnp.concatenate([hi, lo], axis=0))
        lane = iota((slots, LANES), 1)
        send = send_ref[...]
        rev = rev_ref[...]
        for c in range(0, COMPS, 2):
            found = dot(eh_ref[...], jnp.concatenate(columns[c : c + 2], axis=1))
            for i in range(2):
                value = jnp.sum(found[:, i * LANES : (i + 1) * LANES] * wp_ref[...], axis=1, keepdims=True)
                send = jnp.where(lane == (c + i) * STEPS + t, value, send)
                rev = jnp.where(lane == OBS_LANE + (c + i) * STEPS + (STEPS - 1) - t, value, rev)
        send_ref[...] = send
        rev_ref[...] = rev

    def step(t, first, stop):
        for j in range(first, stop):
            couple(j)
        for j in range(first, stop):
            apply(j)
        for j in range(first, stop):
            update(j)

    def body(first, stop):
        def run(t, carry):
            step(t, first, stop)
            sample(t, False)
            return carry

        return run

    lax.fori_loop(0, 3, body(0, pairs), 0)
    lax.fori_loop(3, STEPS, body(0, pairs), 0)


def march(me, own, low, high, operators, last_block):
    wt, wl, ck, eh, wp, acc0 = operators
    planes, elems, _ = own.shape
    fields = planes - 3
    rows = elems + 2 * HALO
    pairs = rows // PAIR_ROWS
    slots = eh.shape[0]
    smem = pl.BlockSpec(memory_space=pltpu.SMEM)
    vmem = pl.BlockSpec(memory_space=VMEM)
    import functools

    return pl.pallas_call(
        functools.partial(march_kernel, last_block=last_block),
        in_specs=[smem] + [vmem] * 9,
        out_shape=(
            jax.ShapeDtypeStruct((slots, LANES), F32),
            jax.ShapeDtypeStruct((slots, LANES), F32),
        ),
        scratch_shapes=[
            VMEM((fields, rows, LANES), F32),
            VMEM((3, rows, LANES), F32),
            VMEM((2, fields, rows + 2 * GROUP, LANES), F32),
            VMEM((fields, rows, LANES), F32),
            VMEM((pairs, fields * PAIR_ROWS, 6 * LANES), BF16),
            VMEM((pairs, fields * PAIR_ROWS, 2 * LANES), BF16),
        ],
        compiler_params=pltpu.CompilerParams(vmem_limit_bytes=40 << 20),
        cost_estimate=pl.CostEstimate(flops=20_000_000_000, bytes_accessed=4_000_000, transcendentals=0),
        name="march",
    )(me, own, low, high, wt, wl, ck, eh, wp, acc0)


def finish_kernel(me_ref, live_ref, got_ref, rev_ref, back_slot_ref, back_pos_ref, seen_ref, res_ref, mis_ref, adj_ref):
    slots, width = res_ref.shape
    got = got_ref[...]
    ordered = pick(back_pos_ref[...], got)
    residual = ordered[:, :width] - seen_ref[...]
    res_ref[...] = residual
    squares = padded(residual * residual, slots, LANES)
    mis_ref[...] = 0.5 * jnp.sum(squares.T, axis=0, keepdims=True)
    adjoint = pick(back_slot_ref[...], pltpu.roll(rev_ref[...] - got, LANES - OBS_LANE, 1))
    live = iota((slots, LANES), 0) < live_ref[me_ref[0]]
    adj_ref[...] = jnp.where(live, adjoint, 0.0)[:, :width]


def finish(me, live_counts, got, rev, back_slot, back_pos, seen):
    slots, width = seen.shape
    smem = pl.BlockSpec(memory_space=pltpu.SMEM)
    vmem = pl.BlockSpec(memory_space=VMEM)
    return pl.pallas_call(
        finish_kernel,
        in_specs=[smem, smem] + [vmem] * 5,
        out_shape=(
            jax.ShapeDtypeStruct((slots, width), F32),
            jax.ShapeDtypeStruct((1, slots), F32),
            jax.ShapeDtypeStruct((slots, width), F32),
        ),
        compiler_params=pltpu.CompilerParams(vmem_limit_bytes=8 << 20),
        name="finish",
    )(me, live_counts, got, rev, back_slot, back_pos, seen)


def shards(
    initial,
    derivative,
    coupling,
    face_lift,
    metric,
    rec_element,
    rec_weight,
    live_counts,
    shot_order,
    observed,
):
    blocks = lax.axis_size(MX)
    slots = rec_element.shape[0]
    me = lax.axis_index(MX).astype(I32).reshape(1)
    own, low, high = turn(initial, metric)
    forward = [(i, i + 1) for i in range(blocks - 1)]
    backward = [(target, source) for source, target in forward]
    from_low = lax.ppermute(high, MX, forward)
    from_high = lax.ppermute(low, MX, backward)
    order = shot_order.reshape(-1, LANES)
    wt, wl, ck, eh, wp, acc0, back_slot, back_pos, seen = plan(
        me, live_counts, derivative, coupling, face_lift, rec_element, rec_weight, order, observed
    )
    send, rev = march(me, own, from_low, from_high, (wt, wl, ck, eh, wp, acc0), blocks - 1)
    got = lax.all_to_all(send.reshape(blocks, 2, LANES), MX, split_axis=0, concat_axis=0, tiled=True)
    residual, misfit, adjoint = finish(me, live_counts, got.reshape(slots, LANES), rev, back_slot, back_pos, seen)
    return (residual, misfit.reshape(slots), adjoint)


def solution(mesh):
    split = Mesh(
        mesh.devices.reshape(mesh.shape["shots"], 8, 8, 2), ("shots", "mx_0", "mx_1", "mx_2")
    )
    in_specs = (
        P("shots", None, MX),
        P(),
        P(),
        P(),
        P(None, MX),
        P(MX),
        P(None, MX),
        P(),
        P(),
        P(SHOTS_MX, None),
    )
    out_specs = (P(SHOTS_MX, None), P(SHOTS_MX), P(SHOTS_MX, None))
    return jax.shard_map(
        shards, mesh=split, in_specs=in_specs, out_specs=out_specs, check_vma=False
    )
```

```python
import jax
import jax.numpy as jnp
from jax import lax
from jax.experimental import pallas as pl
from jax.experimental.pallas import tpu as pltpu
from jax.sharding import Mesh
from jax.sharding import PartitionSpec as P

STEPS = 12
COMPS = 4
MX = ("mx_0", "mx_1", "mx_2")
SHOTS_MX = ("shots", "mx_0", "mx_1", "mx_2")
F32 = jnp.float32
BF16 = jnp.bfloat16
I32 = jnp.int32
LANES = 128
GROUP = 8
PAIR_ROWS = 2 * GROUP
HALO = 16
OBS_LANE = 64
VMEM = pltpu.VMEM


def iota(shape, dim):
    return lax.broadcasted_iota(I32, shape, dim)


def split2(x):
    hi = x.astype(BF16)
    return hi, (x - hi.astype(F32)).astype(BF16)


def split3(x):
    hi = x.astype(BF16)
    rest = x - hi.astype(F32)
    mid = rest.astype(BF16)
    return hi, mid, (rest - mid.astype(F32)).astype(BF16)


def dot(a, b):
    return jnp.dot(a, b, preferred_element_type=F32)


def pick(onehot, x):
    parts = split3(x)
    return dot(onehot, parts[0]) + (dot(onehot, parts[1]) + dot(onehot, parts[2]))


def padded(x, rows, cols):
    if x.shape[1] < cols:
        x = jnp.concatenate([x, jnp.zeros((x.shape[0], cols - x.shape[1]), x.dtype)], axis=1)
    if x.shape[0] < rows:
        x = jnp.concatenate([x, jnp.zeros((rows - x.shape[0], cols), x.dtype)], axis=0)
    return x


def turn_kernel(initial_ref, metric_ref, own_ref, low_ref, high_ref):
    fields, _, elems = initial_ref.shape
    for f in range(fields):
        own_ref[f] = padded(initial_ref[f], LANES, elems).T
    for k in range(metric_ref.shape[0]):
        own_ref[fields + k] = jnp.broadcast_to(metric_ref[k : k + 1, :], (LANES, elems)).T
    low_ref[...] = own_ref[:, :HALO, :]
    high_ref[...] = own_ref[:, elems - HALO :, :]


def turn(initial, metric):
    fields, _, elems = initial.shape
    planes = fields + metric.shape[0]
    return pl.pallas_call(
        turn_kernel,
        out_shape=(
            jax.ShapeDtypeStruct((planes, elems, LANES), F32),
            jax.ShapeDtypeStruct((planes, HALO, LANES), F32),
            jax.ShapeDtypeStruct((planes, HALO, LANES), F32),
        ),
        compiler_params=pltpu.CompilerParams(vmem_limit_bytes=8 << 20),
        name="turn",
    )(initial, metric)


def plan_kernel(
    me_ref,
    live_ref,
    lives_ref,
    derivative_ref,
    coupling_ref,
    lift_ref,
    element_ref,
    weight_ref,
    order_ref,
    observed_ref,
    wt_ref,
    wl_ref,
    ck_ref,
    eh_ref,
    wp_ref,
    acc_ref,
    back_slot_ref,
    back_pos_ref,
    seen_ref,
):
    slots, width = observed_ref.shape
    blocks = slots // 2
    me = me_ref[0]
    axes = derivative_ref.shape[0]
    fields = coupling_ref.shape[1]
    dh, dl = [], []
    for k in range(axes):
        hi, lo = split2(padded(derivative_ref[k], LANES, LANES).T)
        dh.append(hi)
        dl.append(lo)
    zero = jnp.zeros((LANES, LANES), BF16)
    for row, (left, right) in enumerate(
        [(dh[0], dl[0]), (dh[1], dl[1]), (dh[2], dl[2]), (dh[2], zero), (dh[0], zero), (dh[1], zero)]
    ):
        wt_ref[row * LANES : (row + 1) * LANES, :] = jnp.concatenate([left, right], axis=1)
    l0h, l0l = split2(padded(lift_ref[0], LANES, LANES).T)
    l1h, l1l = split2(padded(lift_ref[1], LANES, LANES).T)
    for row, (left, right) in enumerate([(l0h, l1h), (l0h, l1h), (l0l, l1l)]):
        wl_ref[row * LANES : (row + 1) * LANES, :] = jnp.concatenate([left, right], axis=1)
    rows, cols = axes * fields * GROUP, fields * GROUP
    spread_rows = (iota((rows, axes * fields), 0) // GROUP == iota((rows, axes * fields), 1)).astype(BF16)
    spread_cols = (iota((fields, cols), 0) == iota((fields, cols), 1) // GROUP).astype(BF16)
    stacked = jnp.concatenate([coupling_ref[k] for k in range(axes)], axis=0)
    by_row = pick(spread_rows, stacked)
    by_hi, by_mid, by_lo = split3(by_row)
    full = dot(by_hi, spread_cols) + (dot(by_mid, spread_cols) + dot(by_lo, spread_cols))
    diagonal = iota((rows, cols), 0) % GROUP == iota((rows, cols), 1) % GROUP
    full = jnp.where(diagonal, full, 0.0)
    full_hi = full.astype(BF16).astype(F32)
    ck_ref[...] = jnp.concatenate([full_hi, full_hi, full - full_hi], axis=1).astype(BF16)
    order = order_ref[...]
    half = iota((slots, LANES), 0) % 2
    position = half * LANES + iota((slots, LANES), 1)
    slot_of = order % slots
    key = (position * slots + slot_of).astype(F32)
    mine = (order // slots) == me
    big = float(slots * slots)
    first = jnp.min(jnp.where(mine, key, big), axis=1, keepdims=True)
    last = jnp.max(jnp.where(mine, key, -1.0), axis=1, keepdims=True)
    first = jnp.broadcast_to(first, (slots, LANES))
    last = jnp.broadcast_to(last, (slots, LANES))
    up = lambda x: pltpu.roll(x, slots - 1, 0)
    down = lambda x: pltpu.roll(x, 1, 0)
    chosen = jnp.where(half == 0, jnp.minimum(first, up(first)), jnp.maximum(last, down(last)))
    chosen = chosen.astype(I32) % slots
    chosen = jnp.concatenate([chosen, chosen], axis=1)
    send_slot = chosen == iota((slots, slots), 1)
    send_slot_f = send_slot.astype(F32)
    send_slot_b = send_slot_f.astype(BF16)
    my_rows = order_ref[pl.ds(2 * me, 2), :]
    my_row = jnp.concatenate([my_rows[0:1], my_rows[1:2]], axis=1)
    my_block = my_row // slots
    my_slot = (my_row % slots).astype(F32)
    row_id = iota((slots, slots), 0)
    col_id = iota((slots, slots), 1).astype(F32)
    from_block = my_block == row_id // 2
    jmin = jnp.min(jnp.where(from_block, col_id, big), axis=1, keepdims=True)
    jmax = jnp.max(jnp.where(from_block, col_id, -1.0), axis=1, keepdims=True)
    picked = jnp.where(row_id % 2 == 0, jmin, jmax)
    at_pos = (picked == col_id).astype(F32)
    lives = jnp.broadcast_to(lives_ref[...].astype(F32), (slots, blocks))
    live_of = jnp.sum(
        jnp.where(iota((slots, blocks), 0) // 2 == iota((slots, blocks), 1), lives, 0.0), axis=1, keepdims=True
    )
    slot_there = jnp.sum(at_pos * my_slot, axis=1, keepdims=True)
    alive = (slot_there < live_of).astype(F32)
    at_pos_live = (at_pos * alive).T
    back_pos_ref[...] = at_pos_live.astype(BF16)
    live_pos = jnp.sum(at_pos_live, axis=1, keepdims=True)
    observed = observed_ref[...]
    seen_ref[...] = observed * live_pos
    back_slot_ref[...] = send_slot_f.T.astype(BF16)
    my_live = live_ref[me]
    element = element_ref[...].astype(F32)
    element_sent = jnp.sum(send_slot_f * element, axis=1, keepdims=True)
    hit = (element_sent.astype(I32) == iota((slots, LANES), 1)).astype(BF16)
    eh_ref[...] = jnp.concatenate([hit, hit], axis=1)
    weight = jnp.where(iota(weight_ref.shape, 1) < my_live, weight_ref[...], 0.0)
    weight = padded(weight, LANES, slots).T
    wp_ref[...] = pick(send_slot_b, weight)
    lane, time = iota((width, LANES), 1) - OBS_LANE, iota((width, LANES), 0)
    comp = time // STEPS
    flipped = comp * STEPS + (STEPS - 1 - (time - comp * STEPS))
    turn_time = (lane == flipped).astype(BF16)
    hi, mid, lo = split3(observed)
    reversed_rows = dot(hi, turn_time) + (dot(mid, turn_time) + dot(lo, turn_time))
    acc_ref[...] = pick(at_pos.astype(BF16), reversed_rows)


def plan(me, live_counts, derivative, coupling, face_lift, rec_element, rec_weight, order, observed):
    slots, width = observed.shape
    axes, fields = coupling.shape[0], coupling.shape[1]
    block = axes * fields * GROUP
    smem = pl.BlockSpec(memory_space=pltpu.SMEM)
    vmem = pl.BlockSpec(memory_space=VMEM)
    return pl.pallas_call(
        plan_kernel,
        in_specs=[smem, smem] + [vmem] * 8,
        out_shape=(
            jax.ShapeDtypeStruct((6 * LANES, 2 * LANES), BF16),
            jax.ShapeDtypeStruct((3 * LANES, 2 * LANES), BF16),
            jax.ShapeDtypeStruct((block, 3 * fields * GROUP), BF16),
            jax.ShapeDtypeStruct((slots, 2 * LANES), BF16),
            jax.ShapeDtypeStruct((slots, LANES), F32),
            jax.ShapeDtypeStruct((slots, LANES), F32),
            jax.ShapeDtypeStruct((slots, slots), BF16),
            jax.ShapeDtypeStruct((slots, slots), BF16),
            jax.ShapeDtypeStruct((slots, width), F32),
        ),
        compiler_params=pltpu.CompilerParams(vmem_limit_bytes=16 << 20),
        cost_estimate=pl.CostEstimate(flops=4_000_000_000, bytes_accessed=2_000_000, transcendentals=0),
        name="plan",
    )(
        me,
        live_counts,
        live_counts.reshape(1, -1),
        derivative,
        coupling,
        face_lift,
        rec_element.reshape(1, -1),
        rec_weight,
        order,
        observed,
    )


def march_kernel(
    me_ref,
    own_ref,
    low_ref,
    high_ref,
    wt_ref,
    wl_ref,
    ck_ref,
    eh_ref,
    wp_ref,
    acc0_ref,
    send_ref,
    rev_ref,
    u_ref,
    m_ref,
    h_ref,
    t_ref,
    lt_ref,
    lu_ref,
    *,
    last_block,
):
    planes, elems, _ = own_ref.shape
    axes = 3
    fields = planes - axes
    rows = elems + 2 * HALO
    pairs = rows // PAIR_ROWS
    slots = eh_ref.shape[0]
    dt = 0.5 / STEPS
    me = me_ref[0]
    dt_low = jnp.where(me == 0, 0.0, dt).astype(F32)
    dt_high = jnp.where(me == last_block, 0.0, dt).astype(F32)
    u_ref[:, :HALO, :] = low_ref[:fields]
    u_ref[:, HALO : HALO + elems, :] = own_ref[:fields]
    u_ref[:, HALO + elems :, :] = high_ref[:fields]
    m_ref[:, :HALO, :] = low_ref[fields:]
    m_ref[:, HALO : HALO + elems, :] = own_ref[fields:]
    m_ref[:, HALO + elems :, :] = high_ref[fields:]
    send_ref[...] = acc0_ref[...]
    rev_ref[...] = jnp.zeros(rev_ref.shape, F32)
    tile = fields * PAIR_ROWS

    def load_pair(j, r):
        halves = ([], [])
        for f in range(fields):
            x = u_ref[f, r : r + PAIR_ROWS, :]
            hi, lo = split2(x)
            lu_ref[j, f * PAIR_ROWS : (f + 1) * PAIR_ROWS, :LANES] = hi
            lu_ref[j, f * PAIR_ROWS : (f + 1) * PAIR_ROWS, LANES:] = lo
            hi32 = hi.astype(F32)
            lo32 = x - hi32
            for side in range(2):
                halves[side].append((hi32[side * GROUP : (side + 1) * GROUP], lo32[side * GROUP : (side + 1) * GROUP]))
        columns = []
        for side in range(2):
            his = [p[0] for p in halves[side]]
            los = [p[1] for p in halves[side]]
            columns.append(jnp.concatenate(his + los + his, axis=0).astype(BF16))
        return jnp.concatenate(columns, axis=1)

    def couple(j, r):
        v = dot(ck_ref[...], load_pair(j, r))
        for k in range(axes):
            ma = m_ref[k, r : r + GROUP, :]
            mb = m_ref[k, r + GROUP : r + PAIR_ROWS, :]
            parts = []
            for g in range(fields):
                base = (k * fields + g) * GROUP
                parts.append(v[base : base + GROUP, :LANES] * ma)
                parts.append(v[base : base + GROUP, LANES:] * mb)
            hi, lo = split2(jnp.concatenate(parts, axis=0))
            lanes = ((0, 4), (1, 5), (2, 3))[k]
            lt_ref[j, :, lanes[0] * LANES : (lanes[0] + 1) * LANES] = hi
            lt_ref[j, :, lanes[1] * LANES : (lanes[1] + 1) * LANES] = lo

    def apply(j, r):
        both = dot(lt_ref[j], wt_ref[...])
        both = both[:, :LANES] + both[:, LANES:]
        lifted = dot(lu_ref[j], wl_ref[: 2 * LANES, :]) + dot(lu_ref[j, :, :LANES], wl_ref[2 * LANES :, :])
        for g in range(fields):
            t_ref[g, r : r + PAIR_ROWS, :] = both[g * PAIR_ROWS : (g + 1) * PAIR_ROWS]
            for side in range(2):
                h_ref[side, g, GROUP + r : GROUP + r + PAIR_ROWS, :] = lifted[
                    g * PAIR_ROWS : (g + 1) * PAIR_ROWS, side * LANES : (side + 1) * LANES
                ]

    def update(r):
        a = GROUP + r
        factor = dt_low if r < HALO else (dt_high if r >= HALO + elems else dt)
        for g in range(fields):
            lift = (h_ref[0, g, a - 1 : a - 1 + GROUP, :] - h_ref[0, g, a : a + GROUP, :]) + (
                h_ref[1, g, a + 1 : a + 1 + GROUP, :] - h_ref[1, g, a : a + GROUP, :]
            )
            u_ref[g, r : r + GROUP, :] = u_ref[g, r : r + GROUP, :] + factor * (t_ref[g, r : r + GROUP, :] + lift)

    def sample(t):
        columns = []
        own = slice(HALO, HALO + elems)
        for c in range(COMPS):
            if c < 3:
                x = u_ref[c, own, :]
            else:
                x = (u_ref[3, own, :] + u_ref[4, own, :] + u_ref[5, own, :]) / 3.0
            columns.append(jnp.concatenate(split2(x), axis=0))
        lane = iota((slots, LANES), 1)
        send = send_ref[...]
        rev = rev_ref[...]
        for c in range(0, COMPS, 2):
            found = dot(eh_ref[...], jnp.concatenate(columns[c : c + 2], axis=1))
            for i in range(2):
                value = jnp.sum(found[:, i * LANES : (i + 1) * LANES] * wp_ref[...], axis=1, keepdims=True)
                send = jnp.where(lane == (c + i) * STEPS + t, value, send)
                rev = jnp.where(lane == OBS_LANE + (c + i) * STEPS + (STEPS - 1) - t, value, rev)
        send_ref[...] = send
        rev_ref[...] = rev

    def step(t, drop):
        sample(t - 1)
        base = drop * GROUP
        count = (rows - 2 * base) // PAIR_ROWS
        at = lambda j: base + j * PAIR_ROWS
        couple(0, at(0))
        for j in range(count):
            if j + 1 < count:
                couple(j + 1, at(j + 1))
            apply(j, at(j))
            if j >= 1:
                update(at(j - 1))
                update(at(j - 1) + GROUP)
        update(at(count - 1))
        update(at(count - 1) + GROUP)

    def run(drop):
        def body(t, carry):
            step(t, drop)
            return carry

        return body

    groups = [-(-(STEPS - t) // GROUP) for t in range(STEPS)]
    t = 0
    while t < STEPS:
        stop = t
        while stop < STEPS and groups[stop] == groups[t]:
            stop += 1
        lax.fori_loop(t, stop, run(HALO // GROUP - groups[t]), 0)
        t = stop
    sample(STEPS - 1)


def march(me, own, low, high, operators, last_block):
    wt, wl, ck, eh, wp, acc0 = operators
    planes, elems, _ = own.shape
    fields = planes - 3
    rows = elems + 2 * HALO
    pairs = rows // PAIR_ROWS
    slots = eh.shape[0]
    smem = pl.BlockSpec(memory_space=pltpu.SMEM)
    vmem = pl.BlockSpec(memory_space=VMEM)
    import functools

    return pl.pallas_call(
        functools.partial(march_kernel, last_block=last_block),
        in_specs=[smem] + [vmem] * 9,
        out_shape=(
            jax.ShapeDtypeStruct((slots, LANES), F32),
            jax.ShapeDtypeStruct((slots, LANES), F32),
        ),
        scratch_shapes=[
            VMEM((fields, rows, LANES), F32),
            VMEM((3, rows, LANES), F32),
            VMEM((2, fields, rows + 2 * GROUP, LANES), F32),
            VMEM((fields, rows, LANES), F32),
            VMEM((pairs, fields * PAIR_ROWS, 6 * LANES), BF16),
            VMEM((pairs, fields * PAIR_ROWS, 2 * LANES), BF16),
        ],
        compiler_params=pltpu.CompilerParams(vmem_limit_bytes=40 << 20),
        cost_estimate=pl.CostEstimate(flops=20_000_000_000, bytes_accessed=4_000_000, transcendentals=0),
        name="march",
    )(me, own, low, high, wt, wl, ck, eh, wp, acc0)


def finish_kernel(me_ref, live_ref, got_ref, rev_ref, back_slot_ref, back_pos_ref, seen_ref, res_ref, mis_ref, adj_ref):
    slots, width = res_ref.shape
    got = got_ref[...]
    ordered = pick(back_pos_ref[...], got)
    residual = ordered[:, :width] - seen_ref[...]
    res_ref[...] = residual
    squares = padded(residual * residual, slots, LANES)
    mis_ref[...] = 0.5 * jnp.sum(squares.T, axis=0, keepdims=True)
    adjoint = pick(back_slot_ref[...], pltpu.roll(rev_ref[...] - got, LANES - OBS_LANE, 1))
    live = iota((slots, LANES), 0) < live_ref[me_ref[0]]
    adj_ref[...] = jnp.where(live, adjoint, 0.0)[:, :width]


def finish(me, live_counts, got, rev, back_slot, back_pos, seen):
    slots, width = seen.shape
    smem = pl.BlockSpec(memory_space=pltpu.SMEM)
    vmem = pl.BlockSpec(memory_space=VMEM)
    return pl.pallas_call(
        finish_kernel,
        in_specs=[smem, smem] + [vmem] * 5,
        out_shape=(
            jax.ShapeDtypeStruct((slots, width), F32),
            jax.ShapeDtypeStruct((1, slots), F32),
            jax.ShapeDtypeStruct((slots, width), F32),
        ),
        compiler_params=pltpu.CompilerParams(vmem_limit_bytes=8 << 20),
        name="finish",
    )(me, live_counts, got, rev, back_slot, back_pos, seen)


def shards(
    initial,
    derivative,
    coupling,
    face_lift,
    metric,
    rec_element,
    rec_weight,
    live_counts,
    shot_order,
    observed,
):
    blocks = lax.axis_size(MX)
    slots = rec_element.shape[0]
    me = lax.axis_index(MX).astype(I32).reshape(1)
    own, low, high = turn(initial, metric)
    forward = [(i, i + 1) for i in range(blocks - 1)]
    backward = [(target, source) for source, target in forward]
    from_low = lax.ppermute(high, MX, forward)
    from_high = lax.ppermute(low, MX, backward)
    order = shot_order.reshape(-1, LANES)
    wt, wl, ck, eh, wp, acc0, back_slot, back_pos, seen = plan(
        me, live_counts, derivative, coupling, face_lift, rec_element, rec_weight, order, observed
    )
    send, rev = march(me, own, from_low, from_high, (wt, wl, ck, eh, wp, acc0), blocks - 1)
    got = lax.all_to_all(send.reshape(blocks, 2, LANES), MX, split_axis=0, concat_axis=0, tiled=True)
    residual, misfit, adjoint = finish(me, live_counts, got.reshape(slots, LANES), rev, back_slot, back_pos, seen)
    return (residual, misfit.reshape(slots), adjoint)


def solution(mesh):
    split = Mesh(
        mesh.devices.reshape(mesh.shape["shots"], 8, 8, 2), ("shots", "mx_0", "mx_1", "mx_2")
    )
    in_specs = (
        P("shots", None, MX),
        P(),
        P(),
        P(),
        P(None, MX),
        P(MX),
        P(None, MX),
        P(),
        P(),
        P(SHOTS_MX, None),
    )
    out_specs = (P(SHOTS_MX, None), P(SHOTS_MX), P(SHOTS_MX, None))
    return jax.shard_map(
        shards, mesh=split, in_specs=in_specs, out_specs=out_specs, check_vma=False
    )
```

```python
import functools

import jax
import jax.numpy as jnp
from jax import lax
from jax.experimental import pallas as pl
from jax.experimental.pallas import tpu as pltpu
from jax.sharding import Mesh
from jax.sharding import PartitionSpec as P


STEPS = 12
EARLY = 3
DT = 0.5 / STEPS
AXES = 3
COMPS = 4
MX = ("mx_0", "mx_1", "mx_2")
SHOTS_MX = ("shots", "mx_0", "mx_1", "mx_2")
F32 = jnp.float32
BF16 = jnp.bfloat16
I32 = jnp.int32
LANES = 128
GROUP = 8
PAIR_ROWS = 2 * GROUP
HALO = 16
OBS_LANE = 64
VMEM = pltpu.VMEM


def iota(shape, dim):
    return lax.broadcasted_iota(I32, shape, dim)


def split2(x):
    hi = x.astype(BF16)
    return hi, (x - hi.astype(F32)).astype(BF16)


def split3(x):
    hi = x.astype(BF16)
    rest = x - hi.astype(F32)
    mid = rest.astype(BF16)
    return hi, mid, (rest - mid.astype(F32)).astype(BF16)


def dot(a, b):
    return jnp.dot(a, b, preferred_element_type=F32)


def pick(onehot, x):
    parts = split3(x)
    return dot(onehot, parts[0]) + (dot(onehot, parts[1]) + dot(onehot, parts[2]))


def padded(x, rows, cols):
    if x.shape[1] < cols:
        x = jnp.concatenate([x, jnp.zeros((x.shape[0], cols - x.shape[1]), x.dtype)], axis=1)
    if x.shape[0] < rows:
        x = jnp.concatenate([x, jnp.zeros((rows - x.shape[0], cols), x.dtype)], axis=0)
    return x


def turn_kernel(me_ref, *refs):
    staged = (len(refs) - 10) // 2
    initial_hbm, metric_hbm = refs[:2]
    from_refs = refs[2 : 2 + staged]
    own_ref, near_ref, far_ref = refs[2 + staged : 5 + staged]
    to_refs = refs[5 + staged : 5 + 2 * staged]
    initial_ref, metric_ref, low_ref, high_ref, sems = refs[-5:]
    copies = [
        pltpu.make_async_copy(initial_hbm, initial_ref, sems.at[0]),
        pltpu.make_async_copy(metric_hbm, metric_ref, sems.at[1]),
    ]
    copies += [pltpu.make_async_copy(x, y, sems.at[2 + i]) for i, (x, y) in enumerate(zip(from_refs, to_refs))]
    for copy in copies:
        copy.start()
    copies[0].wait()
    copies[1].wait()
    fields, _, elems = initial_ref.shape
    for f in range(fields):
        own_ref[f] = padded(initial_ref[f], LANES, elems).T
    for k in range(metric_ref.shape[0]):
        own_ref[fields + k] = jnp.broadcast_to(metric_ref[k : k + 1, :], (LANES, elems)).T
    third = iota((elems, LANES), 1) // (LANES // 3)
    factors = jnp.where(third == 0, own_ref[fields], jnp.where(third == 1, own_ref[fields + 1], own_ref[fields + 2]))
    for edge_ref, rows in ((low_ref, slice(0, STEPS)), (high_ref, slice(elems - STEPS, elems))):
        for f in range(fields):
            edge_ref[f * STEPS : (f + 1) * STEPS, :] = own_ref[f, rows, :]
        edge_ref[fields * STEPS :, :] = factors[rows]
    odd = me_ref[0] % 2 == 1
    near_ref[...] = jnp.where(odd, low_ref[...], high_ref[...])
    far_ref[...] = jnp.where(odd, high_ref[...], low_ref[...])
    for copy in copies[2:]:
        copy.wait()


def turn(me, initial, metric, staged):
    fields, _, elems = initial.shape
    planes = fields + metric.shape[0]
    edge = jax.ShapeDtypeStruct(((fields + 1) * STEPS, LANES), F32)
    hbm = pl.BlockSpec(memory_space=pltpu.HBM)
    return pl.pallas_call(
        turn_kernel,
        in_specs=[pl.BlockSpec(memory_space=pltpu.SMEM)] + [hbm] * (2 + len(staged)),
        out_shape=(jax.ShapeDtypeStruct((planes, elems, LANES), F32), edge, edge)
        + tuple(jax.ShapeDtypeStruct(x.shape, x.dtype) for x in staged),
        scratch_shapes=[
            VMEM(initial.shape, F32),
            VMEM(metric.shape, F32),
            VMEM(edge.shape, F32),
            VMEM(edge.shape, F32),
            pltpu.SemaphoreType.DMA((2 + len(staged),)),
        ],
        compiler_params=pltpu.CompilerParams(vmem_limit_bytes=8 << 20),
        name="turn",
    )(me, *(pltpu.with_memory_space_constraint(x, pltpu.HBM) for x in (initial, metric, *staged)))


def plan_kernel(
    me_ref,
    lives_ref,
    derivative_ref,
    coupling_ref,
    lift_ref,
    element_ref,
    weight_ref,
    order_ref,
    observed_ref,
    wt_ref,
    wl_ref,
    ck_ref,
    eh_ref,
    wp_ref,
    acc_ref,
    to_slot_ref,
    to_pos_ref,
    seen_ref,
):
    width, slots = observed_ref.shape
    blocks = slots // 2
    me = me_ref[0]
    axes = derivative_ref.shape[0]
    fields = coupling_ref.shape[1]
    dh, dl = [], []
    for k in range(axes):
        hi, lo = split2(padded(derivative_ref[k], LANES, LANES).T)
        dh.append(hi)
        dl.append(lo)
    zero = jnp.zeros((LANES, LANES), BF16)
    for row, (left, right) in enumerate(
        [(dh[0], dl[0]), (dh[1], dl[1]), (dh[2], dl[2]), (dh[2], zero), (dh[0], zero), (dh[1], zero)]
    ):
        wt_ref[row * LANES : (row + 1) * LANES, :] = jnp.concatenate([left, right], axis=1)
    l0h, l0l = split2(padded(lift_ref[0], LANES, LANES).T)
    l1h, l1l = split2(padded(lift_ref[1], LANES, LANES).T)
    for row, (left, right) in enumerate([(l0h, l1h), (l0h, l1h), (l0l, l1l)]):
        wl_ref[row * LANES : (row + 1) * LANES, :] = jnp.concatenate([left, right], axis=1)
    rows, cols = axes * fields * GROUP, fields * GROUP
    spread_rows = (iota((rows, axes * fields), 0) // GROUP == iota((rows, axes * fields), 1)).astype(BF16)
    spread_cols = (iota((fields, cols), 0) == iota((fields, cols), 1) // GROUP).astype(BF16)
    stacked = jnp.concatenate([coupling_ref[k] for k in range(axes)], axis=0)
    by_row = pick(spread_rows, stacked)
    by_hi, by_mid, by_lo = split3(by_row)
    full = dot(by_hi, spread_cols) + (dot(by_mid, spread_cols) + dot(by_lo, spread_cols))
    diagonal = iota((rows, cols), 0) % GROUP == iota((rows, cols), 1) % GROUP
    full = jnp.where(diagonal, full, 0.0)
    full_hi = full.astype(BF16).astype(F32)
    ck_ref[...] = jnp.concatenate([full_hi, full_hi, full - full_hi], axis=1).astype(BF16)
    order = order_ref[...]
    half = iota((slots, LANES), 0) % 2
    position = half * LANES + iota((slots, LANES), 1)
    slot_of = order % slots
    key = (position * slots + slot_of).astype(F32)
    mine = (order // slots) == me
    big = float(slots * slots)
    first = jnp.min(jnp.where(mine, key, big), axis=1, keepdims=True)
    last = jnp.max(jnp.where(mine, key, -1.0), axis=1, keepdims=True)
    first = jnp.broadcast_to(first, (slots, LANES))
    last = jnp.broadcast_to(last, (slots, LANES))
    up = lambda x: pltpu.roll(x, slots - 1, 0)
    down = lambda x: pltpu.roll(x, 1, 0)
    chosen = jnp.where(half == 0, jnp.minimum(first, up(first)), jnp.maximum(last, down(last)))
    chosen = chosen.astype(I32) % slots
    chosen = jnp.concatenate([chosen, chosen], axis=1)
    send_slot = chosen == iota((slots, slots), 1)
    send_slot_f = send_slot.astype(F32)
    send_slot_b = send_slot_f.astype(BF16)
    my_rows = order_ref[pl.ds(2 * me, 2), :]
    my_row = jnp.concatenate([my_rows[0:1], my_rows[1:2]], axis=1)
    my_block = my_row // slots
    my_slot = (my_row % slots).astype(F32)
    row_id = iota((slots, slots), 0)
    col_id = iota((slots, slots), 1).astype(F32)
    from_block = my_block == row_id // 2
    jmin = jnp.min(jnp.where(from_block, col_id, big), axis=1, keepdims=True)
    jmax = jnp.max(jnp.where(from_block, col_id, -1.0), axis=1, keepdims=True)
    picked = jnp.where(row_id % 2 == 0, jmin, jmax)
    at_pos = (picked == col_id).astype(F32)
    lives = jnp.broadcast_to(lives_ref[...].astype(F32), (slots, blocks))
    live_of = jnp.sum(
        jnp.where(iota((slots, blocks), 0) // 2 == iota((slots, blocks), 1), lives, 0.0), axis=1, keepdims=True
    )
    slot_there = jnp.sum(at_pos * my_slot, axis=1, keepdims=True)
    alive = (slot_there < live_of).astype(F32)
    at_pos_live = at_pos * alive
    to_pos_ref[...] = at_pos_live.astype(BF16)
    observed = observed_ref[...]
    seen_ref[...] = observed * jnp.sum(at_pos_live, axis=0, keepdims=True)
    lives_row = lives_ref[...].astype(F32)
    my_live = jnp.sum(jnp.where(iota((1, blocks), 1) == me, lives_row, 0.0), axis=1, keepdims=True)
    element = jnp.concatenate([element_ref[0:1], element_ref[1:2]], axis=1).astype(F32)
    element_sent = jnp.sum(send_slot_f * element, axis=1, keepdims=True)
    hit = (element_sent.astype(I32) == iota((slots, LANES), 1)).astype(BF16)
    eh_ref[...] = jnp.concatenate([hit, hit], axis=1)
    live_slot = iota((1, slots), 1).astype(F32) < my_live
    to_slot_ref[...] = jnp.where(live_slot, send_slot_f, 0.0).astype(BF16)
    weight = jnp.where(live_slot, weight_ref[...], 0.0)
    weight = padded(weight, LANES, slots).T
    wp_ref[...] = pick(send_slot_b, weight)
    lane, time = iota((LANES, width), 0) - OBS_LANE, iota((LANES, width), 1)
    comp = time // STEPS
    flipped = comp * STEPS + (STEPS - 1 - (time - comp * STEPS))
    turn_time = (lane == flipped).astype(BF16)
    sent = at_pos.astype(BF16)
    rows_out = [dot(turn_time, part).astype(BF16) for part in split3(observed)]
    across = lambda part: lax.dot_general(sent, part, (((1,), (1,)), ((), ())), preferred_element_type=F32)
    acc_ref[...] = across(rows_out[0]) + (across(rows_out[1]) + across(rows_out[2]))


def plan(me, lives, derivative, coupling, face_lift, rec_element, rec_weight, order, observed):
    width, slots = observed.shape
    axes, fields = coupling.shape[0], coupling.shape[1]
    block = axes * fields * GROUP
    smem = pl.BlockSpec(memory_space=pltpu.SMEM)
    vmem = pl.BlockSpec(memory_space=VMEM)
    return pl.pallas_call(
        plan_kernel,
        in_specs=[smem] + [vmem] * 8,
        out_shape=(
            jax.ShapeDtypeStruct((6 * LANES, 2 * LANES), BF16),
            jax.ShapeDtypeStruct((3 * LANES, 2 * LANES), BF16),
            jax.ShapeDtypeStruct((block, 3 * fields * GROUP), BF16),
            jax.ShapeDtypeStruct((slots, 2 * LANES), BF16),
            jax.ShapeDtypeStruct((slots, LANES), F32),
            jax.ShapeDtypeStruct((slots, LANES), F32),
            jax.ShapeDtypeStruct((slots, slots), BF16),
            jax.ShapeDtypeStruct((slots, slots), BF16),
            jax.ShapeDtypeStruct((width, slots), F32),
        ),
        compiler_params=pltpu.CompilerParams(vmem_limit_bytes=16 << 20),
        cost_estimate=pl.CostEstimate(flops=4_000_000_000, bytes_accessed=2_000_000, transcendentals=0),
        name="plan",
    )(
        me,
        lives,
        derivative,
        coupling,
        face_lift,
        rec_element,
        rec_weight,
        order,
        observed,
    )


class Stepper:
    def __init__(self, fields, load, store, factor, metric, wt_ref, wl_ref, ck_ref, t_ref, h_ref, lt_ref, lu_ref):
        self.fields, self.load, self.store, self.factor, self.metric = fields, load, store, factor, metric
        self.wt_ref, self.wl_ref, self.ck_ref = wt_ref, wl_ref, ck_ref
        self.t_ref, self.h_ref, self.lt_ref, self.lu_ref = t_ref, h_ref, lt_ref, lu_ref

    def split(self, item):
        halves = ([], [])
        for f in range(self.fields):
            x = jnp.concatenate([self.load(item.t, f, g) for g in item.groups], axis=0)
            hi, lo = split2(x)
            rows = slice(f * PAIR_ROWS, (f + 1) * PAIR_ROWS)
            self.lu_ref[item.slot, rows, :LANES] = hi
            self.lu_ref[item.slot, rows, LANES:] = lo
            hi32 = hi.astype(F32)
            lo32 = x - hi32
            for side in range(2):
                part = slice(side * GROUP, (side + 1) * GROUP)
                halves[side].append((hi32[part], lo32[part]))
        return halves

    def couple(self, item):
        columns = []
        for side in self.split(item):
            his, los = [p[0] for p in side], [p[1] for p in side]
            columns.append(jnp.concatenate(his + los + his, axis=0).astype(BF16))
        if item.lift_only:
            return
        v = dot(self.ck_ref[...], jnp.concatenate(columns, axis=1))
        for k in range(AXES):
            scale = [self.metric(k, g) for g in item.groups]
            parts = []
            for f in range(self.fields):
                base = (k * self.fields + f) * GROUP
                for side in range(2):
                    parts.append(v[base : base + GROUP, side * LANES : (side + 1) * LANES] * scale[side])
            for lane, part in zip(((0, 4), (1, 5), (2, 3))[k], split2(jnp.concatenate(parts, axis=0))):
                self.lt_ref[item.slot, :, lane * LANES : (lane + 1) * LANES] = part

    def apply(self, item):
        lu = self.lu_ref.at[item.slot]
        if not item.lift_only:
            both = dot(self.lt_ref[item.slot], self.wt_ref[...])
            both = both[:, :LANES] + both[:, LANES:]
        lifted = dot(lu[...], self.wl_ref[: 2 * LANES, :]) + dot(lu[:, :LANES], self.wl_ref[2 * LANES :, :])
        for f in range(self.fields):
            for side, g in enumerate(item.groups):
                rows = slice(f * PAIR_ROWS + side * GROUP, f * PAIR_ROWS + (side + 1) * GROUP)
                if not item.lift_only:
                    self.t_ref[f, g * GROUP : (g + 1) * GROUP, :] = both[rows]
                for face in range(2):
                    at = (g + 1) * GROUP
                    self.h_ref[face, f, at : at + GROUP, :] = lifted[rows, face * LANES : (face + 1) * LANES]

    def update(self, t, g):
        at = (g + 1) * GROUP
        here, before, after = slice(at, at + GROUP), slice(at - 1, at - 1 + GROUP), slice(at + 1, at + 1 + GROUP)
        for f in range(self.fields):
            low, high = self.h_ref.at[0, f], self.h_ref.at[1, f]
            lift = (low[before, :] - low[here, :]) + (high[after, :] - high[here, :])
            rate = self.t_ref[f, g * GROUP : (g + 1) * GROUP, :] + lift
            self.store(t, f, g, self.load(t, f, g) + self.factor(g) * rate)

    def run(self, items, ready, after=lambda index: None):
        ready = set(ready)
        product, lifted, done = set(), set(), set()
        wanted = {}
        for item in items:
            for g in item.groups:
                wanted.setdefault(item.t, {})[g] = item
        coupled = 0

        def couple_next(limit):
            nonlocal coupled
            while coupled < limit and all((items[coupled].t, g) in ready for g in items[coupled].groups):
                self.couple(items[coupled])
                coupled += 1

        for index, item in enumerate(items):
            couple_next(min(index + 2, len(items)))
            assert coupled > index
            self.apply(item)
            for g in item.groups:
                lifted.add((item.t, g))
                if not item.lift_only:
                    product.add((item.t, g))
            for t, groups in wanted.items():
                for g in groups:
                    if (t, g) in done or (t, g) not in product:
                        continue
                    if all(n not in groups or (t, n) in lifted for n in (g - 1, g + 1)):
                        self.update(t, g)
                        done.add((t, g))
                        ready.add((t + 1, g))
            after(index)


class Item:
    def __init__(self, t, slot, groups, lift_only=False):
        self.t, self.slot, self.groups, self.lift_only = t, slot, groups, lift_only


def own_pair(t, j):
    first = HALO // GROUP + 2 * j
    return Item(t, j, (first, first + 1))


def early_kernel(own_ref, wt_ref, wl_ref, ck_ref, *refs):
    past = refs[:EARLY]
    t_ref, h_ref, lt_ref, lu_ref = refs[EARLY:]
    planes, elems, _ = own_ref.shape
    fields = planes - AXES
    shift = HALO // GROUP
    rows = lambda g: slice((g - shift) * GROUP, (g - shift + 1) * GROUP)

    def load(t, f, g):
        return own_ref[f, rows(g), :] if t == 0 else past[t - 1][f, rows(g), :]

    def store(t, f, g, value):
        past[t][f, rows(g), :] = value

    pad = slice(HALO, HALO + GROUP), slice(elems + HALO + GROUP, elems + HALO + 2 * GROUP)
    for rim in pad:
        h_ref[:, :, rim, :] = jnp.zeros((2, fields, GROUP, LANES), F32)
    stepper = Stepper(
        fields, load, store, lambda g: DT, lambda k, g: own_ref[fields + k, rows(g), :],
        wt_ref, wl_ref, ck_ref, t_ref, h_ref, lt_ref, lu_ref,
    )
    pairs = elems // PAIR_ROWS
    order = sorted(range(pairs), key=lambda j: abs(2 * j + 1 - pairs))
    items = [own_pair(t, j) for t in range(EARLY) for j in order]
    stepper.run(items, {(0, g) for item in items for g in item.groups})


def scratch(fields, elems):
    rows = elems + 2 * HALO
    tile = fields * PAIR_ROWS
    slots = rows // PAIR_ROWS + 1
    return [
        VMEM((fields, rows, LANES), F32),
        VMEM((2, fields, rows + 2 * GROUP, LANES), F32),
        VMEM((slots, tile, 6 * LANES), BF16),
        VMEM((slots, tile, 2 * LANES), BF16),
    ]


def early(own, wt, wl, ck):
    planes, elems, _ = own.shape
    fields = planes - AXES
    return pl.pallas_call(
        early_kernel,
        out_shape=tuple(jax.ShapeDtypeStruct((fields, elems, LANES), F32) for _ in range(EARLY)),
        scratch_shapes=scratch(fields, elems),
        compiler_params=pltpu.CompilerParams(vmem_limit_bytes=32 << 20),
        cost_estimate=pl.CostEstimate(flops=5_000_000_000, bytes_accessed=4_000_000, transcendentals=0),
        name="early",
    )(own, wt, wl, ck)


def march_kernel(me_ref, own_ref, near_ref, far_ref, *refs, last_block):
    past = (own_ref,) + refs[:EARLY]
    wt_ref, wl_ref, ck_ref, eh_ref, wp_ref, acc0_ref, send_ref, rev_ref, edge_ref, u_ref, m_ref = refs[EARLY : EARLY + 11]
    t_ref, h_ref, lt_ref, lu_ref = refs[EARLY + 11 :]
    planes, elems, _ = own_ref.shape
    fields = planes - AXES
    slots = eh_ref.shape[0]
    shift = HALO // GROUP
    groups = elems // GROUP + 2 * shift
    me = me_ref[0]
    dt_low = jnp.where(me == 0, 0.0, DT).astype(F32)
    dt_high = jnp.where(me == last_block, 0.0, DT).astype(F32)
    rim = list(range(shift + 1)) + list(range(groups - shift - 1, groups))
    own_rows = lambda g: slice((g - shift) * GROUP, (g - shift + 1) * GROUP)
    rim_rows = lambda g: slice(rim.index(g) * GROUP, (rim.index(g) + 1) * GROUP)
    all_rows = lambda g: slice(g * GROUP, (g + 1) * GROUP)

    odd = me % 2 == 1
    low_edge = lambda edge: jnp.where(odd, near_ref[edge], far_ref[edge])
    high_edge = lambda edge: jnp.where(odd, far_ref[edge], near_ref[edge])
    spare = jnp.zeros((HALO - STEPS, LANES), F32)
    low_rim, high_rim = slice(0, HALO), slice((shift + 2) * GROUP, (2 * shift + 2) * GROUP)
    for f in range(fields):
        edge = slice(f * STEPS, (f + 1) * STEPS)
        edge_ref[0, f, low_rim, :] = jnp.concatenate([spare, jnp.where(me > 0, low_edge(edge), 0.0)], axis=0)
        edge_ref[0, f, high_rim, :] = jnp.concatenate([jnp.where(me < last_block, high_edge(edge), 0.0), spare], axis=0)
    edge = slice(fields * STEPS, (fields + 1) * STEPS)
    low_factors, high_factors = low_edge(edge), high_edge(edge)
    for k in range(AXES):
        lane = k * (LANES // AXES)
        spread = lambda x: jnp.broadcast_to(x[:, lane : lane + 1], (STEPS, LANES))
        m_ref[k, :HALO, :] = jnp.concatenate([spare, spread(low_factors)], axis=0)
        m_ref[k, HALO:, :] = jnp.concatenate([spread(high_factors), spare], axis=0)
    h_ref[:, :, :GROUP, :] = jnp.zeros((2, fields, GROUP, LANES), F32)
    h_ref[:, :, (groups + 1) * GROUP :, :] = jnp.zeros((2, fields, GROUP, LANES), F32)
    send_ref[...] = acc0_ref[...]
    rev_ref[...] = jnp.zeros(rev_ref.shape, F32)

    def load(t, f, g):
        if t > EARLY:
            return u_ref[t % 2, f, all_rows(g), :]
        if g in rim and not (t == 0 and shift <= g < groups - shift):
            return edge_ref[t, f, rim_rows(g), :]
        return past[t][f, own_rows(g), :]

    def store(t, f, g, value):
        if t >= EARLY:
            u_ref[(t + 1) % 2, f, all_rows(g), :] = value
            return
        row = iota((GROUP, LANES), 0)
        if g == shift:
            value = jnp.where(row <= t, value, past[t + 1][f, own_rows(g), :])
        if g == groups - shift - 1:
            value = jnp.where(row >= GROUP - 1 - t, value, past[t + 1][f, own_rows(g), :])
        edge_ref[t + 1, f, rim_rows(g), :] = value

    def metric(k, g):
        if g < shift:
            return m_ref[k, g * GROUP : (g + 1) * GROUP, :]
        if g >= groups - shift:
            at = HALO + (g - groups + shift) * GROUP
            return m_ref[k, at : at + GROUP, :]
        return own_ref[fields + k, own_rows(g), :]

    def factor(g):
        return dt_low if g < shift else (dt_high if g >= groups - shift else DT)

    def sample(t):
        field = lambda f: jnp.concatenate([load(t + 1, f, g) for g in range(shift, groups - shift)], axis=0)
        columns = []
        for c in range(COMPS):
            x = field(c) if c < 3 else (field(3) + field(4) + field(5)) / 3.0
            columns.append(jnp.concatenate(split2(x), axis=0))
        lane = iota((slots, LANES), 1)
        send = send_ref[...]
        rev = rev_ref[...]
        for c in range(0, COMPS, 2):
            found = dot(eh_ref[...], jnp.concatenate(columns[c : c + 2], axis=1))
            for i in range(2):
                value = jnp.sum(found[:, i * LANES : (i + 1) * LANES] * wp_ref[...], axis=1, keepdims=True)
                send = jnp.where(lane == (c + i) * STEPS + t, value, send)
                rev = jnp.where(lane == OBS_LANE + (c + i) * STEPS + (STEPS - 1) - t, value, rev)
        send_ref[...] = send
        rev_ref[...] = rev

    pairs = elems // PAIR_ROWS
    order = sorted(range(pairs), key=lambda j: abs(2 * j + 1 - pairs))
    inner, outer = order[:-2], order[-2:]
    halo_pair = lambda t, ring, lift_only=False: Item(t, pairs + ring, (shift - 1 - ring, groups - shift + ring), lift_only)
    first_pair = lambda t: Item(t, pairs + shift, (shift, groups - shift - 1))
    items, samples = [], {}
    fill = -(-len(inner) // EARLY)
    for t in range(EARLY):
        items += [first_pair(t)] + [halo_pair(t, ring) for ring in range(shift)]
        items += [own_pair(EARLY, j) for j in inner[t * fill : (t + 1) * fill]]
        if t >= 1:
            samples[len(items) - 1] = t - 1
    for t in range(EARLY, STEPS):
        items += [own_pair(t, j) for j in (outer if t == EARLY else order)]
        if t > EARLY:
            samples[len(items) - len(order) + 3] = t - 1
        for ring in range(shift):
            if ring * GROUP < STEPS - t:
                items.append(halo_pair(t, ring, lift_only=ring * GROUP >= STEPS - 1 - t))
        if t == EARLY:
            samples[len(items) - 2] = EARLY - 1
    ready = {(0, g) for g in rim} | {(EARLY, g) for g in range(groups) if g not in rim}
    stepper = Stepper(
        fields, load, store, factor, metric, wt_ref, wl_ref, ck_ref, t_ref, h_ref, lt_ref, lu_ref
    )
    stepper.run(items, ready, lambda index: sample(samples[index]) if index in samples else None)
    sample(STEPS - 1)


def march(me, own, near, far, past, operators, last_block):
    eh = operators[3]
    planes, elems, _ = own.shape
    fields = planes - AXES
    slots = eh.shape[0]
    smem = pl.BlockSpec(memory_space=pltpu.SMEM)
    vmem = pl.BlockSpec(memory_space=VMEM)
    return pl.pallas_call(
        functools.partial(march_kernel, last_block=last_block),
        in_specs=[smem] + [vmem] * (3 + EARLY + len(operators)),
        out_shape=(
            jax.ShapeDtypeStruct((slots, LANES), F32),
            jax.ShapeDtypeStruct((slots, LANES), F32),
        ),
        scratch_shapes=[
            VMEM((EARLY + 1, fields, 2 * (HALO + GROUP), LANES), F32),
            VMEM((2, fields, elems + 2 * HALO, LANES), F32),
            VMEM((AXES, 2 * HALO, LANES), F32),
        ]
        + scratch(fields, elems),
        compiler_params=pltpu.CompilerParams(vmem_limit_bytes=40 << 20),
        cost_estimate=pl.CostEstimate(flops=20_000_000_000, bytes_accessed=4_000_000, transcendentals=0),
        name="march",
    )(me, own, near, far, *past, *operators)


def finish_kernel(
    got_ref, rev_ref, to_slot_ref, to_pos_ref, seen_ref, res_hbm, mis_hbm, adj_hbm, res_ref, mis_ref, adj_ref, sems
):
    width, _ = seen_ref.shape
    got = got_ref[...]
    lane = iota(got.shape, 1)
    turned = jnp.where(lane < OBS_LANE, got, rev_ref[...] - got).T

    def place(rows, onehot):
        found = dot(jnp.concatenate(split3(rows), axis=0), onehot)
        return found[:width] + (found[width : 2 * width] + found[2 * width :])

    residual = place(turned[:width], to_pos_ref[...]) - seen_ref[...]
    res_ref[...] = residual
    first = pltpu.make_async_copy(res_ref, res_hbm, sems.at[0])
    first.start()
    mis_ref[...] = 0.5 * jnp.sum(residual * residual, axis=0, keepdims=True)
    second = pltpu.make_async_copy(mis_ref, mis_hbm, sems.at[1])
    second.start()
    adj_ref[...] = place(turned[OBS_LANE : OBS_LANE + width], to_slot_ref[...])
    third = pltpu.make_async_copy(adj_ref, adj_hbm, sems.at[2])
    third.start()
    first.wait()
    second.wait()
    third.wait()


def finish(got, rev, to_slot, to_pos, seen):
    width, slots = seen.shape
    vmem = pl.BlockSpec(memory_space=VMEM)
    hbm = pl.BlockSpec(memory_space=pltpu.HBM)
    shapes = ((width, slots), (1, slots), (width, slots))
    return pl.pallas_call(
        finish_kernel,
        in_specs=[vmem] * 5,
        out_specs=(hbm, hbm, hbm),
        out_shape=tuple(jax.ShapeDtypeStruct(shape, F32) for shape in shapes),
        scratch_shapes=[VMEM(shape, F32) for shape in shapes] + [pltpu.SemaphoreType.DMA((3,))],
        compiler_params=pltpu.CompilerParams(vmem_limit_bytes=8 << 20),
        name="finish",
    )(got, rev, to_slot, to_pos, seen)


def shards(
    initial,
    derivative,
    coupling,
    face_lift,
    metric,
    rec_element,
    rec_weight,
    live_counts,
    shot_order,
    observed,
):
    blocks = lax.axis_size(MX)
    slots = rec_element.shape[0]
    me = lax.axis_index(MX).astype(I32).reshape(1)
    order, element, lives = (x.reshape(-1, LANES) for x in (shot_order, rec_element, live_counts))
    staged = (derivative, rec_weight, order, element, lives, observed.T)
    own, near, far, derivative, rec_weight, order, element, lives, observed = turn(me, initial, metric, staged)
    pairs = [(i, min(i + 1, blocks - 1) if i % 2 else max(i - 1, 0)) for i in range(blocks)]
    far = lax.ppermute(far, MX, pairs)
    near = lax.ppermute(near, MX, [(i, i ^ 1) for i in range(blocks)])
    wt, wl, ck, eh, wp, acc0, to_slot, to_pos, seen = plan(
        me, lives, derivative, coupling, face_lift, element, rec_weight, order, observed
    )
    past = early(own, wt, wl, ck)
    send, rev = march(me, own, near, far, past, (wt, wl, ck, eh, wp, acc0), blocks - 1)
    got = lax.all_to_all(send.reshape(blocks, 2, LANES), MX, split_axis=0, concat_axis=0, tiled=True)
    residual, misfit, adjoint = finish(got.reshape(slots, LANES), rev, to_slot, to_pos, seen)
    return (residual.T, misfit.reshape(slots), adjoint.T)


def solution(mesh):
    split = Mesh(
        mesh.devices.reshape(mesh.shape["shots"], 8, 8, 2), ("shots", "mx_0", "mx_1", "mx_2")
    )
    in_specs = (
        P("shots", None, MX),
        P(),
        P(),
        P(),
        P(None, MX),
        P(MX),
        P(None, MX),
        P(),
        P(),
        P(SHOTS_MX, None),
    )
    out_specs = (P(SHOTS_MX, None), P(SHOTS_MX), P(SHOTS_MX, None))
    return jax.shard_map(
        shards, mesh=split, in_specs=in_specs, out_specs=out_specs, check_vma=False
    )
```

```python
import functools

import jax
import jax.numpy as jnp
from jax import lax
from jax.experimental import pallas as pl
from jax.experimental.pallas import tpu as pltpu
from jax.sharding import Mesh
from jax.sharding import PartitionSpec as P


STEPS = 12
EARLY = 3
DT = 0.5 / STEPS
AXES = 3
COMPS = 4
MX = ("mx_0", "mx_1", "mx_2")
SHOTS_MX = ("shots", "mx_0", "mx_1", "mx_2")
F32 = jnp.float32
BF16 = jnp.bfloat16
I32 = jnp.int32
LANES = 128
GROUP = 8
PAIR_ROWS = 2 * GROUP
HALO = 16
OBS_LANE = 64
VMEM = pltpu.VMEM


def iota(shape, dim):
    return lax.broadcasted_iota(I32, shape, dim)


def split2(x):
    hi = x.astype(BF16)
    return hi, (x - hi.astype(F32)).astype(BF16)


def split3(x):
    hi = x.astype(BF16)
    rest = x - hi.astype(F32)
    mid = rest.astype(BF16)
    return hi, mid, (rest - mid.astype(F32)).astype(BF16)


def dot(a, b):
    return jnp.dot(a, b, preferred_element_type=F32)


def pick(onehot, x):
    parts = split3(x)
    return dot(onehot, parts[0]) + (dot(onehot, parts[1]) + dot(onehot, parts[2]))


def padded(x, rows, cols):
    if x.shape[1] < cols:
        x = jnp.concatenate([x, jnp.zeros((x.shape[0], cols - x.shape[1]), x.dtype)], axis=1)
    if x.shape[0] < rows:
        x = jnp.concatenate([x, jnp.zeros((rows - x.shape[0], cols), x.dtype)], axis=0)
    return x


def turn_kernel(me_ref, *refs):
    staged = (len(refs) - 10) // 2
    initial_hbm, metric_hbm = refs[:2]
    from_refs = refs[2 : 2 + staged]
    own_ref, near_ref, far_ref = refs[2 + staged : 5 + staged]
    to_refs = refs[5 + staged : 5 + 2 * staged]
    initial_ref, metric_ref, low_ref, high_ref, sems = refs[-5:]
    copies = [
        pltpu.make_async_copy(initial_hbm, initial_ref, sems.at[0]),
        pltpu.make_async_copy(metric_hbm, metric_ref, sems.at[1]),
    ]
    copies += [pltpu.make_async_copy(x, y, sems.at[2 + i]) for i, (x, y) in enumerate(zip(from_refs, to_refs))]
    for copy in copies:
        copy.start()
    copies[0].wait()
    copies[1].wait()
    fields, _, elems = initial_ref.shape
    for f in range(fields):
        own_ref[f] = padded(initial_ref[f], LANES, elems).T
    for k in range(metric_ref.shape[0]):
        own_ref[fields + k] = jnp.broadcast_to(metric_ref[k : k + 1, :], (LANES, elems)).T
    third = iota((elems, LANES), 1) // (LANES // 3)
    factors = jnp.where(third == 0, own_ref[fields], jnp.where(third == 1, own_ref[fields + 1], own_ref[fields + 2]))
    for edge_ref, rows in ((low_ref, slice(0, STEPS)), (high_ref, slice(elems - STEPS, elems))):
        for f in range(fields):
            edge_ref[f * STEPS : (f + 1) * STEPS, :] = own_ref[f, rows, :]
        edge_ref[fields * STEPS :, :] = factors[rows]
    odd = me_ref[0] % 2 == 1
    near_ref[...] = jnp.where(odd, low_ref[...], high_ref[...])
    far_ref[...] = jnp.where(odd, high_ref[...], low_ref[...])
    for copy in copies[2:]:
        copy.wait()


def turn(me, initial, metric, staged):
    fields, _, elems = initial.shape
    planes = fields + metric.shape[0]
    edge = jax.ShapeDtypeStruct(((fields + 1) * STEPS, LANES), F32)
    hbm = pl.BlockSpec(memory_space=pltpu.HBM)
    return pl.pallas_call(
        turn_kernel,
        in_specs=[pl.BlockSpec(memory_space=pltpu.SMEM)] + [hbm] * (2 + len(staged)),
        out_shape=(jax.ShapeDtypeStruct((planes, elems, LANES), F32), edge, edge)
        + tuple(jax.ShapeDtypeStruct(x.shape, x.dtype) for x in staged),
        scratch_shapes=[
            VMEM(initial.shape, F32),
            VMEM(metric.shape, F32),
            VMEM(edge.shape, F32),
            VMEM(edge.shape, F32),
            pltpu.SemaphoreType.DMA((2 + len(staged),)),
        ],
        compiler_params=pltpu.CompilerParams(vmem_limit_bytes=8 << 20),
        name="turn",
    )(me, *(pltpu.with_memory_space_constraint(x, pltpu.HBM) for x in (initial, metric, *staged)))


def operators_kernel(derivative_ref, coupling_ref, lift_ref, wt_ref, wl_ref, ck_ref):
    fields = coupling_ref.shape[1]
    dh, dl = zip(*(split2(padded(derivative_ref[k], LANES, LANES).T) for k in range(AXES)))
    zero = jnp.zeros((LANES, LANES), BF16)
    for row, (left, right) in enumerate(
        [(dh[0], dl[0]), (dh[1], dl[1]), (dh[2], dl[2]), (dh[2], zero), (dh[0], zero), (dh[1], zero)]
    ):
        wt_ref[row * LANES : (row + 1) * LANES, :] = jnp.concatenate([left, right], axis=1)
    l0h, l0l = split2(padded(lift_ref[0], LANES, LANES).T)
    l1h, l1l = split2(padded(lift_ref[1], LANES, LANES).T)
    for row, (left, right) in enumerate([(l0h, l1h), (l0h, l1h), (l0l, l1l)]):
        wl_ref[row * LANES : (row + 1) * LANES, :] = jnp.concatenate([left, right], axis=1)
    rows, cols = AXES * fields * GROUP, fields * GROUP
    spread_rows = (iota((rows, AXES * fields), 0) // GROUP == iota((rows, AXES * fields), 1)).astype(BF16)
    spread_cols = (iota((fields, cols), 0) == iota((fields, cols), 1) // GROUP).astype(BF16)
    by_row = pick(spread_rows, jnp.concatenate([coupling_ref[k] for k in range(AXES)], axis=0))
    hi, mid, lo = split3(by_row)
    full = dot(hi, spread_cols) + (dot(mid, spread_cols) + dot(lo, spread_cols))
    full = jnp.where(iota((rows, cols), 0) % GROUP == iota((rows, cols), 1) % GROUP, full, 0.0)
    full_hi = full.astype(BF16).astype(F32)
    ck_ref[...] = jnp.concatenate([full_hi, full_hi, full - full_hi], axis=1).astype(BF16)


def operators(derivative, coupling, face_lift):
    fields = coupling.shape[1]
    block = AXES * fields * GROUP
    return pl.pallas_call(
        operators_kernel,
        out_shape=(
            jax.ShapeDtypeStruct((6 * LANES, 2 * LANES), BF16),
            jax.ShapeDtypeStruct((3 * LANES, 2 * LANES), BF16),
            jax.ShapeDtypeStruct((block, 3 * fields * GROUP), BF16),
        ),
        compiler_params=pltpu.CompilerParams(vmem_limit_bytes=8 << 20),
        cost_estimate=pl.CostEstimate(flops=1_000_000_000, bytes_accessed=1_000_000, transcendentals=0),
        name="operators",
    )(derivative, coupling, face_lift)


class Order:
    def __init__(self, me, ins, outs, place_ref):
        self.me = me
        self.lives_ref, self.element_ref, self.weight_ref, self.order_ref, self.observed_ref = ins
        self.eh_ref, self.wp_ref, self.acc_ref, self.to_slot_ref, self.to_pos_ref, self.seen_ref = outs
        self.place_ref = place_ref
        self.width, self.slots = self.observed_ref.shape
        self.chips = self.slots // 4
        self.big = float(self.slots * self.slots)
        self.bits = self.slots.bit_length() - 1
        assert self.slots == 1 << self.bits
        self.odd = me & 1

    def pieces(self):
        yield from (functools.partial(self.slot_rows, other) for other in range(2))
        yield from (functools.partial(self.position_rows, other) for other in range(2))
        yield from (self.weights, self.observations, self.seen)

    def rows(self, other, which):
        start = (2 * other + which) * self.chips
        return slice(start, start + self.chips)

    def across(self, ref):
        return jnp.concatenate([ref[0:1, :], ref[1:2, :]], axis=1)

    def live_of(self, block):
        lives = self.lives_ref[...]
        there = block == iota((block.shape[0], lives.shape[1]), 1)
        return jnp.sum(jnp.where(there, lives.astype(F32), 0.0), axis=1, keepdims=True)

    def slot_rows(self, other):
        slots, chips = self.slots, self.chips
        first, last = None, None
        for half in range(2):
            core = [self.order_ref[pl.ds(2 * core + half, chips, stride=4), :] for core in range(2)]
            order = jnp.where(self.odd == 1 - other, core[1], core[0])
            key = (((half * LANES + iota(order.shape, 1)) << self.bits) + (order & (slots - 1))).astype(F32)
            mine = (order >> self.bits) == self.me
            low, high = jnp.where(mine, key, self.big), jnp.where(mine, key, -1.0)
            first = low if first is None else jnp.minimum(first, low)
            last = high if last is None else jnp.maximum(last, high)
        found = jnp.min(first, axis=1, keepdims=True), jnp.max(last, axis=1, keepdims=True)
        live_slot = iota((1, slots), 1).astype(F32) < self.live_of(jnp.full((1, 1), self.me, I32))
        element = self.across(self.element_ref).astype(F32)
        for which in range(2):
            rows = self.rows(other, which)
            hot = (found[which].astype(I32) & (slots - 1)) == iota((chips, slots), 1)
            self.to_slot_ref[rows, :] = jnp.where(hot & live_slot, 1.0, 0.0).astype(BF16)
            element_of = jnp.sum(jnp.where(hot, element, 0.0), axis=1, keepdims=True)
            hit = (element_of.astype(I32) == iota((chips, LANES), 1)).astype(BF16)
            self.eh_ref[rows, :] = jnp.concatenate([hit, hit], axis=1)

    def position_rows(self, other):
        slots, shape = self.slots, (self.chips, self.slots)
        mine = self.order_ref[pl.ds(2 * self.me, 2), :]
        mine = jnp.concatenate([mine[0:1], mine[1:2]], axis=1)
        block = 2 * iota((self.chips, 1), 0) + jnp.where(self.odd == 1 - other, 1, 0)
        col = iota(shape, 1).astype(F32)
        here = (mine >> self.bits) == block
        found = (
            jnp.min(jnp.where(here, col, self.big), axis=1, keepdims=True),
            jnp.max(jnp.where(here, col, -1.0), axis=1, keepdims=True),
        )
        live = self.live_of(block)
        slot = (mine & (slots - 1)).astype(F32)
        for which in range(2):
            rows = self.rows(other, which)
            hot = found[which] == col
            self.place_ref[rows, :] = hot.astype(BF16)
            slot_of = jnp.sum(jnp.where(hot, slot, 0.0), axis=1, keepdims=True)
            self.to_pos_ref[rows, :] = jnp.where(hot & (slot_of < live), 1.0, 0.0).astype(BF16)

    def weights(self):
        weight = padded(self.weight_ref[...], LANES, self.slots).T
        self.wp_ref[...] = pick(self.to_slot_ref[...], weight)

    def observations(self):
        lane, time = iota((LANES, self.width), 0) - OBS_LANE, iota((LANES, self.width), 1)
        comp = time // STEPS
        turned = (lane == comp * STEPS + (STEPS - 1 - (time - comp * STEPS))).astype(BF16)
        parts = [dot(turned, part).astype(BF16) for part in split3(self.observed_ref[...])]
        place = self.place_ref[...]
        out = [
            lax.dot_general(place, part, (((1,), (1,)), ((), ())), preferred_element_type=F32) for part in parts
        ]
        self.acc_ref[...] = out[0] + (out[1] + out[2])

    def seen(self):
        live = jnp.sum(self.to_pos_ref[...].astype(F32), axis=0, keepdims=True)
        self.seen_ref[...] = self.observed_ref[...] * live


class Stepper:
    def __init__(self, fields, load, store, factor, metric, wt_ref, wl_ref, ck_ref, t_ref, h_ref, lt_ref, lu_ref):
        self.fields, self.load, self.store, self.factor, self.metric = fields, load, store, factor, metric
        self.wt_ref, self.wl_ref, self.ck_ref = wt_ref, wl_ref, ck_ref
        self.t_ref, self.h_ref, self.lt_ref, self.lu_ref = t_ref, h_ref, lt_ref, lu_ref

    def split(self, item):
        halves = ([], [])
        for f in range(self.fields):
            x = jnp.concatenate([self.load(item.t, f, g) for g in item.groups], axis=0)
            hi, lo = split2(x)
            rows = slice(f * PAIR_ROWS, (f + 1) * PAIR_ROWS)
            self.lu_ref[item.slot, rows, :LANES] = hi
            self.lu_ref[item.slot, rows, LANES:] = lo
            hi32 = hi.astype(F32)
            lo32 = x - hi32
            for side in range(2):
                part = slice(side * GROUP, (side + 1) * GROUP)
                halves[side].append((hi32[part], lo32[part]))
        return halves

    def couple(self, item):
        columns = []
        for side in self.split(item):
            his, los = [p[0] for p in side], [p[1] for p in side]
            columns.append(jnp.concatenate(his + los + his, axis=0).astype(BF16))
        if item.lift_only:
            return
        v = dot(self.ck_ref[...], jnp.concatenate(columns, axis=1))
        for k in range(AXES):
            scale = [self.metric(k, g) for g in item.groups]
            parts = []
            for f in range(self.fields):
                base = (k * self.fields + f) * GROUP
                for side in range(2):
                    parts.append(v[base : base + GROUP, side * LANES : (side + 1) * LANES] * scale[side])
            for lane, part in zip(((0, 4), (1, 5), (2, 3))[k], split2(jnp.concatenate(parts, axis=0))):
                self.lt_ref[item.slot, :, lane * LANES : (lane + 1) * LANES] = part

    def apply(self, item):
        lu = self.lu_ref.at[item.slot]
        if not item.lift_only:
            both = dot(self.lt_ref[item.slot], self.wt_ref[...])
            both = both[:, :LANES] + both[:, LANES:]
        lifted = dot(lu[...], self.wl_ref[: 2 * LANES, :]) + dot(lu[:, :LANES], self.wl_ref[2 * LANES :, :])
        for f in range(self.fields):
            for side, g in enumerate(item.groups):
                rows = slice(f * PAIR_ROWS + side * GROUP, f * PAIR_ROWS + (side + 1) * GROUP)
                if not item.lift_only:
                    self.t_ref[f, g * GROUP : (g + 1) * GROUP, :] = both[rows]
                for face in range(2):
                    at = (g + 1) * GROUP
                    self.h_ref[face, f, at : at + GROUP, :] = lifted[rows, face * LANES : (face + 1) * LANES]

    def update(self, t, g):
        at = (g + 1) * GROUP
        here, before, after = slice(at, at + GROUP), slice(at - 1, at - 1 + GROUP), slice(at + 1, at + 1 + GROUP)
        for f in range(self.fields):
            low, high = self.h_ref.at[0, f], self.h_ref.at[1, f]
            lift = (low[before, :] - low[here, :]) + (high[after, :] - high[here, :])
            rate = self.t_ref[f, g * GROUP : (g + 1) * GROUP, :] + lift
            self.store(t, f, g, self.load(t, f, g) + self.factor(g) * rate)

    def run(self, items, ready, after=lambda index: None):
        ready = set(ready)
        product, lifted, done = set(), set(), set()
        wanted = {}
        for item in items:
            for g in item.groups:
                wanted.setdefault(item.t, {})[g] = item
        coupled = 0

        def couple_next(limit):
            nonlocal coupled
            while coupled < limit and all((items[coupled].t, g) in ready for g in items[coupled].groups):
                self.couple(items[coupled])
                coupled += 1

        for index, item in enumerate(items):
            couple_next(min(index + 2, len(items)))
            assert coupled > index
            self.apply(item)
            for g in item.groups:
                lifted.add((item.t, g))
                if not item.lift_only:
                    product.add((item.t, g))
            for t, groups in wanted.items():
                for g in groups:
                    if (t, g) in done or (t, g) not in product:
                        continue
                    if all(n not in groups or (t, n) in lifted for n in (g - 1, g + 1)):
                        self.update(t, g)
                        done.add((t, g))
                        ready.add((t + 1, g))
            after(index)


class Item:
    def __init__(self, t, slot, groups, lift_only=False):
        self.t, self.slot, self.groups, self.lift_only = t, slot, groups, lift_only


def own_pair(t, j):
    first = HALO // GROUP + 2 * j
    return Item(t, j, (first, first + 1))


def early_kernel(me_ref, own_ref, wt_ref, wl_ref, ck_ref, *refs):
    ins, past, outs = refs[:5], refs[5 : 5 + EARLY], refs[5 + EARLY : 11 + EARLY]
    t_ref, h_ref, lt_ref, lu_ref, place_ref = refs[11 + EARLY :]
    planes, elems, _ = own_ref.shape
    fields = planes - AXES
    shift = HALO // GROUP
    rows = lambda g: slice((g - shift) * GROUP, (g - shift + 1) * GROUP)

    def load(t, f, g):
        return own_ref[f, rows(g), :] if t == 0 else past[t - 1][f, rows(g), :]

    def store(t, f, g, value):
        past[t][f, rows(g), :] = value

    pad = slice(HALO, HALO + GROUP), slice(elems + HALO + GROUP, elems + HALO + 2 * GROUP)
    for rim in pad:
        h_ref[:, :, rim, :] = jnp.zeros((2, fields, GROUP, LANES), F32)
    stepper = Stepper(
        fields, load, store, lambda g: DT, lambda k, g: own_ref[fields + k, rows(g), :],
        wt_ref, wl_ref, ck_ref, t_ref, h_ref, lt_ref, lu_ref,
    )
    pairs = elems // PAIR_ROWS
    order = sorted(range(pairs), key=lambda j: abs(2 * j + 1 - pairs))
    items = [own_pair(t, j) for t in range(EARLY) for j in order]
    pieces = list(Order(me_ref[0], ins, outs, place_ref).pieces())
    at = {1 + (len(items) - 3) * i // len(pieces): piece for i, piece in enumerate(pieces)}
    stepper.run(
        items, {(0, g) for item in items for g in item.groups}, lambda index: at[index]() if index in at else None
    )


def scratch(fields, elems):
    rows = elems + 2 * HALO
    tile = fields * PAIR_ROWS
    slots = rows // PAIR_ROWS + 1
    return [
        VMEM((fields, rows, LANES), F32),
        VMEM((2, fields, rows + 2 * GROUP, LANES), F32),
        VMEM((slots, tile, 6 * LANES), BF16),
        VMEM((slots, tile, 2 * LANES), BF16),
    ]


def early(me, own, operators, ins):
    planes, elems, _ = own.shape
    fields = planes - AXES
    width, slots = ins[-1].shape
    smem = pl.BlockSpec(memory_space=pltpu.SMEM)
    vmem = pl.BlockSpec(memory_space=VMEM)
    return pl.pallas_call(
        early_kernel,
        in_specs=[smem] + [vmem] * (1 + len(operators) + len(ins)),
        out_shape=tuple(jax.ShapeDtypeStruct((fields, elems, LANES), F32) for _ in range(EARLY))
        + (
            jax.ShapeDtypeStruct((slots, 2 * LANES), BF16),
            jax.ShapeDtypeStruct((slots, LANES), F32),
            jax.ShapeDtypeStruct((slots, LANES), F32),
            jax.ShapeDtypeStruct((slots, slots), BF16),
            jax.ShapeDtypeStruct((slots, slots), BF16),
            jax.ShapeDtypeStruct((width, slots), F32),
        ),
        scratch_shapes=scratch(fields, elems) + [VMEM((slots, slots), BF16)],
        compiler_params=pltpu.CompilerParams(vmem_limit_bytes=32 << 20),
        cost_estimate=pl.CostEstimate(flops=5_000_000_000, bytes_accessed=4_000_000, transcendentals=0),
        name="early",
    )(me, own, *operators, *ins)


def march_kernel(me_ref, own_ref, near_ref, far_ref, *refs, last_block):
    past = (own_ref,) + refs[:EARLY]
    wt_ref, wl_ref, ck_ref, eh_ref, wp_ref, acc0_ref, keep_ref, give_ref, rev_ref = refs[EARLY : EARLY + 9]
    edge_ref, u_ref, m_ref, t_ref, h_ref, lt_ref, lu_ref = refs[EARLY + 9 :]
    planes, elems, _ = own_ref.shape
    fields = planes - AXES
    slots = eh_ref.shape[0]
    shift = HALO // GROUP
    groups = elems // GROUP + 2 * shift
    me = me_ref[0]
    dt_low = jnp.where(me == 0, 0.0, DT).astype(F32)
    dt_high = jnp.where(me == last_block, 0.0, DT).astype(F32)
    rim = list(range(shift + 1)) + list(range(groups - shift - 1, groups))
    own_rows = lambda g: slice((g - shift) * GROUP, (g - shift + 1) * GROUP)
    rim_rows = lambda g: slice(rim.index(g) * GROUP, (rim.index(g) + 1) * GROUP)
    all_rows = lambda g: slice(g * GROUP, (g + 1) * GROUP)

    odd = me % 2 == 1
    low_edge = lambda edge: jnp.where(odd, near_ref[edge], far_ref[edge])
    high_edge = lambda edge: jnp.where(odd, far_ref[edge], near_ref[edge])
    spare = jnp.zeros((HALO - STEPS, LANES), F32)
    low_rim, high_rim = slice(0, HALO), slice((shift + 2) * GROUP, (2 * shift + 2) * GROUP)
    for f in range(fields):
        edge = slice(f * STEPS, (f + 1) * STEPS)
        edge_ref[0, f, low_rim, :] = jnp.concatenate([spare, jnp.where(me > 0, low_edge(edge), 0.0)], axis=0)
        edge_ref[0, f, high_rim, :] = jnp.concatenate([jnp.where(me < last_block, high_edge(edge), 0.0), spare], axis=0)
    edge = slice(fields * STEPS, (fields + 1) * STEPS)
    low_factors, high_factors = low_edge(edge), high_edge(edge)
    for k in range(AXES):
        lane = k * (LANES // AXES)
        spread = lambda x: jnp.broadcast_to(x[:, lane : lane + 1], (STEPS, LANES))
        m_ref[k, :HALO, :] = jnp.concatenate([spare, spread(low_factors)], axis=0)
        m_ref[k, HALO:, :] = jnp.concatenate([spread(high_factors), spare], axis=0)
    h_ref[:, :, :GROUP, :] = jnp.zeros((2, fields, GROUP, LANES), F32)
    h_ref[:, :, (groups + 1) * GROUP :, :] = jnp.zeros((2, fields, GROUP, LANES), F32)
    half = slots // 2
    keep_ref[...] = acc0_ref[:half]
    give_ref[...] = acc0_ref[half:]
    rev_ref[...] = jnp.zeros(rev_ref.shape, F32)

    def load(t, f, g):
        if t > EARLY:
            return u_ref[t % 2, f, all_rows(g), :]
        if g in rim and not (t == 0 and shift <= g < groups - shift):
            return edge_ref[t, f, rim_rows(g), :]
        return past[t][f, own_rows(g), :]

    def store(t, f, g, value):
        if t >= EARLY:
            u_ref[(t + 1) % 2, f, all_rows(g), :] = value
            return
        row = iota((GROUP, LANES), 0)
        if g == shift:
            value = jnp.where(row <= t, value, past[t + 1][f, own_rows(g), :])
        if g == groups - shift - 1:
            value = jnp.where(row >= GROUP - 1 - t, value, past[t + 1][f, own_rows(g), :])
        edge_ref[t + 1, f, rim_rows(g), :] = value

    def metric(k, g):
        if g < shift:
            return m_ref[k, g * GROUP : (g + 1) * GROUP, :]
        if g >= groups - shift:
            at = HALO + (g - groups + shift) * GROUP
            return m_ref[k, at : at + GROUP, :]
        return own_ref[fields + k, own_rows(g), :]

    def factor(g):
        return dt_low if g < shift else (dt_high if g >= groups - shift else DT)

    def sample(t):
        field = lambda f: jnp.concatenate([load(t + 1, f, g) for g in range(shift, groups - shift)], axis=0)
        columns = []
        for c in range(COMPS):
            x = field(c) if c < 3 else (field(3) + field(4) + field(5)) / 3.0
            columns.append(jnp.concatenate(split2(x), axis=0))
        lane = iota((slots, LANES), 1)
        send = jnp.concatenate([keep_ref[...], give_ref[...]], axis=0)
        rev = rev_ref[...]
        for c in range(0, COMPS, 2):
            found = dot(eh_ref[...], jnp.concatenate(columns[c : c + 2], axis=1))
            for i in range(2):
                value = jnp.sum(found[:, i * LANES : (i + 1) * LANES] * wp_ref[...], axis=1, keepdims=True)
                send = jnp.where(lane == (c + i) * STEPS + t, value, send)
                rev = jnp.where(lane == OBS_LANE + (c + i) * STEPS + (STEPS - 1) - t, value, rev)
        keep_ref[...] = send[:half]
        give_ref[...] = send[half:]
        rev_ref[...] = rev

    pairs = elems // PAIR_ROWS
    order = sorted(range(pairs), key=lambda j: abs(2 * j + 1 - pairs))
    inner, outer = order[:-2], order[-2:]
    halo_pair = lambda t, ring, lift_only=False: Item(t, pairs + ring, (shift - 1 - ring, groups - shift + ring), lift_only)
    first_pair = lambda t: Item(t, pairs + shift, (shift, groups - shift - 1))
    items, samples = [], {}
    fill = -(-len(inner) // EARLY)
    for t in range(EARLY):
        items += [first_pair(t)] + [halo_pair(t, ring) for ring in range(shift)]
        items += [own_pair(EARLY, j) for j in inner[t * fill : (t + 1) * fill]]
        if t >= 1:
            samples[len(items) - 1] = t - 1
    for t in range(EARLY, STEPS):
        items += [own_pair(t, j) for j in (outer if t == EARLY else order)]
        if t > EARLY:
            samples[len(items) - len(order) + 3] = t - 1
        for ring in range(shift):
            if ring * GROUP < STEPS - t:
                items.append(halo_pair(t, ring, lift_only=ring * GROUP >= STEPS - 1 - t))
        if t == EARLY:
            samples[len(items) - 2] = EARLY - 1
    ready = {(0, g) for g in rim} | {(EARLY, g) for g in range(groups) if g not in rim}
    stepper = Stepper(
        fields, load, store, factor, metric, wt_ref, wl_ref, ck_ref, t_ref, h_ref, lt_ref, lu_ref
    )
    stepper.run(items, ready, lambda index: sample(samples[index]) if index in samples else None)
    sample(STEPS - 1)


def march(me, own, near, far, past, ops, last_block):
    eh = ops[3]
    planes, elems, _ = own.shape
    fields = planes - AXES
    slots = eh.shape[0]
    smem = pl.BlockSpec(memory_space=pltpu.SMEM)
    vmem = pl.BlockSpec(memory_space=VMEM)
    return pl.pallas_call(
        functools.partial(march_kernel, last_block=last_block),
        in_specs=[smem] + [vmem] * (3 + EARLY + len(ops)),
        out_shape=(
            jax.ShapeDtypeStruct((slots // 2, LANES), F32),
            jax.ShapeDtypeStruct((slots // 2, LANES), F32),
            jax.ShapeDtypeStruct((slots, LANES), F32),
        ),
        scratch_shapes=[
            VMEM((EARLY + 1, fields, 2 * (HALO + GROUP), LANES), F32),
            VMEM((2, fields, elems + 2 * HALO, LANES), F32),
            VMEM((AXES, 2 * HALO, LANES), F32),
        ]
        + scratch(fields, elems),
        compiler_params=pltpu.CompilerParams(vmem_limit_bytes=40 << 20),
        cost_estimate=pl.CostEstimate(flops=20_000_000_000, bytes_accessed=4_000_000, transcendentals=0),
        name="march",
    )(me, own, near, far, *past, *ops)


def pack_kernel(keep_ref, given_ref, out_ref):
    chips = keep_ref.shape[0] // 2
    for other, ref in enumerate((keep_ref, given_ref)):
        for which in range(2):
            out_ref[pl.ds(2 * other + which, chips, stride=4), :] = ref[which * chips : (which + 1) * chips, :]


def pack(keep, given):
    return pl.pallas_call(
        pack_kernel,
        out_shape=jax.ShapeDtypeStruct((2 * keep.shape[0], LANES), F32),
        compiler_params=pltpu.CompilerParams(vmem_limit_bytes=4 << 20),
        name="pack",
    )(keep, given)


def finish_kernel(
    got_ref, rev_ref, to_slot_ref, to_pos_ref, seen_ref, res_hbm, mis_hbm, adj_hbm, res_ref, mis_ref, adj_ref, sems
):
    width, slots = seen_ref.shape
    chips = slots // 4
    got = jnp.concatenate([got_ref[pl.ds(i, chips, stride=4), :] for i in range(4)], axis=0)
    lane = iota(got.shape, 1)
    turned = jnp.where(lane < OBS_LANE, got, rev_ref[...] - got).T

    def place(rows, onehot):
        found = dot(jnp.concatenate(split3(rows), axis=0), onehot)
        return found[:width] + (found[width : 2 * width] + found[2 * width :])

    residual = place(turned[:width], to_pos_ref[...]) - seen_ref[...]
    res_ref[...] = residual
    first = pltpu.make_async_copy(res_ref, res_hbm, sems.at[0])
    first.start()
    mis_ref[...] = 0.5 * jnp.sum(residual * residual, axis=0, keepdims=True)
    second = pltpu.make_async_copy(mis_ref, mis_hbm, sems.at[1])
    second.start()
    adj_ref[...] = place(turned[OBS_LANE : OBS_LANE + width], to_slot_ref[...])
    third = pltpu.make_async_copy(adj_ref, adj_hbm, sems.at[2])
    third.start()
    first.wait()
    second.wait()
    third.wait()


def finish(got, rev, to_slot, to_pos, seen):
    width, slots = seen.shape
    vmem = pl.BlockSpec(memory_space=VMEM)
    hbm = pl.BlockSpec(memory_space=pltpu.HBM)
    shapes = ((width, slots), (1, slots), (width, slots))
    return pl.pallas_call(
        finish_kernel,
        in_specs=[vmem] * 5,
        out_specs=(hbm, hbm, hbm),
        out_shape=tuple(jax.ShapeDtypeStruct(shape, F32) for shape in shapes),
        scratch_shapes=[VMEM(shape, F32) for shape in shapes] + [pltpu.SemaphoreType.DMA((3,))],
        compiler_params=pltpu.CompilerParams(vmem_limit_bytes=8 << 20),
        name="finish",
    )(got, rev, to_slot, to_pos, seen)


def shards(
    initial,
    derivative,
    coupling,
    face_lift,
    metric,
    rec_element,
    rec_weight,
    live_counts,
    shot_order,
    observed,
):
    blocks = lax.axis_size(MX)
    slots = rec_element.shape[0]
    me = lax.axis_index(MX).astype(I32).reshape(1)
    order, element, lives = (x.reshape(-1, LANES) for x in (shot_order, rec_element, live_counts))
    staged = (derivative, rec_weight, order, element, lives, observed.T)
    own, near, far, derivative, rec_weight, order, element, lives, observed = turn(me, initial, metric, staged)
    pairs = [(i, min(i + 1, blocks - 1) if i % 2 else max(i - 1, 0)) for i in range(blocks)]
    far = lax.ppermute(far, MX, pairs)
    near = lax.ppermute(near, MX, [(i, i ^ 1) for i in range(blocks)])
    ops = operators(derivative, coupling, face_lift)
    outs = early(me, own, ops, (lives, element, rec_weight, order, observed))
    past, eh, wp, acc0, to_slot, to_pos, seen = (outs[:EARLY],) + tuple(outs[EARLY:])
    keep, give, rev = march(me, own, near, far, past, (*ops, eh, wp, acc0), blocks - 1)
    given = lax.ppermute(give, MX, [(i, i ^ 1) for i in range(blocks)])
    rows = pack(keep, given).reshape(blocks // 2, 4, LANES)
    got = lax.all_to_all(rows, MX[:2], split_axis=0, concat_axis=0, tiled=True)
    residual, misfit, adjoint = finish(got.reshape(slots, LANES), rev, to_slot, to_pos, seen)
    return (residual.T, misfit.reshape(slots), adjoint.T)


def solution(mesh):
    split = Mesh(
        mesh.devices.reshape(mesh.shape["shots"], 8, 8, 2), ("shots", "mx_0", "mx_1", "mx_2")
    )
    in_specs = (
        P("shots", None, MX),
        P(),
        P(),
        P(),
        P(None, MX),
        P(MX),
        P(None, MX),
        P(),
        P(),
        P(SHOTS_MX, None),
    )
    out_specs = (P(SHOTS_MX, None), P(SHOTS_MX), P(SHOTS_MX, None))
    return jax.shard_map(
        shards, mesh=split, in_specs=in_specs, out_specs=out_specs, check_vma=False
    )
```

```python
import functools

import jax
import jax.numpy as jnp
from jax import lax
from jax.experimental import pallas as pl
from jax.experimental.pallas import tpu as pltpu
from jax.sharding import Mesh
from jax.sharding import PartitionSpec as P


STEPS = 12
EARLY = 3
DT = 0.5 / STEPS
AXES = 3
COMPS = 4
MX = ("mx_0", "mx_1", "mx_2")
SHOTS_MX = ("shots", "mx_0", "mx_1", "mx_2")
F32 = jnp.float32
BF16 = jnp.bfloat16
I32 = jnp.int32
LANES = 128
GROUP = 8
PAIR_ROWS = 2 * GROUP
HALO = 16
OBS_LANE = 64
VMEM = pltpu.VMEM


def iota(shape, dim):
    return lax.broadcasted_iota(I32, shape, dim)


def split2(x):
    hi = x.astype(BF16)
    return hi, (x - hi.astype(F32)).astype(BF16)


def dot(a, b):
    return jnp.dot(a, b, preferred_element_type=F32)


def pick(onehot, x):
    both = dot(onehot, jnp.concatenate(split2(x), axis=1))
    return both[:, : x.shape[1]] + both[:, x.shape[1] :]


def padded(x, rows, cols):
    if x.shape[1] < cols:
        x = jnp.concatenate([x, jnp.zeros((x.shape[0], cols - x.shape[1]), x.dtype)], axis=1)
    if x.shape[0] < rows:
        x = jnp.concatenate([x, jnp.zeros((rows - x.shape[0], cols), x.dtype)], axis=0)
    return x


def turn_kernel(me_ref, *refs):
    staged = (len(refs) - 10) // 2
    initial_hbm, metric_hbm = refs[:2]
    from_refs = refs[2 : 2 + staged]
    own_ref, near_ref, far_ref = refs[2 + staged : 5 + staged]
    to_refs = refs[5 + staged : 5 + 2 * staged]
    initial_ref, metric_ref, low_ref, high_ref, sems = refs[-5:]
    fields, _, elems = initial_ref.shape
    pairs = [(initial_hbm, initial_ref), (metric_hbm, metric_ref)] + list(zip(from_refs, to_refs))
    copies = [pltpu.make_async_copy(x, y, sems.at[i]) for i, (x, y) in enumerate(pairs)]
    for copy in copies:
        copy.start()
    copies[0].wait()
    copies[1].wait()
    for f in range(fields):
        own_ref[f] = padded(initial_ref[f], LANES, elems).T
    for k in range(metric_ref.shape[0]):
        own_ref[fields + k] = jnp.broadcast_to(metric_ref[k : k + 1, :], (LANES, elems)).T
    third = iota((elems, LANES), 1) // (LANES // 3)
    factors = jnp.where(third == 0, own_ref[fields], jnp.where(third == 1, own_ref[fields + 1], own_ref[fields + 2]))
    for edge_ref, rows in ((low_ref, slice(0, STEPS)), (high_ref, slice(elems - STEPS, elems))):
        for f in range(fields):
            edge_ref[f * STEPS : (f + 1) * STEPS, :] = own_ref[f, rows, :]
        edge_ref[fields * STEPS :, :] = factors[rows]
    odd = me_ref[0] % 2 == 1
    near_ref[...] = jnp.where(odd, low_ref[...], high_ref[...])
    far_ref[...] = jnp.where(odd, high_ref[...], low_ref[...])
    for copy in copies[2:]:
        copy.wait()


def turn(me, initial, metric, staged):
    fields, _, elems = initial.shape
    planes = fields + metric.shape[0]
    edge = jax.ShapeDtypeStruct(((fields + 1) * STEPS, LANES), F32)
    hbm = pl.BlockSpec(memory_space=pltpu.HBM)
    return pl.pallas_call(
        turn_kernel,
        in_specs=[pl.BlockSpec(memory_space=pltpu.SMEM)] + [hbm] * (2 + len(staged)),
        out_shape=(jax.ShapeDtypeStruct((planes, elems, LANES), F32), edge, edge)
        + tuple(jax.ShapeDtypeStruct(x.shape, x.dtype) for x in staged),
        scratch_shapes=[
            VMEM(initial.shape, F32),
            VMEM(metric.shape, F32),
            VMEM(edge.shape, F32),
            VMEM(edge.shape, F32),
            pltpu.SemaphoreType.DMA((2 + len(staged),)),
        ],
        compiler_params=pltpu.CompilerParams(vmem_limit_bytes=8 << 20),
        name="turn",
    )(me, *(pltpu.with_memory_space_constraint(x, pltpu.HBM) for x in (initial, metric, *staged)))


def operators_kernel(derivative_ref, coupling_ref, lift_ref, wt_ref, wl_ref, ck_ref):
    fields = coupling_ref.shape[1]
    dh, dl = zip(*(split2(padded(DT * derivative_ref[k], LANES, LANES).T) for k in range(AXES)))
    zero = jnp.zeros((LANES, LANES), BF16)
    for row, (left, right) in enumerate(
        [(dh[0], dl[0]), (dh[1], dl[1]), (dh[2], dl[2]), (dh[2], zero), (dh[0], zero), (dh[1], zero)]
    ):
        wt_ref[row * LANES : (row + 1) * LANES, :] = jnp.concatenate([left, right], axis=1)
    l0h, l0l = split2(padded(DT * lift_ref[0], LANES, LANES).T)
    l1h, l1l = split2(padded(DT * lift_ref[1], LANES, LANES).T)
    for row, (left, right) in enumerate([(l0h, l1h), (l0h, l1h), (l0l, l1l)]):
        wl_ref[row * LANES : (row + 1) * LANES, :] = jnp.concatenate([left, right], axis=1)
    rows, cols = AXES * fields * GROUP, fields * GROUP
    spread_rows = (iota((rows, AXES * fields), 0) // GROUP == iota((rows, AXES * fields), 1)).astype(BF16)
    spread_cols = (iota((fields, cols), 0) == iota((fields, cols), 1) // GROUP).astype(BF16)
    hi, lo = split2(jnp.concatenate([coupling_ref[k] for k in range(AXES)], axis=0))
    full = dot(dot(spread_rows, hi).astype(BF16), spread_cols) + dot(dot(spread_rows, lo).astype(BF16), spread_cols)
    full = jnp.where(iota((rows, cols), 0) % GROUP == iota((rows, cols), 1) % GROUP, full, 0.0)
    full_hi = full.astype(BF16).astype(F32)
    ck_ref[...] = jnp.concatenate([full_hi, full_hi, full - full_hi], axis=1).astype(BF16)


def operators(derivative, coupling, face_lift):
    fields = coupling.shape[1]
    block = AXES * fields * GROUP
    return pl.pallas_call(
        operators_kernel,
        out_shape=(
            jax.ShapeDtypeStruct((6 * LANES, 2 * LANES), BF16),
            jax.ShapeDtypeStruct((3 * LANES, 2 * LANES), BF16),
            jax.ShapeDtypeStruct((block, 3 * fields * GROUP), BF16),
        ),
        compiler_params=pltpu.CompilerParams(vmem_limit_bytes=8 << 20),
        cost_estimate=pl.CostEstimate(flops=1_000_000_000, bytes_accessed=1_000_000, transcendentals=0),
        name="operators",
    )(derivative, coupling, face_lift)


class Order:
    def __init__(self, me, ins, outs, place_ref):
        self.me = me
        self.lives_ref, self.element_ref, self.weight_ref, self.order_ref, self.observed_ref = ins
        self.eh_ref, self.wp_ref, self.acc_ref, self.to_slot_ref, self.to_pos_ref, self.seen_ref = outs
        self.place_ref = place_ref
        self.width, self.slots = self.observed_ref.shape
        self.chips = self.slots // 4
        self.big = float(self.slots * self.slots)
        self.bits = self.slots.bit_length() - 1
        assert self.slots == 1 << self.bits
        self.odd = me & 1

    def pieces(self):
        yield from (functools.partial(self.slot_rows, other) for other in range(2))
        yield from (functools.partial(self.position_rows, other) for other in range(2))
        yield from (self.weights, self.observations, self.seen)

    def rows(self, other, which):
        start = (2 * other + which) * self.chips
        return slice(start, start + self.chips)

    def across(self, ref):
        return jnp.concatenate([ref[0:1, :], ref[1:2, :]], axis=1)

    def live_of(self, block):
        lives = self.lives_ref[...]
        there = block == iota((block.shape[0], lives.shape[1]), 1)
        return jnp.sum(jnp.where(there, lives.astype(F32), 0.0), axis=1, keepdims=True)

    def slot_rows(self, other):
        slots, chips = self.slots, self.chips
        first, last = None, None
        for half in range(2):
            core = [self.order_ref[pl.ds(2 * core + half, chips, stride=4), :] for core in range(2)]
            order = jnp.where(self.odd == 1 - other, core[1], core[0])
            key = (((half * LANES + iota(order.shape, 1)) << self.bits) + (order & (slots - 1))).astype(F32)
            mine = (order >> self.bits) == self.me
            low, high = jnp.where(mine, key, self.big), jnp.where(mine, key, -1.0)
            first = low if first is None else jnp.minimum(first, low)
            last = high if last is None else jnp.maximum(last, high)
        found = jnp.min(first, axis=1, keepdims=True), jnp.max(last, axis=1, keepdims=True)
        live_slot = iota((1, slots), 1).astype(F32) < self.live_of(jnp.full((1, 1), self.me, I32))
        element = self.across(self.element_ref).astype(F32)
        for which in range(2):
            rows = self.rows(other, which)
            hot = (found[which].astype(I32) & (slots - 1)) == iota((chips, slots), 1)
            self.to_slot_ref[rows, :] = jnp.where(hot & live_slot, 1.0, 0.0).astype(BF16)
            element_of = jnp.sum(jnp.where(hot, element, 0.0), axis=1, keepdims=True)
            hit = (element_of.astype(I32) == iota((chips, LANES), 1)).astype(BF16)
            self.eh_ref[rows, :] = jnp.concatenate([hit, hit], axis=1)

    def position_rows(self, other):
        slots, shape = self.slots, (self.chips, self.slots)
        mine = self.order_ref[pl.ds(2 * self.me, 2), :]
        mine = jnp.concatenate([mine[0:1], mine[1:2]], axis=1)
        block = 2 * iota((self.chips, 1), 0) + jnp.where(self.odd == 1 - other, 1, 0)
        col = iota(shape, 1).astype(F32)
        here = (mine >> self.bits) == block
        found = (
            jnp.min(jnp.where(here, col, self.big), axis=1, keepdims=True),
            jnp.max(jnp.where(here, col, -1.0), axis=1, keepdims=True),
        )
        live = self.live_of(block)
        slot = (mine & (slots - 1)).astype(F32)
        for which in range(2):
            rows = self.rows(other, which)
            hot = found[which] == col
            self.place_ref[rows, :] = hot.astype(BF16)
            slot_of = jnp.sum(jnp.where(hot, slot, 0.0), axis=1, keepdims=True)
            self.to_pos_ref[rows, :] = jnp.where(hot & (slot_of < live), 1.0, 0.0).astype(BF16)

    def weights(self):
        weight = padded(self.weight_ref[...], LANES, self.slots).T
        self.wp_ref[...] = pick(self.to_slot_ref[...], weight)

    def observations(self):
        lane, time = iota((LANES, self.width), 0) - OBS_LANE, iota((LANES, self.width), 1)
        comp = time // STEPS
        turned = (lane == comp * STEPS + (STEPS - 1 - (time - comp * STEPS))).astype(BF16)
        parts = jnp.concatenate([dot(turned, part) for part in split2(self.observed_ref[...])], axis=0).astype(BF16)
        both = lax.dot_general(self.place_ref[...], parts, (((1,), (1,)), ((), ())), preferred_element_type=F32)
        self.acc_ref[...] = both[:, :LANES] + both[:, LANES:]

    def seen(self):
        live = jnp.sum(self.to_pos_ref[...].astype(F32), axis=0, keepdims=True)
        self.seen_ref[...] = self.observed_ref[...] * live


class Stepper:
    def __init__(self, fields, load, store, factor, metric, wt_ref, wl_ref, ck_ref, t_ref, h_ref, lt_ref, lu_ref):
        self.fields, self.load, self.store, self.factor, self.metric = fields, load, store, factor, metric
        self.wt_ref, self.wl_ref, self.ck_ref = wt_ref, wl_ref, ck_ref
        self.t_ref, self.h_ref, self.lt_ref, self.lu_ref = t_ref, h_ref, lt_ref, lu_ref

    def split(self, item):
        halves = ([], [])
        for f in range(self.fields):
            x = jnp.concatenate([self.load(item.t, f, g) for g in item.groups], axis=0)
            hi, lo = split2(x)
            rows = slice(f * PAIR_ROWS, (f + 1) * PAIR_ROWS)
            self.lu_ref[item.slot, rows, :LANES] = hi
            self.lu_ref[item.slot, rows, LANES:] = lo
            hi32 = hi.astype(F32)
            lo32 = x - hi32
            for side in range(2):
                part = slice(side * GROUP, (side + 1) * GROUP)
                halves[side].append((hi32[part], lo32[part]))
        return halves

    def couple(self, item):
        columns = []
        for side in self.split(item):
            his, los = [p[0] for p in side], [p[1] for p in side]
            columns.append(jnp.concatenate(his + los + his, axis=0).astype(BF16))
        if item.lift_only:
            return
        size = 3 * self.fields * GROUP
        v = dot(self.ck_ref[:size, :size], jnp.concatenate(columns, axis=1))
        for k in range(AXES):
            scale = [self.metric(k, g) for g in item.groups]
            parts = []
            for f in range(self.fields):
                base = (k * self.fields + f) * GROUP
                for side in range(2):
                    parts.append(v[base : base + GROUP, side * LANES : (side + 1) * LANES] * scale[side])
            for lane, part in zip(((0, 4), (1, 5), (2, 3))[k], split2(jnp.concatenate(parts, axis=0))):
                self.lt_ref[item.slot, :, lane * LANES : (lane + 1) * LANES] = part

    def apply(self, item):
        lu = self.lu_ref.at[item.slot]
        if not item.lift_only:
            both = dot(self.lt_ref[item.slot], self.wt_ref[...])
            both = both[:, :LANES] + both[:, LANES:]
        lifted = dot(lu[...], self.wl_ref[: 2 * LANES, :]) + dot(lu[:, :LANES], self.wl_ref[2 * LANES :, :])
        for f in range(self.fields):
            for side, g in enumerate(item.groups):
                rows = slice(f * PAIR_ROWS + side * GROUP, f * PAIR_ROWS + (side + 1) * GROUP)
                if not item.lift_only:
                    self.t_ref[f, g : g + GROUP, :] = both[rows]
                for face in range(2):
                    at = g + GROUP
                    self.h_ref[face, f, at : at + GROUP, :] = lifted[rows, face * LANES : (face + 1) * LANES]

    def update(self, t, g):
        at = g + GROUP
        here, before, after = slice(at, at + GROUP), slice(at - 1, at - 1 + GROUP), slice(at + 1, at + 1 + GROUP)
        for f in range(self.fields):
            low, high = self.h_ref.at[0, f], self.h_ref.at[1, f]
            lift = (low[before, :] - low[here, :]) + (high[after, :] - high[here, :])
            change = self.t_ref[f, g : g + GROUP, :] + lift
            if self.factor(g) is not None:
                change = self.factor(g) * change
            self.store(t, f, g, self.load(t, f, g) + change)

    def run(self, items, ready, after=lambda index: None, mended=(set(), set())):
        ready = set(ready)
        product, lifted, done = set(), set(), set()
        wanted = {}
        for item in items:
            for g in item.groups:
                wanted.setdefault(item.t, {})[g] = item
        coupled = 0

        def couple_next(limit):
            nonlocal coupled
            while coupled < limit and all((items[coupled].t, g) in ready for g in items[coupled].groups):
                self.couple(items[coupled])
                coupled += 1

        for index, item in enumerate(items):
            couple_next(min(index + 2, len(items)))
            assert coupled > index
            self.apply(item)
            for g in item.groups:
                lifted.add((item.t, g))
                if not item.lift_only:
                    product.add((item.t, g))
            for t, groups in wanted.items():
                for g in groups:
                    if (t, g) in done or (t, g) not in product:
                        continue
                    if all(n not in groups or (t, n) in lifted for n in (g - GROUP, g + GROUP)):
                        self.update(t, g)
                        done.add((t, g))
                        ready.add((t + 1, g))
            if mended[1] <= ready:
                ready |= mended[0]
            after(index)


class Item:
    def __init__(self, t, slot, groups, lift_only=False):
        self.t, self.slot, self.groups, self.lift_only = t, slot, groups, lift_only


def own_pair(t, j):
    first = HALO + PAIR_ROWS * j
    return Item(t, j, (first, first + GROUP))


def hold(refs, local):
    for ref, to in zip(refs, local):
        rows, cols = ref.shape
        to[:rows, :cols] = ref[...]
    return local


def early_kernel(me_ref, own_ref, wt_ref, wl_ref, ck_ref, *refs):
    ins, past, outs = refs[:5], refs[5 : 5 + EARLY], refs[5 + EARLY : 11 + EARLY]
    t_ref, h_ref, lt_ref, lu_ref, *local, place_ref = refs[11 + EARLY :]
    wt_ref, wl_ref, ck_ref = hold((wt_ref, wl_ref, ck_ref), local)
    planes, elems, _ = own_ref.shape
    fields = planes - AXES
    rows = lambda g: slice(g - HALO, g - HALO + GROUP)

    def load(t, f, g):
        return own_ref[f, rows(g), :] if t == 0 else past[t - 1][f, rows(g), :]

    def store(t, f, g, value):
        past[t][f, rows(g), :] = value

    pad = slice(HALO, HALO + GROUP), slice(elems + HALO + GROUP, elems + HALO + 2 * GROUP)
    for rim in pad:
        h_ref[:, :, rim, :] = jnp.zeros((2, fields, GROUP, LANES), F32)
    stepper = Stepper(
        fields, load, store, lambda g: None, lambda k, g: own_ref[fields + k, rows(g), :],
        wt_ref, wl_ref, ck_ref, t_ref, h_ref, lt_ref, lu_ref,
    )
    pairs = elems // PAIR_ROWS
    order = sorted(range(pairs), key=lambda j: abs(2 * j + 1 - pairs))
    items = [own_pair(t, j) for t in range(EARLY) for j in order]
    pieces = list(Order(me_ref[0], ins, outs, place_ref).pieces())
    at = {1 + (len(items) - 3) * i // len(pieces): piece for i, piece in enumerate(pieces)}
    stepper.run(
        items, {(0, g) for item in items for g in item.groups}, lambda index: at[index]() if index in at else None
    )


def scratch(fields, elems):
    rows = elems + 2 * HALO
    tile = fields * PAIR_ROWS
    slots = rows // PAIR_ROWS + 2
    return [
        VMEM((fields, rows, LANES), F32),
        VMEM((2, fields, rows + 2 * GROUP, LANES), F32),
        VMEM((slots, tile, 6 * LANES), BF16),
        VMEM((slots, tile, 2 * LANES), BF16),
        VMEM((6 * LANES, 2 * LANES), BF16),
        VMEM((3 * LANES, 2 * LANES), BF16),
        VMEM((2 * LANES, 2 * LANES), BF16),
    ]


def early(me, own, operators, ins):
    planes, elems, _ = own.shape
    fields = planes - AXES
    width, slots = ins[-1].shape
    smem = pl.BlockSpec(memory_space=pltpu.SMEM)
    vmem = pl.BlockSpec(memory_space=VMEM)
    return pl.pallas_call(
        early_kernel,
        in_specs=[smem] + [vmem] * (1 + len(operators) + len(ins)),
        out_shape=tuple(jax.ShapeDtypeStruct((fields, elems, LANES), F32) for _ in range(EARLY))
        + (
            jax.ShapeDtypeStruct((slots, 2 * LANES), BF16),
            jax.ShapeDtypeStruct((slots, LANES), F32),
            jax.ShapeDtypeStruct((slots, LANES), F32),
            jax.ShapeDtypeStruct((slots, slots), BF16),
            jax.ShapeDtypeStruct((slots, slots), BF16),
            jax.ShapeDtypeStruct((width, slots), F32),
        ),
        scratch_shapes=scratch(fields, elems) + [VMEM((slots, slots), BF16)],
        compiler_params=pltpu.CompilerParams(vmem_limit_bytes=32 << 20),
        cost_estimate=pl.CostEstimate(flops=5_000_000_000, bytes_accessed=4_000_000, transcendentals=0),
        name="early",
    )(me, own, *operators, *ins)


def march_kernel(me_ref, own_ref, near_ref, far_ref, *refs, last_block):
    past = (own_ref,) + refs[:EARLY]
    wt_ref, wl_ref, ck_ref, eh_ref, wp_ref, acc0_ref, keep_ref, give_ref, rev_ref = refs[EARLY : EARLY + 9]
    edge_ref, u_ref, m_ref, t_ref, h_ref, lt_ref, lu_ref, *local = refs[EARLY + 9 :]
    wt_ref, wl_ref, ck_ref = hold((wt_ref, wl_ref, ck_ref), local)
    planes, elems, _ = own_ref.shape
    fields = planes - AXES
    slots = eh_ref.shape[0]
    end = HALO + elems
    me = me_ref[0]
    in_low = jnp.where(me == 0, 0.0, 1.0).astype(F32)
    in_high = jnp.where(me == last_block, 0.0, 1.0).astype(F32)
    skip = HALO - STEPS
    side_rows = HALO + GROUP
    low_rim, high_rim = [skip, skip + GROUP], [end - skip, end - skip + GROUP]
    low_groups, high_groups = list(range(0, side_rows, GROUP)), list(range(end - GROUP, end + HALO, GROUP))
    own_rows = lambda g: slice(g - HALO, g - HALO + GROUP)

    def rim_rows(g):
        at = g if g < HALO + GROUP else side_rows + g - (end - GROUP)
        return slice(at, at + GROUP)

    odd = me % 2 == 1
    low_edge = lambda edge: jnp.where(odd, near_ref[edge], far_ref[edge])
    high_edge = lambda edge: jnp.where(odd, far_ref[edge], near_ref[edge])
    spare = jnp.zeros((skip, LANES), F32)
    for f in range(fields):
        edge = slice(f * STEPS, (f + 1) * STEPS)
        low = jnp.where(me > 0, low_edge(edge), 0.0)
        high = jnp.where(me < last_block, high_edge(edge), 0.0)
        edge_ref[0, f, :side_rows, :] = jnp.concatenate([spare, low, own_ref[f, :GROUP, :]], axis=0)
        edge_ref[0, f, side_rows:, :] = jnp.concatenate([own_ref[f, elems - GROUP :, :], high, spare], axis=0)
    edge_ref[EARLY] = jnp.zeros(edge_ref.shape[1:], F32)
    edge = slice(fields * STEPS, (fields + 1) * STEPS)
    low_factors, high_factors = low_edge(edge), high_edge(edge)
    for k in range(AXES):
        lane = k * (LANES // AXES)
        spread = lambda x: jnp.broadcast_to(x[:, lane : lane + 1], (STEPS, LANES))
        own_low, own_high = own_ref[fields + k, :GROUP, :], own_ref[fields + k, elems - GROUP :, :]
        m_ref[k, :side_rows, :] = jnp.concatenate([spare, spread(low_factors), own_low], axis=0)
        m_ref[k, side_rows:, :] = jnp.concatenate([own_high, spread(high_factors), spare], axis=0)
    h_ref[:, :, :PAIR_ROWS, :] = jnp.zeros((2, fields, PAIR_ROWS, LANES), F32)
    h_ref[:, :, end + GROUP + HALO - GROUP :, :] = jnp.zeros((2, fields, PAIR_ROWS, LANES), F32)
    half = slots // 2
    keep_ref[...] = acc0_ref[:half]
    give_ref[...] = acc0_ref[half:]
    rev_ref[...] = jnp.zeros(rev_ref.shape, F32)

    def load(t, f, g):
        if t > EARLY:
            return u_ref[t % 2, f, g : g + GROUP, :]
        if t == EARLY and g in low_groups + high_groups or g in low_rim + high_rim:
            return edge_ref[t, f, rim_rows(g), :]
        return past[t][f, own_rows(g), :]

    def store(t, f, g, value):
        if t >= EARLY:
            u_ref[(t + 1) % 2, f, g : g + GROUP, :] = value
            return
        row = iota((GROUP, LANES), 0)
        if g == low_rim[1]:
            rest = past[t + 1][f, : GROUP - skip, :]
            value = jnp.where(row <= skip + t, value, jnp.concatenate([rest[:skip], rest], axis=0))
            if t == EARLY - 1:
                edge_ref[EARLY, f, side_rows - skip : side_rows, :] = past[t + 1][f, GROUP - skip : GROUP, :]
        if g == high_rim[0]:
            rest = past[t + 1][f, elems - (GROUP - skip) :, :]
            value = jnp.where(row >= GROUP - skip - 1 - t, value, jnp.concatenate([rest, rest[:skip]], axis=0))
            if t == EARLY - 1:
                at = elems - GROUP
                edge_ref[EARLY, f, side_rows : side_rows + skip, :] = past[t + 1][f, at : at + skip, :]
        edge_ref[t + 1, f, rim_rows(g), :] = value

    def metric(k, g):
        if g < HALO or g > end - GROUP:
            return m_ref[k, rim_rows(g), :]
        return own_ref[fields + k, own_rows(g), :]

    def factor(g):
        if g + GROUP <= HALO:
            return in_low
        if g >= end:
            return in_high
        if g < HALO:
            return jnp.where(iota((GROUP, LANES), 0) < HALO - g, in_low, 1.0)
        if g + GROUP > end:
            return jnp.where(iota((GROUP, LANES), 0) >= end - g, in_high, 1.0)
        return None

    def own_load(t, f, g):
        if t < EARLY and g in (HALO, end - GROUP):
            rest, row = past[t][f, own_rows(g), :], iota((GROUP, LANES), 0)
            mended = edge_ref[t, f, rim_rows(g), :]
            return jnp.where(row < t, mended, rest) if g == HALO else jnp.where(row >= GROUP - t, mended, rest)
        return load(t, f, g)

    def sample(t):
        field = lambda f: jnp.concatenate([own_load(t + 1, f, g) for g in range(HALO, end, GROUP)], axis=0)
        columns = []
        for c in range(COMPS):
            x = field(c) if c < 3 else (field(3) + field(4) + field(5)) / 3.0
            columns.append(jnp.concatenate(split2(x), axis=0))
        lane = iota((slots, LANES), 1)
        send = jnp.concatenate([keep_ref[...], give_ref[...]], axis=0)
        rev = rev_ref[...]
        for c in range(0, COMPS, 2):
            found = dot(eh_ref[...], jnp.concatenate(columns[c : c + 2], axis=1))
            for i in range(2):
                value = jnp.sum(found[:, i * LANES : (i + 1) * LANES] * wp_ref[...], axis=1, keepdims=True)
                send = jnp.where(lane == (c + i) * STEPS + t, value, send)
                rev = jnp.where(lane == OBS_LANE + (c + i) * STEPS + (STEPS - 1) - t, value, rev)
        keep_ref[...] = send[:half]
        give_ref[...] = send[half:]
        rev_ref[...] = rev

    pairs = elems // PAIR_ROWS
    order = sorted(range(pairs), key=lambda j: abs(2 * j + 1 - pairs))
    inner, outer = order[:-2], order[-2:]
    ring_rows = lambda ring: (HALO - GROUP * (ring + 1), end + GROUP * ring)
    items, samples = [], {}
    fill = -(-len(inner) // EARLY)
    for t in range(EARLY):
        items += [Item(t, pairs, (low_rim[1], high_rim[0])), Item(t, pairs + 1, (low_rim[0], high_rim[1]))]
        items += [own_pair(EARLY, j) for j in inner[t * fill : (t + 1) * fill]]
        if t >= 1:
            samples[len(items) - 1] = t - 1
    for t in range(EARLY, STEPS):
        items += [own_pair(t, j) for j in (outer if t == EARLY else order)]
        if t > EARLY:
            samples[len(items) - len(order) + 3] = t - 1
        for ring in range(HALO // GROUP):
            if ring * GROUP < STEPS - t:
                items.append(Item(t, pairs + ring, ring_rows(ring), lift_only=ring * GROUP >= STEPS - 1 - t))
        if t == EARLY:
            samples[len(items) - 2] = EARLY - 1
    ready = {(0, g) for g in low_rim + high_rim}
    ready |= {(EARLY, g) for g in range(HALO + GROUP, end - GROUP, GROUP)}
    mended = {(EARLY, g) for g in low_groups + high_groups}, {(EARLY, g) for g in low_rim + high_rim}
    stepper = Stepper(
        fields, load, store, factor, metric, wt_ref, wl_ref, ck_ref, t_ref, h_ref, lt_ref, lu_ref
    )
    stepper.run(items, ready, lambda index: sample(samples[index]) if index in samples else None, mended)
    sample(STEPS - 1)


def march(me, own, near, far, past, ops, last_block):
    eh = ops[3]
    planes, elems, _ = own.shape
    fields = planes - AXES
    slots = eh.shape[0]
    smem = pl.BlockSpec(memory_space=pltpu.SMEM)
    vmem = pl.BlockSpec(memory_space=VMEM)
    return pl.pallas_call(
        functools.partial(march_kernel, last_block=last_block),
        in_specs=[smem] + [vmem] * (3 + EARLY + len(ops)),
        out_shape=(
            jax.ShapeDtypeStruct((slots // 2, LANES), F32),
            jax.ShapeDtypeStruct((slots // 2, LANES), F32),
            jax.ShapeDtypeStruct((slots, LANES), F32),
        ),
        scratch_shapes=[
            VMEM((EARLY + 1, fields, 2 * (HALO + GROUP), LANES), F32),
            VMEM((2, fields, elems + 2 * HALO, LANES), F32),
            VMEM((AXES, 2 * (HALO + GROUP), LANES), F32),
        ]
        + scratch(fields, elems),
        compiler_params=pltpu.CompilerParams(vmem_limit_bytes=40 << 20),
        cost_estimate=pl.CostEstimate(flops=20_000_000_000, bytes_accessed=4_000_000, transcendentals=0),
        name="march",
    )(me, own, near, far, *past, *ops)


def pack_kernel(keep_ref, given_ref, out_ref):
    chips = keep_ref.shape[0] // 2
    for other, ref in enumerate((keep_ref, given_ref)):
        for which in range(2):
            out_ref[pl.ds(2 * other + which, chips, stride=4), :] = ref[which * chips : (which + 1) * chips, :]


def pack(keep, given):
    return pl.pallas_call(
        pack_kernel,
        out_shape=jax.ShapeDtypeStruct((2 * keep.shape[0], LANES), F32),
        compiler_params=pltpu.CompilerParams(vmem_limit_bytes=4 << 20),
        name="pack",
    )(keep, given)


def finish_kernel(
    got_ref, rev_ref, to_slot_ref, to_pos_ref, seen_ref, res_hbm, mis_hbm, adj_hbm, res_ref, mis_ref, adj_ref, sems
):
    width, slots = seen_ref.shape
    chips = slots // 4
    got = jnp.concatenate([got_ref[pl.ds(i, chips, stride=4), :] for i in range(4)], axis=0)
    lane = iota(got.shape, 1)
    turned = jnp.where(lane < OBS_LANE, got, rev_ref[...] - got).T

    def place(rows, onehot):
        found = dot(jnp.concatenate(split2(rows), axis=0), onehot)
        return found[:width] + found[width:]

    residual = place(turned[:width], to_pos_ref[...]) - seen_ref[...]
    res_ref[...] = residual
    mis_ref[...] = 0.5 * jnp.sum(residual * residual, axis=0, keepdims=True)
    adj_ref[...] = place(turned[OBS_LANE : OBS_LANE + width], to_slot_ref[...])
    pairs = ((res_ref, res_hbm), (adj_ref, adj_hbm), (mis_ref, mis_hbm))
    copies = [pltpu.make_async_copy(here, out, sems.at[i]) for i, (here, out) in enumerate(pairs)]
    for copy in copies:
        copy.start()
    for copy in copies:
        copy.wait()


def finish(got, rev, to_slot, to_pos, seen):
    width, slots = seen.shape
    vmem = pl.BlockSpec(memory_space=VMEM)
    hbm = pl.BlockSpec(memory_space=pltpu.HBM)
    shapes = ((width, slots), (1, slots), (width, slots))
    return pl.pallas_call(
        finish_kernel,
        in_specs=[vmem] * 5,
        out_specs=(hbm, hbm, hbm),
        out_shape=tuple(jax.ShapeDtypeStruct(shape, F32) for shape in shapes),
        scratch_shapes=[VMEM(shape, F32) for shape in shapes] + [pltpu.SemaphoreType.DMA((3,))],
        compiler_params=pltpu.CompilerParams(vmem_limit_bytes=8 << 20),
        name="finish",
    )(got, rev, to_slot, to_pos, seen)


def shards(
    initial,
    derivative,
    coupling,
    face_lift,
    metric,
    rec_element,
    rec_weight,
    live_counts,
    shot_order,
    observed,
):
    blocks = lax.axis_size(MX)
    slots = rec_element.shape[0]
    me = lax.axis_index(MX).astype(I32).reshape(1)
    order, element, lives = (x.reshape(-1, LANES) for x in (shot_order, rec_element, live_counts))
    staged = (derivative, rec_weight, order, element, lives, observed.T)
    own, near, far, derivative, rec_weight, order, element, lives, observed = turn(me, initial, metric, staged)
    pairs = [(i, min(i + 1, blocks - 1) if i % 2 else max(i - 1, 0)) for i in range(blocks)]
    far = lax.ppermute(far, MX, pairs)
    near = lax.ppermute(near, MX, [(i, i ^ 1) for i in range(blocks)])
    ops = operators(derivative, coupling, face_lift)
    outs = early(me, own, ops, (lives, element, rec_weight, order, observed))
    past, eh, wp, acc0, to_slot, to_pos, seen = (outs[:EARLY],) + tuple(outs[EARLY:])
    keep, give, rev = march(me, own, near, far, past, (*ops, eh, wp, acc0), blocks - 1)
    given = lax.ppermute(give, MX, [(i, i ^ 1) for i in range(blocks)])
    rows = pack(keep, given).reshape(blocks // 2, 4, LANES)
    got = lax.all_to_all(rows, MX[:2], split_axis=0, concat_axis=0, tiled=True)
    residual, misfit, adjoint = finish(got.reshape(slots, LANES), rev, to_slot, to_pos, seen)
    return (residual.T, misfit.reshape(slots), adjoint.T)


def solution(mesh):
    split = Mesh(
        mesh.devices.reshape(mesh.shape["shots"], 8, 8, 2), ("shots", "mx_0", "mx_1", "mx_2")
    )
    in_specs = (
        P("shots", None, MX),
        P(),
        P(),
        P(),
        P(None, MX),
        P(MX),
        P(None, MX),
        P(),
        P(),
        P(SHOTS_MX, None),
    )
    out_specs = (P(SHOTS_MX, None), P(SHOTS_MX), P(SHOTS_MX, None))
    return jax.shard_map(
        shards, mesh=split, in_specs=in_specs, out_specs=out_specs, check_vma=False
    )
```

```python
import functools

import jax
import jax.numpy as jnp
from jax import lax
from jax.experimental import pallas as pl
from jax.experimental.pallas import tpu as pltpu
from jax.sharding import Mesh
from jax.sharding import PartitionSpec as P


STEPS = 12
EARLY = 3
DT = 0.5 / STEPS
AXES = 3
COMPS = 4
MX = ("mx_0", "mx_1", "mx_2")
SHOTS_MX = ("shots", "mx_0", "mx_1", "mx_2")
F32 = jnp.float32
BF16 = jnp.bfloat16
I32 = jnp.int32
LANES = 128
GROUP = 8
PAIR_ROWS = 2 * GROUP
HALO = 16
WHOLE = 32
OBS_LANE = 64
VMEM = pltpu.VMEM


def iota(shape, dim):
    return lax.broadcasted_iota(I32, shape, dim)


def split2(x):
    hi = x.astype(BF16)
    return hi, (x - hi.astype(F32)).astype(BF16)


def dot(a, b):
    return jnp.dot(a, b, preferred_element_type=F32)


def block_index():
    index = 0
    for axis in MX:
        index = index * lax.axis_size(axis) + lax.axis_index(axis)
    return index


def whole(rows):
    return -(-rows // WHOLE) * WHOLE


def padded(x, rows, cols):
    if x.shape[1] < cols:
        x = jnp.concatenate([x, jnp.zeros((x.shape[0], cols - x.shape[1]), x.dtype)], axis=1)
    if x.shape[0] < rows:
        x = jnp.concatenate([x, jnp.zeros((rows - x.shape[0], cols), x.dtype)], axis=0)
    return x


def turn_kernel(*refs):
    staged = (len(refs) - 10) // 2
    initial_hbm, metric_hbm = refs[:2]
    from_refs = refs[2 : 2 + staged]
    own_ref, near_ref, far_ref = refs[2 + staged : 5 + staged]
    to_refs = refs[5 + staged : 5 + 2 * staged]
    initial_ref, metric_ref, low_ref, high_ref, sems = refs[-5:]
    fields, _, elems = initial_ref.shape
    pairs = [(initial_hbm, initial_ref), (metric_hbm, metric_ref)]
    pairs += [(x, y if x.shape == y.shape else y.at[: x.shape[0]]) for x, y in zip(from_refs, to_refs)]
    copies = [pltpu.make_async_copy(x, y, sems.at[i]) for i, (x, y) in enumerate(pairs)]
    for copy in copies:
        copy.start()
    copies[0].wait()
    copies[1].wait()
    for f in range(fields):
        own_ref[f] = padded(initial_ref[f], LANES, elems).T
    for k in range(metric_ref.shape[0]):
        own_ref[fields + k] = jnp.broadcast_to(metric_ref[k : k + 1, :], (LANES, elems)).T
    third = iota((elems, LANES), 1) // (LANES // 3)
    factors = jnp.where(third == 0, own_ref[fields], jnp.where(third == 1, own_ref[fields + 1], own_ref[fields + 2]))
    for edge_ref, rows in ((low_ref, slice(0, STEPS)), (high_ref, slice(elems - STEPS, elems))):
        for f in range(fields):
            edge_ref[f * STEPS : (f + 1) * STEPS, :] = own_ref[f, rows, :]
        edge_ref[fields * STEPS : (fields + 1) * STEPS, :] = factors[rows]
        edge_ref[(fields + 1) * STEPS :, :] = jnp.zeros((edge_ref.shape[0] - (fields + 1) * STEPS, LANES), F32)
    odd = block_index() % 2 == 1
    near_ref[...] = jnp.where(odd, low_ref[...], high_ref[...])
    far_ref[...] = jnp.where(odd, high_ref[...], low_ref[...])
    for copy in copies[2:]:
        copy.wait()


def turn(initial, metric, staged):
    fields, _, elems = initial.shape
    planes = fields + metric.shape[0]
    edge = jax.ShapeDtypeStruct((whole((fields + 1) * STEPS), LANES), F32)
    hbm = pl.BlockSpec(memory_space=pltpu.HBM)
    return pl.pallas_call(
        turn_kernel,
        in_specs=[hbm] * (2 + len(staged)),
        out_shape=(jax.ShapeDtypeStruct((planes, elems, LANES), F32), edge, edge)
        + tuple(jax.ShapeDtypeStruct((whole(x.shape[0]),) + x.shape[1:] if x.shape[0] < GROUP and x.ndim == 2 else x.shape, x.dtype) for x in staged),
        scratch_shapes=[
            VMEM(initial.shape, F32),
            VMEM(metric.shape, F32),
            VMEM(edge.shape, F32),
            VMEM(edge.shape, F32),
            pltpu.SemaphoreType.DMA((2 + len(staged),)),
        ],
        compiler_params=pltpu.CompilerParams(vmem_limit_bytes=8 << 20),
        name="turn",
    )(*(pltpu.with_memory_space_constraint(x, pltpu.HBM) for x in (initial, metric, *staged)))


def operators_kernel(derivative_ref, coupling_ref, lift_ref, wt_ref, wl_ref, ck_ref):
    fields = coupling_ref.shape[1]
    dh, dl = zip(*(split2(padded(DT * derivative_ref[k], LANES, LANES).T) for k in range(AXES)))
    zero = jnp.zeros((LANES, LANES), BF16)
    for row, (left, right) in enumerate(
        [(dh[0], dl[0]), (dh[1], dl[1]), (dh[2], dl[2]), (dh[2], zero), (dh[0], zero), (dh[1], zero)]
    ):
        wt_ref[row * LANES : (row + 1) * LANES, :] = jnp.concatenate([left, right], axis=1)
    l0h, l0l = split2(padded(DT * lift_ref[0], LANES, LANES).T)
    l1h, l1l = split2(padded(DT * lift_ref[1], LANES, LANES).T)
    for row, (left, right) in enumerate([(l0h, l1h), (l0h, l1h), (l0l, l1l)]):
        wl_ref[row * LANES : (row + 1) * LANES, :] = jnp.concatenate([left, right], axis=1)
    rows, cols = AXES * fields * GROUP, fields * GROUP
    spread_rows = (iota((rows, AXES * fields), 0) // GROUP == iota((rows, AXES * fields), 1)).astype(BF16)
    spread_cols = (iota((fields, cols), 0) == iota((fields, cols), 1) // GROUP).astype(BF16)
    hi, lo = split2(jnp.concatenate([coupling_ref[k] for k in range(AXES)], axis=0))
    full = dot(dot(spread_rows, hi).astype(BF16), spread_cols) + dot(dot(spread_rows, lo).astype(BF16), spread_cols)
    full = jnp.where(iota((rows, cols), 0) % GROUP == iota((rows, cols), 1) % GROUP, full, 0.0)
    full_hi = full.astype(BF16).astype(F32)
    spread = padded(jnp.concatenate([full_hi, full_hi, full - full_hi], axis=1), *ck_ref.shape)
    ck_ref[...] = spread.astype(BF16)


def operators(derivative, coupling, face_lift):
    fields = coupling.shape[1]
    block = AXES * fields * GROUP
    return pl.pallas_call(
        operators_kernel,
        out_shape=(
            jax.ShapeDtypeStruct((6 * LANES, 2 * LANES), BF16),
            jax.ShapeDtypeStruct((3 * LANES, 2 * LANES), BF16),
            jax.ShapeDtypeStruct((whole(block), 2 * LANES), BF16),
        ),
        compiler_params=pltpu.CompilerParams(vmem_limit_bytes=8 << 20),
        cost_estimate=pl.CostEstimate(flops=1_000_000_000, bytes_accessed=1_000_000, transcendentals=0),
        name="operators",
    )(derivative, coupling, face_lift)


class Order:
    def __init__(self, me, ins, outs, local):
        self.me = me
        self.lives_ref, self.element_ref, self.weight_ref, self.order_ref, self.observed_ref = ins
        self.eh_ref, self.wp_ref, self.acc_ref, self.to_slot_ref, self.to_pos_ref, self.seen_ref = outs
        self.place_ref, self.weight_parts_ref, self.observed_parts_ref = local
        self.width, self.slots = self.observed_ref.shape
        self.chips = self.slots // 4
        self.big = float(self.slots * self.slots)
        self.bits = self.slots.bit_length() - 1
        assert self.slots == 1 << self.bits
        self.odd = me & 1

    def pieces(self):
        yield from (functools.partial(self.slot_rows, 0), self.weights, functools.partial(self.slot_rows, 1))
        yield from (self.observations, functools.partial(self.position_rows, 0), self.place_weights)
        yield from (functools.partial(self.position_rows, 1), self.seen, self.place_observations)

    def rows(self, other, which):
        start = (2 * other + which) * self.chips
        return slice(start, start + self.chips)

    def across(self, ref):
        return jnp.concatenate([ref[0:1, :], ref[1:2, :]], axis=1)

    def live_of(self, block):
        lives = self.lives_ref[:1, :]
        there = block == iota((block.shape[0], lives.shape[1]), 1)
        return jnp.sum(jnp.where(there, lives.astype(F32), 0.0), axis=1, keepdims=True)

    def slot_rows(self, other):
        slots, chips = self.slots, self.chips
        first, last = None, None
        for half in range(2):
            core = [self.order_ref[pl.ds(2 * core + half, chips, stride=4), :] for core in range(2)]
            order = jnp.where(self.odd == 1 - other, core[1], core[0])
            key = (((half * LANES + iota(order.shape, 1)) << self.bits) + (order & (slots - 1))).astype(F32)
            mine = (order >> self.bits) == self.me
            low, high = jnp.where(mine, key, self.big), jnp.where(mine, key, -1.0)
            first = low if first is None else jnp.minimum(first, low)
            last = high if last is None else jnp.maximum(last, high)
        found = jnp.min(first, axis=1, keepdims=True), jnp.max(last, axis=1, keepdims=True)
        live_slot = iota((1, slots), 1).astype(F32) < self.live_of(jnp.full((1, 1), self.me, I32))
        element = self.across(self.element_ref).astype(F32)
        done = 0.0
        for which in range(2):
            rows = self.rows(other, which)
            hot = (found[which].astype(I32) & (slots - 1)) == iota((chips, slots), 1)
            self.to_slot_ref[rows, :] = jnp.where(hot & live_slot, 1.0, 0.0).astype(BF16)
            element_of = jnp.sum(jnp.where(hot, element, 0.0), axis=1, keepdims=True)
            hit = (element_of.astype(I32) == iota((chips, LANES), 1)).astype(BF16)
            self.eh_ref[rows, :] = jnp.concatenate([hit, hit], axis=1)
            done = done + element_of[:GROUP]
        return jnp.broadcast_to(done, (GROUP, LANES))

    def position_rows(self, other):
        slots, shape = self.slots, (self.chips, self.slots)
        mine = self.order_ref[pl.ds(2 * self.me, 2), :]
        mine = jnp.concatenate([mine[0:1], mine[1:2]], axis=1)
        block = 2 * iota((self.chips, 1), 0) + jnp.where(self.odd == 1 - other, 1, 0)
        col = iota(shape, 1).astype(F32)
        here = (mine >> self.bits) == block
        found = (
            jnp.min(jnp.where(here, col, self.big), axis=1, keepdims=True),
            jnp.max(jnp.where(here, col, -1.0), axis=1, keepdims=True),
        )
        live = self.live_of(block)
        slot = (mine & (slots - 1)).astype(F32)
        done = 0.0
        for which in range(2):
            rows = self.rows(other, which)
            hot = found[which] == col
            self.place_ref[rows, :] = hot.astype(BF16)
            slot_of = jnp.sum(jnp.where(hot, slot, 0.0), axis=1, keepdims=True)
            self.to_pos_ref[rows, :] = jnp.where(hot & (slot_of < live), 1.0, 0.0).astype(BF16)
            done = done + slot_of[:GROUP]
        return jnp.broadcast_to(done, (GROUP, LANES))

    def weights(self):
        weight = padded(self.weight_ref[...], LANES, self.slots).T
        self.weight_parts_ref[...] = jnp.concatenate(split2(weight), axis=1)

    def place_weights(self):
        both = dot(self.to_slot_ref[...], self.weight_parts_ref[...])
        self.wp_ref[...] = both[:, :LANES] + both[:, LANES:]

    def observations(self):
        lane, time = iota((LANES, self.width), 0) - OBS_LANE, iota((LANES, self.width), 1)
        comp = time // STEPS
        turned = (lane == comp * STEPS + (STEPS - 1 - (time - comp * STEPS))).astype(BF16)
        parts = [dot(turned, part).astype(BF16) for part in split2(self.observed_ref[...])]
        self.observed_parts_ref[...] = jnp.concatenate(parts, axis=0)

    def place_observations(self):
        parts = self.observed_parts_ref[...]
        both = lax.dot_general(self.place_ref[...], parts, (((1,), (1,)), ((), ())), preferred_element_type=F32)
        self.acc_ref[...] = both[:, :LANES] + both[:, LANES:]

    def seen(self):
        live = jnp.sum(self.to_pos_ref[...].astype(F32), axis=0, keepdims=True)
        self.seen_ref[...] = self.observed_ref[...] * live


class Stepper:
    def __init__(self, fields, load, store, factor, metric, wt_ref, wl_ref, ck_ref, t_ref, h_ref, lt_ref, lu_ref):
        self.fields, self.load, self.store, self.factor, self.metric = fields, load, store, factor, metric
        self.wt_ref, self.wl_ref, self.ck_ref = wt_ref, wl_ref, ck_ref
        self.t_ref, self.h_ref, self.lt_ref, self.lu_ref = t_ref, h_ref, lt_ref, lu_ref

    def split(self, item):
        halves = ([], [])
        for f in range(self.fields):
            x = jnp.concatenate([self.load(item.t, f, g) for g in item.groups], axis=0)
            hi, lo = split2(x)
            rows = slice(f * PAIR_ROWS, (f + 1) * PAIR_ROWS)
            self.lu_ref[item.slot, rows, :LANES] = hi
            self.lu_ref[item.slot, rows, LANES:] = lo
            hi32 = hi.astype(F32)
            lo32 = x - hi32
            for side in range(2):
                part = slice(side * GROUP, (side + 1) * GROUP)
                halves[side].append((hi32[part], lo32[part]))
        return halves

    def couple(self, item):
        columns = []
        for side in self.split(item):
            his, los = [p[0] for p in side], [p[1] for p in side]
            columns.append(jnp.concatenate(his + los + his, axis=0).astype(BF16))
        if item.lift_only:
            return
        size = 3 * self.fields * GROUP
        v = dot(self.ck_ref[:size, :size], jnp.concatenate(columns, axis=1))
        for k in range(AXES):
            scale = [self.metric(k, g) for g in item.groups]
            if item.after is not None:
                scale = [x + 0.0 * item.after for x in scale]
            parts = []
            for f in range(self.fields):
                base = (k * self.fields + f) * GROUP
                for side in range(2):
                    parts.append(v[base : base + GROUP, side * LANES : (side + 1) * LANES] * scale[side])
            for lane, part in zip(((0, 4), (1, 5), (2, 3))[k], split2(jnp.concatenate(parts, axis=0))):
                self.lt_ref[item.slot, :, lane * LANES : (lane + 1) * LANES] = part

    def apply(self, item):
        lu = self.lu_ref.at[item.slot]
        if not item.lift_only:
            both = dot(self.lt_ref[item.slot], self.wt_ref[...])
            both = both[:, :LANES] + both[:, LANES:]
        lifted = dot(lu[...], self.wl_ref[: 2 * LANES, :]) + dot(lu[:, :LANES], self.wl_ref[2 * LANES :, :])
        for f in range(self.fields):
            for side, g in enumerate(item.groups):
                rows = slice(f * PAIR_ROWS + side * GROUP, f * PAIR_ROWS + (side + 1) * GROUP)
                if not item.lift_only:
                    self.t_ref[f, g : g + GROUP, :] = both[rows]
                for face in range(2):
                    at = g + GROUP
                    self.h_ref[face, f, at : at + GROUP, :] = lifted[rows, face * LANES : (face + 1) * LANES]

    def update(self, t, g):
        at = g + GROUP
        here, before, after = slice(at, at + GROUP), slice(at - 1, at - 1 + GROUP), slice(at + 1, at + 1 + GROUP)
        for f in range(self.fields):
            low, high = self.h_ref.at[0, f], self.h_ref.at[1, f]
            lift = (low[before, :] - low[here, :]) + (high[after, :] - high[here, :])
            change = self.t_ref[f, g : g + GROUP, :] + lift
            if self.factor(g) is not None:
                change = self.factor(g) * change
            self.store(t, f, g, self.load(t, f, g) + change)

    def run(self, items, ready, after, mended=(set(), set())):
        ready = set(ready)
        product, lifted, done = set(), set(), set()
        wanted = {}
        for item in items:
            for g in item.groups:
                wanted.setdefault(item.t, {})[g] = item
        coupled = 0

        def couple_next(limit):
            nonlocal coupled
            while coupled < limit and all((items[coupled].t, g) in ready for g in items[coupled].groups):
                self.couple(items[coupled])
                coupled += 1

        for index, item in enumerate(items):
            couple_next(min(index + 2, len(items)))
            assert coupled > index
            self.apply(item)
            for g in item.groups:
                lifted.add((item.t, g))
                if not item.lift_only:
                    product.add((item.t, g))
            for t, groups in wanted.items():
                for g in groups:
                    if (t, g) in done or (t, g) not in product:
                        continue
                    if all(n not in groups or (t, n) in lifted for n in (g - GROUP, g + GROUP)):
                        self.update(t, g)
                        done.add((t, g))
                        ready.add((t + 1, g))
            if mended[1] <= ready:
                ready |= mended[0]
            after(index)


class Item:
    after = None

    def __init__(self, t, slot, groups, lift_only=False):
        self.t, self.slot, self.groups, self.lift_only = t, slot, groups, lift_only


def own_pair(t, j):
    first = HALO + PAIR_ROWS * j
    return Item(t, j, (first, first + GROUP))


def early_kernel(own_ref, wt_ref, wl_ref, ck_ref, *refs):
    ins, past, outs = refs[:5], refs[5 : 5 + EARLY], refs[5 + EARLY : 11 + EARLY]
    t_ref, h_ref, lt_ref, lu_ref, *local = refs[11 + EARLY :]
    planes, elems, _ = own_ref.shape
    fields = planes - AXES
    rows = lambda g: slice(g - HALO, g - HALO + GROUP)

    def load(t, f, g):
        return own_ref[f, rows(g), :] if t == 0 else past[t - 1][f, rows(g), :]

    def store(t, f, g, value):
        past[t][f, rows(g), :] = value

    pad = slice(HALO, HALO + GROUP), slice(elems + HALO + GROUP, elems + HALO + 2 * GROUP)
    for rim in pad:
        h_ref[:, :, rim, :] = jnp.zeros((2, fields, GROUP, LANES), F32)
    stepper = Stepper(
        fields, load, store, lambda g: None, lambda k, g: own_ref[fields + k, rows(g), :],
        wt_ref, wl_ref, ck_ref, t_ref, h_ref, lt_ref, lu_ref,
    )
    pairs = elems // PAIR_ROWS
    order = sorted(range(pairs), key=lambda j: abs(2 * j + 1 - pairs))
    items = [own_pair(t, j) for t in range(EARLY) for j in order]
    pieces = list(Order(block_index(), ins, outs, local).pieces())
    at = {(len(items) - 4) * i // len(pieces): piece for i, piece in enumerate(pieces)}

    def beside(index):
        if index in at:
            items[index + 4].after = at[index]()

    stepper.run(items, {(0, g) for item in items for g in item.groups}, beside)


def scratch(fields, elems):
    rows = elems + 2 * HALO
    tile = fields * PAIR_ROWS
    slots = rows // PAIR_ROWS + 2
    return [
        VMEM((fields, rows, LANES), F32),
        VMEM((2, fields, rows + 2 * GROUP, LANES), F32),
        VMEM((slots, tile, 6 * LANES), BF16),
        VMEM((slots, tile, 2 * LANES), BF16),
    ]


def early(own, operators, ins):
    planes, elems, _ = own.shape
    fields = planes - AXES
    width, slots = ins[-1].shape
    vmem = pl.BlockSpec(memory_space=VMEM)
    return pl.pallas_call(
        early_kernel,
        in_specs=[vmem] * (1 + len(operators) + len(ins)),
        out_shape=tuple(jax.ShapeDtypeStruct((fields, elems, LANES), F32) for _ in range(EARLY))
        + (
            jax.ShapeDtypeStruct((slots, 2 * LANES), BF16),
            jax.ShapeDtypeStruct((slots, LANES), F32),
            jax.ShapeDtypeStruct((slots, LANES), F32),
            jax.ShapeDtypeStruct((slots, slots), BF16),
            jax.ShapeDtypeStruct((slots, slots), BF16),
            jax.ShapeDtypeStruct((width, slots), F32),
        ),
        scratch_shapes=scratch(fields, elems) + [VMEM((slots, slots), BF16)] * 3,
        compiler_params=pltpu.CompilerParams(vmem_limit_bytes=32 << 20),
        cost_estimate=pl.CostEstimate(flops=5_000_000_000, bytes_accessed=4_000_000, transcendentals=0),
        name="early",
    )(own, *operators, *ins)


def march_kernel(own_ref, near_ref, far_ref, *refs, last_block):
    past = (own_ref,) + refs[:EARLY]
    wt_ref, wl_ref, ck_ref, eh_ref, wp_ref, acc0_ref, keep_ref, give_ref, rev_ref = refs[EARLY : EARLY + 9]
    edge_ref, u_ref, m_ref, t_ref, h_ref, lt_ref, lu_ref = refs[EARLY + 9 :]
    planes, elems, _ = own_ref.shape
    fields = planes - AXES
    slots = eh_ref.shape[0]
    end = HALO + elems
    me = block_index()
    in_low = jnp.where(me == 0, 0.0, 1.0).astype(F32)
    in_high = jnp.where(me == last_block, 0.0, 1.0).astype(F32)
    skip = HALO - STEPS
    side_rows = HALO + GROUP
    low_rim, high_rim = [skip, skip + GROUP], [end - skip, end - skip + GROUP]
    low_groups, high_groups = list(range(0, side_rows, GROUP)), list(range(end - GROUP, end + HALO, GROUP))
    own_rows = lambda g: slice(g - HALO, g - HALO + GROUP)

    def rim_rows(g):
        at = g if g < HALO + GROUP else side_rows + g - (end - GROUP)
        return slice(at, at + GROUP)

    odd = me % 2 == 1
    low_edge = lambda edge: jnp.where(odd, near_ref[edge], far_ref[edge])
    high_edge = lambda edge: jnp.where(odd, far_ref[edge], near_ref[edge])
    spare = jnp.zeros((skip, LANES), F32)
    for f in range(fields):
        edge = slice(f * STEPS, (f + 1) * STEPS)
        low = jnp.where(me > 0, low_edge(edge), 0.0)
        high = jnp.where(me < last_block, high_edge(edge), 0.0)
        edge_ref[0, f, :side_rows, :] = jnp.concatenate([spare, low, own_ref[f, :GROUP, :]], axis=0)
        edge_ref[0, f, side_rows:, :] = jnp.concatenate([own_ref[f, elems - GROUP :, :], high, spare], axis=0)
    edge_ref[EARLY] = jnp.zeros(edge_ref.shape[1:], F32)
    edge = slice(fields * STEPS, (fields + 1) * STEPS)
    low_factors, high_factors = low_edge(edge), high_edge(edge)
    for k in range(AXES):
        lane = k * (LANES // AXES)
        spread = lambda x: jnp.broadcast_to(x[:, lane : lane + 1], (STEPS, LANES))
        own_low, own_high = own_ref[fields + k, :GROUP, :], own_ref[fields + k, elems - GROUP :, :]
        m_ref[k, :side_rows, :] = jnp.concatenate([spare, spread(low_factors), own_low], axis=0)
        m_ref[k, side_rows:, :] = jnp.concatenate([own_high, spread(high_factors), spare], axis=0)
    h_ref[:, :, :PAIR_ROWS, :] = jnp.zeros((2, fields, PAIR_ROWS, LANES), F32)
    h_ref[:, :, end + GROUP + HALO - GROUP :, :] = jnp.zeros((2, fields, PAIR_ROWS, LANES), F32)
    half = slots // 2
    keep_ref[...] = acc0_ref[:half]
    give_ref[...] = acc0_ref[half:]
    rev_ref[...] = jnp.zeros(rev_ref.shape, F32)

    def load(t, f, g):
        if t > EARLY:
            return u_ref[t % 2, f, g : g + GROUP, :]
        if t == EARLY and g in low_groups + high_groups or g in low_rim + high_rim:
            return edge_ref[t, f, rim_rows(g), :]
        return past[t][f, own_rows(g), :]

    def store(t, f, g, value):
        if t >= EARLY:
            u_ref[(t + 1) % 2, f, g : g + GROUP, :] = value
            return
        row = iota((GROUP, LANES), 0)
        if g == low_rim[1]:
            rest = past[t + 1][f, : GROUP - skip, :]
            value = jnp.where(row <= skip + t, value, jnp.concatenate([rest[:skip], rest], axis=0))
            if t == EARLY - 1:
                edge_ref[EARLY, f, side_rows - skip : side_rows, :] = past[t + 1][f, GROUP - skip : GROUP, :]
        if g == high_rim[0]:
            rest = past[t + 1][f, elems - (GROUP - skip) :, :]
            value = jnp.where(row >= GROUP - skip - 1 - t, value, jnp.concatenate([rest, rest[:skip]], axis=0))
            if t == EARLY - 1:
                at = elems - GROUP
                edge_ref[EARLY, f, side_rows : side_rows + skip, :] = past[t + 1][f, at : at + skip, :]
        edge_ref[t + 1, f, rim_rows(g), :] = value

    def metric(k, g):
        if g < HALO or g > end - GROUP:
            return m_ref[k, rim_rows(g), :]
        return own_ref[fields + k, own_rows(g), :]

    def factor(g):
        if g + GROUP <= HALO:
            return in_low
        if g >= end:
            return in_high
        if g < HALO:
            return jnp.where(iota((GROUP, LANES), 0) < HALO - g, in_low, 1.0)
        if g + GROUP > end:
            return jnp.where(iota((GROUP, LANES), 0) >= end - g, in_high, 1.0)
        return None

    def own_load(t, f, g):
        if t < EARLY and g in (HALO, end - GROUP):
            rest, row = past[t][f, own_rows(g), :], iota((GROUP, LANES), 0)
            mended = edge_ref[t, f, rim_rows(g), :]
            return jnp.where(row < t, mended, rest) if g == HALO else jnp.where(row >= GROUP - t, mended, rest)
        return load(t, f, g)

    def sample(t):
        field = lambda f: jnp.concatenate([own_load(t + 1, f, g) for g in range(HALO, end, GROUP)], axis=0)
        columns = []
        for c in range(COMPS):
            x = field(c) if c < 3 else (field(3) + field(4) + field(5)) / 3.0
            columns.append(jnp.concatenate(split2(x), axis=0))
        lane = iota((slots, LANES), 1)
        send = jnp.concatenate([keep_ref[...], give_ref[...]], axis=0)
        rev = rev_ref[...]
        for c in range(0, COMPS, 2):
            found = dot(eh_ref[...], jnp.concatenate(columns[c : c + 2], axis=1))
            for i in range(2):
                value = jnp.sum(found[:, i * LANES : (i + 1) * LANES] * wp_ref[...], axis=1, keepdims=True)
                send = jnp.where(lane == (c + i) * STEPS + t, value, send)
                rev = jnp.where(lane == OBS_LANE + (c + i) * STEPS + (STEPS - 1) - t, value, rev)
        keep_ref[...] = send[:half]
        give_ref[...] = send[half:]
        rev_ref[...] = rev

    pairs = elems // PAIR_ROWS
    order = sorted(range(pairs), key=lambda j: abs(2 * j + 1 - pairs))
    inner, outer = order[:-2], order[-2:]
    ring_rows = lambda ring: (HALO - GROUP * (ring + 1), end + GROUP * ring)
    items, samples = [], {}
    fill = -(-len(inner) // EARLY)
    for t in range(EARLY):
        items += [Item(t, pairs, (low_rim[1], high_rim[0])), Item(t, pairs + 1, (low_rim[0], high_rim[1]))]
        items += [own_pair(EARLY, j) for j in inner[t * fill : (t + 1) * fill]]
        if t >= 1:
            samples[len(items) - 1] = t - 1
    for t in range(EARLY, STEPS):
        items += [own_pair(t, j) for j in (outer if t == EARLY else order)]
        if t > EARLY:
            samples[len(items) - len(order) + 3] = t - 1
        for ring in range(HALO // GROUP):
            if ring * GROUP < STEPS - t:
                items.append(Item(t, pairs + ring, ring_rows(ring), lift_only=ring * GROUP >= STEPS - 1 - t))
        if t == EARLY:
            samples[len(items) - 2] = EARLY - 1
    ready = {(0, g) for g in low_rim + high_rim}
    ready |= {(EARLY, g) for g in range(HALO + GROUP, end - GROUP, GROUP)}
    mended = {(EARLY, g) for g in low_groups + high_groups}, {(EARLY, g) for g in low_rim + high_rim}
    stepper = Stepper(
        fields, load, store, factor, metric, wt_ref, wl_ref, ck_ref, t_ref, h_ref, lt_ref, lu_ref
    )
    stepper.run(items, ready, lambda index: sample(samples[index]) if index in samples else None, mended)
    sample(STEPS - 1)


def march(own, near, far, past, ops, last_block):
    eh = ops[3]
    planes, elems, _ = own.shape
    fields = planes - AXES
    slots = eh.shape[0]
    vmem = pl.BlockSpec(memory_space=VMEM)
    return pl.pallas_call(
        functools.partial(march_kernel, last_block=last_block),
        in_specs=[vmem] * (3 + EARLY + len(ops)),
        out_shape=(
            jax.ShapeDtypeStruct((slots // 2, LANES), F32),
            jax.ShapeDtypeStruct((slots // 2, LANES), F32),
            jax.ShapeDtypeStruct((slots, LANES), F32),
        ),
        scratch_shapes=[
            VMEM((EARLY + 1, fields, 2 * (HALO + GROUP), LANES), F32),
            VMEM((2, fields, elems + 2 * HALO, LANES), F32),
            VMEM((AXES, 2 * (HALO + GROUP), LANES), F32),
        ]
        + scratch(fields, elems),
        compiler_params=pltpu.CompilerParams(vmem_limit_bytes=40 << 20),
        cost_estimate=pl.CostEstimate(flops=20_000_000_000, bytes_accessed=4_000_000, transcendentals=0),
        name="march",
    )(own, near, far, *past, *ops)


def pack_kernel(keep_ref, given_ref, out_ref):
    chips = keep_ref.shape[0] // 2
    for other, ref in enumerate((keep_ref, given_ref)):
        for which in range(2):
            out_ref[pl.ds(2 * other + which, chips, stride=4), :] = ref[which * chips : (which + 1) * chips, :]


def pack(keep, given):
    return pl.pallas_call(
        pack_kernel,
        out_shape=jax.ShapeDtypeStruct((2 * keep.shape[0], LANES), F32),
        compiler_params=pltpu.CompilerParams(vmem_limit_bytes=4 << 20),
        name="pack",
    )(keep, given)


def finish_kernel(
    got_ref, rev_ref, to_slot_ref, to_pos_ref, seen_ref, res_hbm, mis_hbm, adj_hbm, res_ref, mis_ref, adj_ref, sems
):
    width, slots = seen_ref.shape
    chips = slots // 4
    got = jnp.concatenate([got_ref[pl.ds(i, chips, stride=4), :] for i in range(4)], axis=0)
    lane = iota(got.shape, 1)
    turned = jnp.where(lane < OBS_LANE, got, rev_ref[...] - got).T

    def place(rows, onehot):
        found = dot(jnp.concatenate(split2(rows), axis=0), onehot)
        return found[:width] + found[width:]

    residual = place(turned[:width], to_pos_ref[...]) - seen_ref[...]
    res_ref[...] = residual
    mis_ref[...] = 0.5 * jnp.sum(residual * residual, axis=0, keepdims=True)
    adj_ref[...] = place(turned[OBS_LANE : OBS_LANE + width], to_slot_ref[...])
    pairs = ((res_ref, res_hbm), (adj_ref, adj_hbm), (mis_ref, mis_hbm))
    copies = [pltpu.make_async_copy(here, out, sems.at[i]) for i, (here, out) in enumerate(pairs)]
    for copy in copies:
        copy.start()
    for copy in copies:
        copy.wait()


def finish(got, rev, to_slot, to_pos, seen):
    width, slots = seen.shape
    vmem = pl.BlockSpec(memory_space=VMEM)
    hbm = pl.BlockSpec(memory_space=pltpu.HBM)
    shapes = ((width, slots), (1, slots), (width, slots))
    return pl.pallas_call(
        finish_kernel,
        in_specs=[vmem] * 5,
        out_specs=(hbm, hbm, hbm),
        out_shape=tuple(jax.ShapeDtypeStruct(shape, F32) for shape in shapes),
        scratch_shapes=[VMEM(shape, F32) for shape in shapes] + [pltpu.SemaphoreType.DMA((3,))],
        compiler_params=pltpu.CompilerParams(vmem_limit_bytes=8 << 20),
        name="finish",
    )(got, rev, to_slot, to_pos, seen)


def shards(
    initial,
    derivative,
    coupling,
    face_lift,
    metric,
    rec_element,
    rec_weight,
    live_counts,
    shot_order,
    observed,
):
    blocks = lax.axis_size(MX)
    slots = rec_element.shape[0]
    order, element, lives = (x.reshape(-1, LANES) for x in (shot_order, rec_element, live_counts))
    staged = (derivative, rec_weight, order, element, lives, observed.T)
    own, near, far, derivative, rec_weight, order, element, lives, observed = turn(initial, metric, staged)
    pairs = [(i, min(i + 1, blocks - 1) if i % 2 else max(i - 1, 0)) for i in range(blocks)]
    far = lax.ppermute(far, MX, pairs)
    near = lax.ppermute(near, MX, [(i, i ^ 1) for i in range(blocks)])
    ops = operators(derivative, coupling, face_lift)
    outs = early(own, ops, (lives, element, rec_weight, order, observed))
    past, eh, wp, acc0, to_slot, to_pos, seen = (outs[:EARLY],) + tuple(outs[EARLY:])
    keep, give, rev = march(own, near, far, past, (*ops, eh, wp, acc0), blocks - 1)
    given = lax.ppermute(give, MX, [(i, i ^ 1) for i in range(blocks)])
    rows = pack(keep, given).reshape(blocks // 2, 4, LANES)
    got = lax.all_to_all(rows, MX[:2], split_axis=0, concat_axis=0, tiled=True)
    residual, misfit, adjoint = finish(got.reshape(slots, LANES), rev, to_slot, to_pos, seen)
    return (residual.T, misfit.reshape(slots), adjoint.T)


def solution(mesh):
    split = Mesh(
        mesh.devices.reshape(mesh.shape["shots"], 8, 8, 2), ("shots", "mx_0", "mx_1", "mx_2")
    )
    in_specs = (
        P("shots", None, MX),
        P(),
        P(),
        P(),
        P(None, MX),
        P(MX),
        P(None, MX),
        P(),
        P(),
        P(SHOTS_MX, None),
    )
    out_specs = (P(SHOTS_MX, None), P(SHOTS_MX), P(SHOTS_MX, None))
    return jax.shard_map(
        shards, mesh=split, in_specs=in_specs, out_specs=out_specs, check_vma=False
    )
```

```python
import functools

import jax
import jax.numpy as jnp
from jax import lax
from jax.experimental import pallas as pl
from jax.experimental.pallas import tpu as pltpu
from jax.sharding import Mesh
from jax.sharding import PartitionSpec as P


STEPS = 12
EARLY = 3
DT = 0.5 / STEPS
AXES = 3
COMPS = 4
MX = ("mx_0", "mx_1", "mx_2")
SHOTS_MX = ("shots", "mx_0", "mx_1", "mx_2")
F32 = jnp.float32
BF16 = jnp.bfloat16
I32 = jnp.int32
LANES = 128
GROUP = 8
PAIR_ROWS = 2 * GROUP
HALO = 16
WHOLE = 32
OBS_LANE = 64
VMEM = pltpu.VMEM


def iota(shape, dim):
    return lax.broadcasted_iota(I32, shape, dim)


def split2(x):
    hi = x.astype(BF16)
    return hi, (x - hi.astype(F32)).astype(BF16)


def dot(a, b):
    return jnp.dot(a, b, preferred_element_type=F32)


def block_index():
    index = 0
    for axis in MX:
        index = index * lax.axis_size(axis) + lax.axis_index(axis)
    return index


def whole(rows):
    return -(-rows // WHOLE) * WHOLE


def padded(x, rows, cols):
    if x.shape[1] < cols:
        x = jnp.concatenate([x, jnp.zeros((x.shape[0], cols - x.shape[1]), x.dtype)], axis=1)
    if x.shape[0] < rows:
        x = jnp.concatenate([x, jnp.zeros((rows - x.shape[0], cols), x.dtype)], axis=0)
    return x


def turn_kernel(*refs):
    staged = (len(refs) - 10) // 2
    initial_hbm, metric_hbm = refs[:2]
    from_refs = refs[2 : 2 + staged]
    own_ref, near_ref, far_ref = refs[2 + staged : 5 + staged]
    to_refs = refs[5 + staged : 5 + 2 * staged]
    initial_ref, metric_ref, low_ref, high_ref, sems = refs[-5:]
    fields, _, elems = initial_ref.shape
    pairs = [(initial_hbm, initial_ref), (metric_hbm, metric_ref)]
    pairs += [(x, y if x.shape == y.shape else y.at[: x.shape[0]]) for x, y in zip(from_refs, to_refs)]
    copies = [pltpu.make_async_copy(x, y, sems.at[i]) for i, (x, y) in enumerate(pairs)]
    for copy in copies:
        copy.start()
    copies[0].wait()
    copies[1].wait()
    for f in range(fields):
        own_ref[f] = padded(initial_ref[f], LANES, elems).T
    for k in range(metric_ref.shape[0]):
        own_ref[fields + k] = jnp.broadcast_to(metric_ref[k : k + 1, :], (LANES, elems)).T
    third = iota((elems, LANES), 1) // (LANES // 3)
    factors = jnp.where(third == 0, own_ref[fields], jnp.where(third == 1, own_ref[fields + 1], own_ref[fields + 2]))
    for edge_ref, rows in ((low_ref, slice(0, STEPS)), (high_ref, slice(elems - STEPS, elems))):
        for f in range(fields):
            edge_ref[f * STEPS : (f + 1) * STEPS, :] = own_ref[f, rows, :]
        edge_ref[fields * STEPS : (fields + 1) * STEPS, :] = factors[rows]
        edge_ref[(fields + 1) * STEPS :, :] = jnp.zeros((edge_ref.shape[0] - (fields + 1) * STEPS, LANES), F32)
    odd = block_index() % 2 == 1
    near_ref[...] = jnp.where(odd, low_ref[...], high_ref[...])
    far_ref[...] = jnp.where(odd, high_ref[...], low_ref[...])
    for copy in copies[2:]:
        copy.wait()


def turn(initial, metric, staged):
    fields, _, elems = initial.shape
    planes = fields + metric.shape[0]
    edge = jax.ShapeDtypeStruct((whole((fields + 1) * STEPS), LANES), F32)
    hbm = pl.BlockSpec(memory_space=pltpu.HBM)
    return pl.pallas_call(
        turn_kernel,
        in_specs=[hbm] * (2 + len(staged)),
        out_shape=(jax.ShapeDtypeStruct((planes, elems, LANES), F32), edge, edge)
        + tuple(jax.ShapeDtypeStruct((whole(x.shape[0]),) + x.shape[1:] if x.shape[0] < GROUP and x.ndim == 2 else x.shape, x.dtype) for x in staged),
        scratch_shapes=[
            VMEM(initial.shape, F32),
            VMEM(metric.shape, F32),
            VMEM(edge.shape, F32),
            VMEM(edge.shape, F32),
            pltpu.SemaphoreType.DMA((2 + len(staged),)),
        ],
        compiler_params=pltpu.CompilerParams(vmem_limit_bytes=8 << 20),
        name="turn",
    )(*(pltpu.with_memory_space_constraint(x, pltpu.HBM) for x in (initial, metric, *staged)))


def operators_kernel(derivative_ref, coupling_ref, lift_ref, wt_ref, wl_ref, ck_ref):
    fields = coupling_ref.shape[1]
    dh, dl = zip(*(split2(padded(DT * derivative_ref[k], LANES, LANES).T) for k in range(AXES)))
    zero = jnp.zeros((LANES, LANES), BF16)
    for row, (left, right) in enumerate(
        [(dh[0], dl[0]), (dh[1], dl[1]), (dh[2], dl[2]), (dh[2], zero), (dh[0], zero), (dh[1], zero)]
    ):
        wt_ref[row * LANES : (row + 1) * LANES, :] = jnp.concatenate([left, right], axis=1)
    l0h, l0l = split2(padded(DT * lift_ref[0], LANES, LANES).T)
    l1h, l1l = split2(padded(DT * lift_ref[1], LANES, LANES).T)
    for row, (left, right) in enumerate([(l0h, l1h), (l0h, l1h), (l0l, l1l)]):
        wl_ref[row * LANES : (row + 1) * LANES, :] = jnp.concatenate([left, right], axis=1)
    rows, cols = AXES * fields * GROUP, fields * GROUP
    spread_rows = (iota((rows, AXES * fields), 0) // GROUP == iota((rows, AXES * fields), 1)).astype(BF16)
    spread_cols = (iota((fields, cols), 0) == iota((fields, cols), 1) // GROUP).astype(BF16)
    hi, lo = split2(jnp.concatenate([coupling_ref[k] for k in range(AXES)], axis=0))
    full = dot(dot(spread_rows, hi).astype(BF16), spread_cols) + dot(dot(spread_rows, lo).astype(BF16), spread_cols)
    full = jnp.where(iota((rows, cols), 0) % GROUP == iota((rows, cols), 1) % GROUP, full, 0.0)
    full_hi = full.astype(BF16).astype(F32)
    spread = padded(jnp.concatenate([full_hi, full_hi, full - full_hi], axis=1), *ck_ref.shape)
    ck_ref[...] = spread.astype(BF16)


def operators(derivative, coupling, face_lift):
    fields = coupling.shape[1]
    block = AXES * fields * GROUP
    return pl.pallas_call(
        operators_kernel,
        out_shape=(
            jax.ShapeDtypeStruct((6 * LANES, 2 * LANES), BF16),
            jax.ShapeDtypeStruct((3 * LANES, 2 * LANES), BF16),
            jax.ShapeDtypeStruct((whole(block), 2 * LANES), BF16),
        ),
        compiler_params=pltpu.CompilerParams(vmem_limit_bytes=8 << 20),
        cost_estimate=pl.CostEstimate(flops=1_000_000_000, bytes_accessed=1_000_000, transcendentals=0),
        name="operators",
    )(derivative, coupling, face_lift)


class Order:
    def __init__(self, me, ins, outs, local):
        self.me = me
        self.lives_ref, self.element_ref, self.weight_ref, self.order_ref, self.observed_ref = ins
        self.eh_ref, self.wp_ref, self.acc_ref, self.to_slot_ref, self.to_pos_ref, self.seen_ref = outs
        self.place_ref, self.weight_parts_ref, self.observed_parts_ref = local
        self.width, self.slots = self.observed_ref.shape
        self.chips = self.slots // 4
        self.big = float(self.slots * self.slots)
        self.bits = self.slots.bit_length() - 1
        assert self.slots == 1 << self.bits
        self.odd = me & 1

    def pieces(self):
        yield from (functools.partial(self.slot_rows, 0), self.weights, functools.partial(self.slot_rows, 1))
        yield from (self.observations, functools.partial(self.position_rows, 0), self.place_weights)
        yield from (functools.partial(self.position_rows, 1), self.seen, self.place_observations)

    def rows(self, other, which):
        start = (2 * other + which) * self.chips
        return slice(start, start + self.chips)

    def across(self, ref):
        return jnp.concatenate([ref[0:1, :], ref[1:2, :]], axis=1)

    def live_of(self, block):
        lives = self.lives_ref[:1, :]
        there = block == iota((block.shape[0], lives.shape[1]), 1)
        return jnp.sum(jnp.where(there, lives.astype(F32), 0.0), axis=1, keepdims=True)

    def slot_rows(self, other):
        slots, chips = self.slots, self.chips
        first, last = None, None
        for half in range(2):
            core = [self.order_ref[pl.ds(2 * core + half, chips, stride=4), :] for core in range(2)]
            order = jnp.where(self.odd == 1 - other, core[1], core[0])
            key = (((half * LANES + iota(order.shape, 1)) << self.bits) + (order & (slots - 1))).astype(F32)
            mine = (order >> self.bits) == self.me
            low, high = jnp.where(mine, key, self.big), jnp.where(mine, key, -1.0)
            first = low if first is None else jnp.minimum(first, low)
            last = high if last is None else jnp.maximum(last, high)
        found = jnp.min(first, axis=1, keepdims=True), jnp.max(last, axis=1, keepdims=True)
        live_slot = iota((1, slots), 1).astype(F32) < self.live_of(jnp.full((1, 1), self.me, I32))
        element = self.across(self.element_ref).astype(F32)
        done = 0.0
        for which in range(2):
            rows = self.rows(other, which)
            hot = (found[which].astype(I32) & (slots - 1)) == iota((chips, slots), 1)
            self.to_slot_ref[rows, :] = jnp.where(hot & live_slot, 1.0, 0.0).astype(BF16)
            element_of = jnp.sum(jnp.where(hot, element, 0.0), axis=1, keepdims=True)
            hit = (element_of.astype(I32) == iota((chips, LANES), 1)).astype(BF16)
            self.eh_ref[rows, :] = jnp.concatenate([hit, hit], axis=1)
            done = done + element_of[:GROUP]
        return jnp.broadcast_to(done, (GROUP, LANES))

    def position_rows(self, other):
        slots, shape = self.slots, (self.chips, self.slots)
        mine = self.order_ref[pl.ds(2 * self.me, 2), :]
        mine = jnp.concatenate([mine[0:1], mine[1:2]], axis=1)
        block = 2 * iota((self.chips, 1), 0) + jnp.where(self.odd == 1 - other, 1, 0)
        col = iota(shape, 1).astype(F32)
        here = (mine >> self.bits) == block
        found = (
            jnp.min(jnp.where(here, col, self.big), axis=1, keepdims=True),
            jnp.max(jnp.where(here, col, -1.0), axis=1, keepdims=True),
        )
        live = self.live_of(block)
        slot = (mine & (slots - 1)).astype(F32)
        done = 0.0
        for which in range(2):
            rows = self.rows(other, which)
            hot = found[which] == col
            self.place_ref[rows, :] = hot.astype(BF16)
            slot_of = jnp.sum(jnp.where(hot, slot, 0.0), axis=1, keepdims=True)
            self.to_pos_ref[rows, :] = jnp.where(hot & (slot_of < live), 1.0, 0.0).astype(BF16)
            done = done + slot_of[:GROUP]
        return jnp.broadcast_to(done, (GROUP, LANES))

    def weights(self):
        weight = padded(self.weight_ref[...], LANES, self.slots).T
        self.weight_parts_ref[...] = jnp.concatenate(split2(weight), axis=1)

    def place_weights(self):
        both = dot(self.to_slot_ref[...], self.weight_parts_ref[...])
        self.wp_ref[...] = both[:, :LANES] + both[:, LANES:]

    def observations(self):
        lane, time = iota((LANES, self.width), 0) - OBS_LANE, iota((LANES, self.width), 1)
        comp = time // STEPS
        turned = (lane == comp * STEPS + (STEPS - 1 - (time - comp * STEPS))).astype(BF16)
        parts = [dot(turned, part).astype(BF16) for part in split2(self.observed_ref[...])]
        self.observed_parts_ref[...] = jnp.concatenate(parts, axis=0)

    def place_observations(self):
        parts = self.observed_parts_ref[...]
        both = lax.dot_general(self.place_ref[...], parts, (((1,), (1,)), ((), ())), preferred_element_type=F32)
        self.acc_ref[...] = both[:, :LANES] + both[:, LANES:]

    def seen(self):
        live = jnp.sum(self.to_pos_ref[...].astype(F32), axis=0, keepdims=True)
        self.seen_ref[...] = self.observed_ref[...] * live


class Stepper:
    def __init__(self, fields, load, store, factor, metric, wt_ref, wl_ref, ck_ref, t_ref, h_ref, lt_ref, lu_ref):
        self.fields, self.load, self.store, self.factor, self.metric = fields, load, store, factor, metric
        self.wt_ref, self.wl_ref, self.ck_ref = wt_ref, wl_ref, ck_ref
        self.t_ref, self.h_ref, self.lt_ref, self.lu_ref = t_ref, h_ref, lt_ref, lu_ref

    def split(self, item):
        halves = ([], [])
        for f in range(self.fields):
            x = jnp.concatenate([self.load(item.t, f, g) for g in item.groups], axis=0)
            hi, lo = split2(x)
            rows = slice(f * PAIR_ROWS, (f + 1) * PAIR_ROWS)
            self.lu_ref[item.slot, rows, :LANES] = hi
            self.lu_ref[item.slot, rows, LANES:] = lo
            hi32 = hi.astype(F32)
            lo32 = x - hi32
            for side in range(2):
                part = slice(side * GROUP, (side + 1) * GROUP)
                halves[side].append((hi32[part], lo32[part]))
        return halves

    def couple(self, item):
        columns = []
        for side in self.split(item):
            his, los = [p[0] for p in side], [p[1] for p in side]
            columns.append(jnp.concatenate(his + los + his, axis=0).astype(BF16))
        if item.lift_only:
            return
        size = 3 * self.fields * GROUP
        v = dot(self.ck_ref[:size, :size], jnp.concatenate(columns, axis=1))
        for k in range(AXES):
            scale = [self.metric(k, g) for g in item.groups]
            if item.after is not None:
                scale = [x + 0.0 * item.after for x in scale]
            parts = []
            for f in range(self.fields):
                base = (k * self.fields + f) * GROUP
                for side in range(2):
                    parts.append(v[base : base + GROUP, side * LANES : (side + 1) * LANES] * scale[side])
            for lane, part in zip(((0, 4), (1, 5), (2, 3))[k], split2(jnp.concatenate(parts, axis=0))):
                self.lt_ref[item.slot, :, lane * LANES : (lane + 1) * LANES] = part

    def apply(self, item):
        lu = self.lu_ref.at[item.slot]
        if not item.lift_only:
            both = dot(self.lt_ref[item.slot], self.wt_ref[...])
            both = both[:, :LANES] + both[:, LANES:]
        lifted = dot(lu[...], self.wl_ref[: 2 * LANES, :]) + dot(lu[:, :LANES], self.wl_ref[2 * LANES :, :])
        for f in range(self.fields):
            for side, g in enumerate(item.groups):
                rows = slice(f * PAIR_ROWS + side * GROUP, f * PAIR_ROWS + (side + 1) * GROUP)
                if not item.lift_only:
                    self.t_ref[f, g : g + GROUP, :] = both[rows]
                for face in range(2):
                    at = g + GROUP
                    self.h_ref[face, f, at : at + GROUP, :] = lifted[rows, face * LANES : (face + 1) * LANES]

    def update(self, t, g):
        at = g + GROUP
        here, before, after = slice(at, at + GROUP), slice(at - 1, at - 1 + GROUP), slice(at + 1, at + 1 + GROUP)
        for f in range(self.fields):
            low, high = self.h_ref.at[0, f], self.h_ref.at[1, f]
            lift = (low[before, :] - low[here, :]) + (high[after, :] - high[here, :])
            change = self.t_ref[f, g : g + GROUP, :] + lift
            if self.factor(g) is not None:
                change = self.factor(g) * change
            self.store(t, f, g, self.load(t, f, g) + change)

    def run(self, items, ready, after, mended=(set(), set())):
        ready = set(ready)
        product, lifted, done = set(), set(), set()
        wanted = {}
        for item in items:
            for g in item.groups:
                wanted.setdefault(item.t, {})[g] = item
        coupled = 0

        def couple_next(limit):
            nonlocal coupled
            while coupled < limit and all((items[coupled].t, g) in ready for g in items[coupled].groups):
                self.couple(items[coupled])
                coupled += 1

        for index, item in enumerate(items):
            couple_next(min(index + 2, len(items)))
            assert coupled > index
            self.apply(item)
            for g in item.groups:
                lifted.add((item.t, g))
                if not item.lift_only:
                    product.add((item.t, g))
            for t, groups in wanted.items():
                for g in groups:
                    if (t, g) in done or (t, g) not in product:
                        continue
                    if all(n not in groups or (t, n) in lifted for n in (g - GROUP, g + GROUP)):
                        self.update(t, g)
                        done.add((t, g))
                        ready.add((t + 1, g))
            if mended[1] <= ready:
                ready |= mended[0]
            after(index)


class Item:
    after = None

    def __init__(self, t, slot, groups, lift_only=False):
        self.t, self.slot, self.groups, self.lift_only = t, slot, groups, lift_only


def own_pair(t, j):
    first = HALO + PAIR_ROWS * j
    return Item(t, j, (first, first + GROUP))


def hold(refs, local):
    for ref, to in zip(refs, local):
        rows, cols = ref.shape
        to[:rows, :cols] = ref[...]
    return local


def early_kernel(own_ref, wt_ref, wl_ref, ck_ref, *refs):
    ins, past, outs = refs[:5], refs[5 : 5 + EARLY], refs[5 + EARLY : 11 + EARLY]
    t_ref, h_ref, lt_ref, lu_ref, *local = refs[11 + EARLY :]
    planes, elems, _ = own_ref.shape
    fields = planes - AXES
    rows = lambda g: slice(g - HALO, g - HALO + GROUP)

    def load(t, f, g):
        return own_ref[f, rows(g), :] if t == 0 else past[t - 1][f, rows(g), :]

    def store(t, f, g, value):
        past[t][f, rows(g), :] = value

    pad = slice(HALO, HALO + GROUP), slice(elems + HALO + GROUP, elems + HALO + 2 * GROUP)
    for rim in pad:
        h_ref[:, :, rim, :] = jnp.zeros((2, fields, GROUP, LANES), F32)
    stepper = Stepper(
        fields, load, store, lambda g: None, lambda k, g: own_ref[fields + k, rows(g), :],
        wt_ref, wl_ref, ck_ref, t_ref, h_ref, lt_ref, lu_ref,
    )
    pairs = elems // PAIR_ROWS
    order = sorted(range(pairs), key=lambda j: abs(2 * j + 1 - pairs))
    items = [own_pair(t, j) for t in range(EARLY) for j in order]
    pieces = list(Order(block_index(), ins, outs, local).pieces())
    at = {(len(items) - 4) * i // len(pieces): piece for i, piece in enumerate(pieces)}

    def beside(index):
        if index in at:
            items[index + 4].after = at[index]()

    stepper.run(items, {(0, g) for item in items for g in item.groups}, beside)


def scratch(fields, elems):
    rows = elems + 2 * HALO
    tile = fields * PAIR_ROWS
    slots = rows // PAIR_ROWS + 2
    return [
        VMEM((fields, rows, LANES), F32),
        VMEM((2, fields, rows + 2 * GROUP, LANES), F32),
        VMEM((slots, tile, 6 * LANES), BF16),
        VMEM((slots, tile, 2 * LANES), BF16),
    ]


def early(own, operators, ins):
    planes, elems, _ = own.shape
    fields = planes - AXES
    width, slots = ins[-1].shape
    vmem = pl.BlockSpec(memory_space=VMEM)
    return pl.pallas_call(
        early_kernel,
        in_specs=[vmem] * (1 + len(operators) + len(ins)),
        out_shape=tuple(jax.ShapeDtypeStruct((fields, elems, LANES), F32) for _ in range(EARLY))
        + (
            jax.ShapeDtypeStruct((slots, 2 * LANES), BF16),
            jax.ShapeDtypeStruct((slots, LANES), F32),
            jax.ShapeDtypeStruct((slots, LANES), F32),
            jax.ShapeDtypeStruct((slots, slots), BF16),
            jax.ShapeDtypeStruct((slots, slots), BF16),
            jax.ShapeDtypeStruct((width, slots), F32),
        ),
        scratch_shapes=scratch(fields, elems) + [VMEM((slots, slots), BF16)] * 3,
        compiler_params=pltpu.CompilerParams(vmem_limit_bytes=32 << 20),
        cost_estimate=pl.CostEstimate(flops=5_000_000_000, bytes_accessed=4_000_000, transcendentals=0),
        name="early",
    )(own, *operators, *ins)


def march_kernel(own_ref, near_ref, far_ref, *refs, last_block):
    past = (own_ref,) + refs[:EARLY]
    wt_ref, wl_ref, ck_ref, eh_ref, wp_ref, acc0_ref, keep_ref, give_ref, rev_ref = refs[EARLY : EARLY + 9]
    edge_ref, u_ref, m_ref, t_ref, h_ref, lt_ref, lu_ref, *local = refs[EARLY + 9 :]
    wt_ref, wl_ref, ck_ref = hold((wt_ref, wl_ref, ck_ref), local)
    planes, elems, _ = own_ref.shape
    fields = planes - AXES
    slots = eh_ref.shape[0]
    end = HALO + elems
    me = block_index()
    in_low = jnp.where(me == 0, 0.0, 1.0).astype(F32)
    in_high = jnp.where(me == last_block, 0.0, 1.0).astype(F32)
    skip = HALO - STEPS
    side_rows = HALO + GROUP
    low_rim, high_rim = [skip, skip + GROUP], [end - skip, end - skip + GROUP]
    low_groups, high_groups = list(range(0, side_rows, GROUP)), list(range(end - GROUP, end + HALO, GROUP))
    own_rows = lambda g: slice(g - HALO, g - HALO + GROUP)

    def rim_rows(g):
        at = g if g < HALO + GROUP else side_rows + g - (end - GROUP)
        return slice(at, at + GROUP)

    odd = me % 2 == 1
    low_edge = lambda edge: jnp.where(odd, near_ref[edge], far_ref[edge])
    high_edge = lambda edge: jnp.where(odd, far_ref[edge], near_ref[edge])
    spare = jnp.zeros((skip, LANES), F32)
    for f in range(fields):
        edge = slice(f * STEPS, (f + 1) * STEPS)
        low = jnp.where(me > 0, low_edge(edge), 0.0)
        high = jnp.where(me < last_block, high_edge(edge), 0.0)
        edge_ref[0, f, :side_rows, :] = jnp.concatenate([spare, low, own_ref[f, :GROUP, :]], axis=0)
        edge_ref[0, f, side_rows:, :] = jnp.concatenate([own_ref[f, elems - GROUP :, :], high, spare], axis=0)
    edge_ref[EARLY] = jnp.zeros(edge_ref.shape[1:], F32)
    edge = slice(fields * STEPS, (fields + 1) * STEPS)
    low_factors, high_factors = low_edge(edge), high_edge(edge)
    for k in range(AXES):
        lane = k * (LANES // AXES)
        spread = lambda x: jnp.broadcast_to(x[:, lane : lane + 1], (STEPS, LANES))
        own_low, own_high = own_ref[fields + k, :GROUP, :], own_ref[fields + k, elems - GROUP :, :]
        m_ref[k, :side_rows, :] = jnp.concatenate([spare, spread(low_factors), own_low], axis=0)
        m_ref[k, side_rows:, :] = jnp.concatenate([own_high, spread(high_factors), spare], axis=0)
    h_ref[:, :, :PAIR_ROWS, :] = jnp.zeros((2, fields, PAIR_ROWS, LANES), F32)
    h_ref[:, :, end + GROUP + HALO - GROUP :, :] = jnp.zeros((2, fields, PAIR_ROWS, LANES), F32)
    half = slots // 2
    keep_ref[...] = acc0_ref[:half]
    give_ref[...] = acc0_ref[half:]
    rev_ref[...] = jnp.zeros(rev_ref.shape, F32)

    def load(t, f, g):
        if t > EARLY:
            return u_ref[t % 2, f, g : g + GROUP, :]
        if t == EARLY and g in low_groups + high_groups or g in low_rim + high_rim:
            return edge_ref[t, f, rim_rows(g), :]
        return past[t][f, own_rows(g), :]

    def store(t, f, g, value):
        if t >= EARLY:
            u_ref[(t + 1) % 2, f, g : g + GROUP, :] = value
            return
        row = iota((GROUP, LANES), 0)
        if g == low_rim[1]:
            rest = past[t + 1][f, : GROUP - skip, :]
            value = jnp.where(row <= skip + t, value, jnp.concatenate([rest[:skip], rest], axis=0))
            if t == EARLY - 1:
                edge_ref[EARLY, f, side_rows - skip : side_rows, :] = past[t + 1][f, GROUP - skip : GROUP, :]
        if g == high_rim[0]:
            rest = past[t + 1][f, elems - (GROUP - skip) :, :]
            value = jnp.where(row >= GROUP - skip - 1 - t, value, jnp.concatenate([rest, rest[:skip]], axis=0))
            if t == EARLY - 1:
                at = elems - GROUP
                edge_ref[EARLY, f, side_rows : side_rows + skip, :] = past[t + 1][f, at : at + skip, :]
        edge_ref[t + 1, f, rim_rows(g), :] = value

    def metric(k, g):
        if g < HALO or g > end - GROUP:
            return m_ref[k, rim_rows(g), :]
        return own_ref[fields + k, own_rows(g), :]

    def factor(g):
        if g + GROUP <= HALO:
            return in_low
        if g >= end:
            return in_high
        if g < HALO:
            return jnp.where(iota((GROUP, LANES), 0) < HALO - g, in_low, 1.0)
        if g + GROUP > end:
            return jnp.where(iota((GROUP, LANES), 0) >= end - g, in_high, 1.0)
        return None

    def own_load(t, f, g):
        if t < EARLY and g in (HALO, end - GROUP):
            rest, row = past[t][f, own_rows(g), :], iota((GROUP, LANES), 0)
            mended = edge_ref[t, f, rim_rows(g), :]
            return jnp.where(row < t, mended, rest) if g == HALO else jnp.where(row >= GROUP - t, mended, rest)
        return load(t, f, g)

    def sample(t):
        field = lambda f: jnp.concatenate([own_load(t + 1, f, g) for g in range(HALO, end, GROUP)], axis=0)
        columns = []
        for c in range(COMPS):
            x = field(c) if c < 3 else (field(3) + field(4) + field(5)) / 3.0
            columns.append(jnp.concatenate(split2(x), axis=0))
        lane = iota((slots, LANES), 1)
        send = jnp.concatenate([keep_ref[...], give_ref[...]], axis=0)
        rev = rev_ref[...]
        for c in range(0, COMPS, 2):
            found = dot(eh_ref[...], jnp.concatenate(columns[c : c + 2], axis=1))
            for i in range(2):
                value = jnp.sum(found[:, i * LANES : (i + 1) * LANES] * wp_ref[...], axis=1, keepdims=True)
                send = jnp.where(lane == (c + i) * STEPS + t, value, send)
                rev = jnp.where(lane == OBS_LANE + (c + i) * STEPS + (STEPS - 1) - t, value, rev)
        keep_ref[...] = send[:half]
        give_ref[...] = send[half:]
        rev_ref[...] = rev

    pairs = elems // PAIR_ROWS
    order = sorted(range(pairs), key=lambda j: abs(2 * j + 1 - pairs))
    inner, outer = order[:-2], order[-2:]
    ring_rows = lambda ring: (HALO - GROUP * (ring + 1), end + GROUP * ring)
    items, samples = [], {}
    fill = -(-len(inner) // EARLY)
    for t in range(EARLY):
        items += [Item(t, pairs, (low_rim[1], high_rim[0])), Item(t, pairs + 1, (low_rim[0], high_rim[1]))]
        items += [own_pair(EARLY, j) for j in inner[t * fill : (t + 1) * fill]]
        if t >= 1:
            samples[len(items) - 1] = t - 1
    for t in range(EARLY, STEPS):
        items += [own_pair(t, j) for j in (outer if t == EARLY else order)]
        if t > EARLY:
            samples[len(items) - len(order) + 3] = t - 1
        for ring in range(HALO // GROUP):
            if ring * GROUP < STEPS - t:
                items.append(Item(t, pairs + ring, ring_rows(ring), lift_only=ring * GROUP >= STEPS - 1 - t))
        if t == EARLY:
            samples[len(items) - 2] = EARLY - 1
    ready = {(0, g) for g in low_rim + high_rim}
    ready |= {(EARLY, g) for g in range(HALO + GROUP, end - GROUP, GROUP)}
    mended = {(EARLY, g) for g in low_groups + high_groups}, {(EARLY, g) for g in low_rim + high_rim}
    stepper = Stepper(
        fields, load, store, factor, metric, wt_ref, wl_ref, ck_ref, t_ref, h_ref, lt_ref, lu_ref
    )
    stepper.run(items, ready, lambda index: sample(samples[index]) if index in samples else None, mended)
    sample(STEPS - 1)


def march(own, near, far, past, ops, last_block):
    eh = ops[3]
    planes, elems, _ = own.shape
    fields = planes - AXES
    slots = eh.shape[0]
    vmem = pl.BlockSpec(memory_space=VMEM)
    return pl.pallas_call(
        functools.partial(march_kernel, last_block=last_block),
        in_specs=[vmem] * (3 + EARLY + len(ops)),
        out_shape=(
            jax.ShapeDtypeStruct((slots // 2, LANES), F32),
            jax.ShapeDtypeStruct((slots // 2, LANES), F32),
            jax.ShapeDtypeStruct((slots, LANES), F32),
        ),
        scratch_shapes=[
            VMEM((EARLY + 1, fields, 2 * (HALO + GROUP), LANES), F32),
            VMEM((2, fields, elems + 2 * HALO, LANES), F32),
            VMEM((AXES, 2 * (HALO + GROUP), LANES), F32),
        ]
        + scratch(fields, elems)
        + [VMEM((6 * LANES, 2 * LANES), BF16), VMEM((3 * LANES, 2 * LANES), BF16), VMEM((2 * LANES, 2 * LANES), BF16)],
        compiler_params=pltpu.CompilerParams(vmem_limit_bytes=40 << 20),
        cost_estimate=pl.CostEstimate(flops=20_000_000_000, bytes_accessed=4_000_000, transcendentals=0),
        name="march",
    )(own, near, far, *past, *ops)


def pack_kernel(keep_ref, given_ref, out_ref):
    chips = keep_ref.shape[0] // 2
    for other, ref in enumerate((keep_ref, given_ref)):
        for which in range(2):
            out_ref[pl.ds(2 * other + which, chips, stride=4), :] = ref[which * chips : (which + 1) * chips, :]


def pack(keep, given):
    return pl.pallas_call(
        pack_kernel,
        out_shape=jax.ShapeDtypeStruct((2 * keep.shape[0], LANES), F32),
        compiler_params=pltpu.CompilerParams(vmem_limit_bytes=4 << 20),
        name="pack",
    )(keep, given)


def finish_kernel(
    got_ref, rev_ref, to_slot_ref, to_pos_ref, seen_ref, res_hbm, mis_hbm, adj_hbm, res_ref, mis_ref, adj_ref, sems
):
    width, slots = seen_ref.shape
    chips = slots // 4
    got = jnp.concatenate([got_ref[pl.ds(i, chips, stride=4), :] for i in range(4)], axis=0)
    lane = iota(got.shape, 1)
    turned = jnp.where(lane < OBS_LANE, got, rev_ref[...] - got).T

    def place(rows, onehot):
        found = dot(jnp.concatenate(split2(rows), axis=0), onehot)
        return found[:width] + found[width:]

    residual = place(turned[:width], to_pos_ref[...]) - seen_ref[...]
    res_ref[...] = residual
    mis_ref[...] = 0.5 * jnp.sum(residual * residual, axis=0, keepdims=True)
    adj_ref[...] = place(turned[OBS_LANE : OBS_LANE + width], to_slot_ref[...])
    pairs = ((res_ref, res_hbm), (adj_ref, adj_hbm), (mis_ref, mis_hbm))
    copies = [pltpu.make_async_copy(here, out, sems.at[i]) for i, (here, out) in enumerate(pairs)]
    for copy in copies:
        copy.start()
    for copy in copies:
        copy.wait()


def finish(got, rev, to_slot, to_pos, seen):
    width, slots = seen.shape
    vmem = pl.BlockSpec(memory_space=VMEM)
    hbm = pl.BlockSpec(memory_space=pltpu.HBM)
    shapes = ((width, slots), (1, slots), (width, slots))
    return pl.pallas_call(
        finish_kernel,
        in_specs=[vmem] * 5,
        out_specs=(hbm, hbm, hbm),
        out_shape=tuple(jax.ShapeDtypeStruct(shape, F32) for shape in shapes),
        scratch_shapes=[VMEM(shape, F32) for shape in shapes] + [pltpu.SemaphoreType.DMA((3,))],
        compiler_params=pltpu.CompilerParams(vmem_limit_bytes=8 << 20),
        name="finish",
    )(got, rev, to_slot, to_pos, seen)


def shards(
    initial,
    derivative,
    coupling,
    face_lift,
    metric,
    rec_element,
    rec_weight,
    live_counts,
    shot_order,
    observed,
):
    blocks = lax.axis_size(MX)
    slots = rec_element.shape[0]
    order, element, lives = (x.reshape(-1, LANES) for x in (shot_order, rec_element, live_counts))
    staged = (derivative, rec_weight, order, element, lives, observed.T)
    own, near, far, derivative, rec_weight, order, element, lives, observed = turn(initial, metric, staged)
    pairs = [(i, min(i + 1, blocks - 1) if i % 2 else max(i - 1, 0)) for i in range(blocks)]
    far = lax.ppermute(far, MX, pairs)
    near = lax.ppermute(near, MX, [(i, i ^ 1) for i in range(blocks)])
    ops = operators(derivative, coupling, face_lift)
    outs = early(own, ops, (lives, element, rec_weight, order, observed))
    past, eh, wp, acc0, to_slot, to_pos, seen = (outs[:EARLY],) + tuple(outs[EARLY:])
    keep, give, rev = march(own, near, far, past, (*ops, eh, wp, acc0), blocks - 1)
    given = lax.ppermute(give, MX, [(i, i ^ 1) for i in range(blocks)])
    rows = pack(keep, given).reshape(blocks // 2, 4, LANES)
    got = lax.all_to_all(rows, MX[:2], split_axis=0, concat_axis=0, tiled=True)
    residual, misfit, adjoint = finish(got.reshape(slots, LANES), rev, to_slot, to_pos, seen)
    return (residual.T, misfit.reshape(slots), adjoint.T)


def solution(mesh):
    split = Mesh(
        mesh.devices.reshape(mesh.shape["shots"], 8, 8, 2), ("shots", "mx_0", "mx_1", "mx_2")
    )
    in_specs = (
        P("shots", None, MX),
        P(),
        P(),
        P(),
        P(None, MX),
        P(MX),
        P(None, MX),
        P(),
        P(),
        P(SHOTS_MX, None),
    )
    out_specs = (P(SHOTS_MX, None), P(SHOTS_MX), P(SHOTS_MX, None))
    return jax.shard_map(
        shards, mesh=split, in_specs=in_specs, out_specs=out_specs, check_vma=False
    )
```

```python
import functools

import jax
import jax.numpy as jnp
from jax import lax
from jax.experimental import pallas as pl
from jax.experimental.pallas import tpu as pltpu
from jax.sharding import Mesh
from jax.sharding import PartitionSpec as P


STEPS = 12
EARLY = 3
DT = 0.5 / STEPS
AXES = 3
COMPS = 4
MX = ("mx_0", "mx_1", "mx_2")
SHOTS_MX = ("shots", "mx_0", "mx_1", "mx_2")
F32 = jnp.float32
BF16 = jnp.bfloat16
I32 = jnp.int32
LANES = 128
GROUP = 8
PAIR_ROWS = 2 * GROUP
HALO = 16
WHOLE = 32
OBS_LANE = 64
VMEM = pltpu.VMEM


def iota(shape, dim):
    return lax.broadcasted_iota(I32, shape, dim)


def split2(x):
    hi = x.astype(BF16)
    return hi, (x - hi.astype(F32)).astype(BF16)


def dot(a, b):
    return jnp.dot(a, b, preferred_element_type=F32)


def block_index():
    index = 0
    for axis in MX:
        index = index * lax.axis_size(axis) + lax.axis_index(axis)
    return index


def whole(rows):
    return -(-rows // WHOLE) * WHOLE


def padded(x, rows, cols):
    if x.shape[1] < cols:
        x = jnp.concatenate([x, jnp.zeros((x.shape[0], cols - x.shape[1]), x.dtype)], axis=1)
    if x.shape[0] < rows:
        x = jnp.concatenate([x, jnp.zeros((rows - x.shape[0], cols), x.dtype)], axis=0)
    return x


def turn_kernel(*refs):
    staged = (len(refs) - 10) // 2
    initial_hbm, metric_hbm = refs[:2]
    from_refs = refs[2 : 2 + staged]
    own_ref, near_ref, far_ref = refs[2 + staged : 5 + staged]
    to_refs = refs[5 + staged : 5 + 2 * staged]
    initial_ref, metric_ref, low_ref, high_ref, sems = refs[-5:]
    fields, _, elems = initial_ref.shape
    pairs = [(initial_hbm, initial_ref), (metric_hbm, metric_ref)]
    pairs += [(x, y if x.shape == y.shape else y.at[: x.shape[0]]) for x, y in zip(from_refs, to_refs)]
    copies = [pltpu.make_async_copy(x, y, sems.at[i]) for i, (x, y) in enumerate(pairs)]
    for copy in copies:
        copy.start()
    copies[0].wait()
    copies[1].wait()
    for f in range(fields):
        own_ref[f] = padded(initial_ref[f], LANES, elems).T
    for k in range(metric_ref.shape[0]):
        own_ref[fields + k] = jnp.broadcast_to(metric_ref[k : k + 1, :], (LANES, elems)).T
    third = iota((elems, LANES), 1) // (LANES // 3)
    factors = jnp.where(third == 0, own_ref[fields], jnp.where(third == 1, own_ref[fields + 1], own_ref[fields + 2]))
    for edge_ref, rows in ((low_ref, slice(0, STEPS)), (high_ref, slice(elems - STEPS, elems))):
        for f in range(fields):
            edge_ref[f * STEPS : (f + 1) * STEPS, :] = own_ref[f, rows, :]
        edge_ref[fields * STEPS : (fields + 1) * STEPS, :] = factors[rows]
        edge_ref[(fields + 1) * STEPS :, :] = jnp.zeros((edge_ref.shape[0] - (fields + 1) * STEPS, LANES), F32)
    odd = block_index() % 2 == 1
    near_ref[...] = jnp.where(odd, low_ref[...], high_ref[...])
    far_ref[...] = jnp.where(odd, high_ref[...], low_ref[...])
    for copy in copies[2:]:
        copy.wait()


def turn(initial, metric, staged):
    fields, _, elems = initial.shape
    planes = fields + metric.shape[0]
    edge = jax.ShapeDtypeStruct((whole((fields + 1) * STEPS), LANES), F32)
    hbm = pl.BlockSpec(memory_space=pltpu.HBM)
    return pl.pallas_call(
        turn_kernel,
        in_specs=[hbm] * (2 + len(staged)),
        out_shape=(jax.ShapeDtypeStruct((planes, elems, LANES), F32), edge, edge)
        + tuple(jax.ShapeDtypeStruct((whole(x.shape[0]),) + x.shape[1:] if x.shape[0] < GROUP and x.ndim == 2 else x.shape, x.dtype) for x in staged),
        scratch_shapes=[
            VMEM(initial.shape, F32),
            VMEM(metric.shape, F32),
            VMEM(edge.shape, F32),
            VMEM(edge.shape, F32),
            pltpu.SemaphoreType.DMA((2 + len(staged),)),
        ],
        compiler_params=pltpu.CompilerParams(vmem_limit_bytes=8 << 20),
        name="turn",
    )(*(pltpu.with_memory_space_constraint(x, pltpu.HBM) for x in (initial, metric, *staged)))


def operators_kernel(derivative_ref, coupling_ref, lift_ref, wt_ref, wl_ref, ck_ref):
    fields = coupling_ref.shape[1]
    dh, dl = zip(*(split2(padded(DT * derivative_ref[k], LANES, LANES).T) for k in range(AXES)))
    zero = jnp.zeros((LANES, LANES), BF16)
    for row, (left, right) in enumerate(
        [(dh[0], dl[0]), (dh[1], dl[1]), (dh[2], dl[2]), (dh[2], zero), (dh[0], zero), (dh[1], zero)]
    ):
        wt_ref[row * LANES : (row + 1) * LANES, :] = jnp.concatenate([left, right], axis=1)
    l0h, l0l = split2(padded(DT * lift_ref[0], LANES, LANES).T)
    l1h, l1l = split2(padded(DT * lift_ref[1], LANES, LANES).T)
    for row, (left, right) in enumerate([(l0h, l1h), (l0h, l1h), (l0l, l1l)]):
        wl_ref[row * LANES : (row + 1) * LANES, :] = jnp.concatenate([left, right], axis=1)
    rows, cols = AXES * fields * GROUP, fields * GROUP
    spread_rows = (iota((rows, AXES * fields), 0) // GROUP == iota((rows, AXES * fields), 1)).astype(BF16)
    spread_cols = (iota((fields, cols), 0) == iota((fields, cols), 1) // GROUP).astype(BF16)
    hi, lo = split2(jnp.concatenate([coupling_ref[k] for k in range(AXES)], axis=0))
    full = dot(dot(spread_rows, hi).astype(BF16), spread_cols) + dot(dot(spread_rows, lo).astype(BF16), spread_cols)
    full = jnp.where(iota((rows, cols), 0) % GROUP == iota((rows, cols), 1) % GROUP, full, 0.0)
    full_hi = full.astype(BF16).astype(F32)
    spread = padded(jnp.concatenate([full_hi, full_hi, full - full_hi], axis=1), *ck_ref.shape)
    ck_ref[...] = spread.astype(BF16)


def operators(derivative, coupling, face_lift):
    fields = coupling.shape[1]
    block = AXES * fields * GROUP
    return pl.pallas_call(
        operators_kernel,
        out_shape=(
            jax.ShapeDtypeStruct((6 * LANES, 2 * LANES), BF16),
            jax.ShapeDtypeStruct((3 * LANES, 2 * LANES), BF16),
            jax.ShapeDtypeStruct((whole(block), 2 * LANES), BF16),
        ),
        compiler_params=pltpu.CompilerParams(vmem_limit_bytes=8 << 20),
        cost_estimate=pl.CostEstimate(flops=1_000_000_000, bytes_accessed=1_000_000, transcendentals=0),
        name="operators",
    )(derivative, coupling, face_lift)


class Order:
    def __init__(self, me, ins, outs, local):
        self.me = me
        self.lives_ref, self.element_ref, self.weight_ref, self.order_ref, self.observed_ref = ins
        self.eh_ref, self.wp_ref, self.acc_ref, self.to_slot_ref, self.to_pos_ref, self.seen_ref = outs
        self.place_ref, self.weight_parts_ref, self.observed_parts_ref = local
        self.width, self.slots = self.observed_ref.shape
        self.chips = self.slots // 4
        self.big = float(self.slots * self.slots)
        self.bits = self.slots.bit_length() - 1
        assert self.slots == 1 << self.bits
        self.odd = me & 1

    def pieces(self):
        yield from (functools.partial(self.slot_rows, 0), self.weights, functools.partial(self.slot_rows, 1))
        yield from (self.observations, functools.partial(self.position_rows, 0), self.place_weights)
        yield from (functools.partial(self.position_rows, 1), self.seen, self.place_observations)

    def rows(self, other, which):
        start = (2 * other + which) * self.chips
        return slice(start, start + self.chips)

    def across(self, ref):
        return jnp.concatenate([ref[0:1, :], ref[1:2, :]], axis=1)

    def live_of(self, block):
        lives = self.lives_ref[:1, :]
        there = block == iota((block.shape[0], lives.shape[1]), 1)
        return jnp.sum(jnp.where(there, lives.astype(F32), 0.0), axis=1, keepdims=True)

    def slot_rows(self, other):
        slots, chips = self.slots, self.chips
        first, last = None, None
        for half in range(2):
            core = [self.order_ref[pl.ds(2 * core + half, chips, stride=4), :] for core in range(2)]
            order = jnp.where(self.odd == 1 - other, core[1], core[0])
            key = (((half * LANES + iota(order.shape, 1)) << self.bits) + (order & (slots - 1))).astype(F32)
            mine = (order >> self.bits) == self.me
            low, high = jnp.where(mine, key, self.big), jnp.where(mine, key, -1.0)
            first = low if first is None else jnp.minimum(first, low)
            last = high if last is None else jnp.maximum(last, high)
        found = jnp.min(first, axis=1, keepdims=True), jnp.max(last, axis=1, keepdims=True)
        live_slot = iota((1, slots), 1).astype(F32) < self.live_of(jnp.full((1, 1), self.me, I32))
        element = self.across(self.element_ref).astype(F32)
        done = 0.0
        for which in range(2):
            rows = self.rows(other, which)
            hot = (found[which].astype(I32) & (slots - 1)) == iota((chips, slots), 1)
            self.to_slot_ref[rows, :] = jnp.where(hot & live_slot, 1.0, 0.0).astype(BF16)
            element_of = jnp.sum(jnp.where(hot, element, 0.0), axis=1, keepdims=True)
            hit = (element_of.astype(I32) == iota((chips, LANES), 1)).astype(BF16)
            self.eh_ref[rows, :] = jnp.concatenate([hit, hit], axis=1)
            done = done + element_of[:GROUP]
        return jnp.broadcast_to(done, (GROUP, LANES))

    def position_rows(self, other):
        slots, shape = self.slots, (self.chips, self.slots)
        mine = self.order_ref[pl.ds(2 * self.me, 2), :]
        mine = jnp.concatenate([mine[0:1], mine[1:2]], axis=1)
        block = 2 * iota((self.chips, 1), 0) + jnp.where(self.odd == 1 - other, 1, 0)
        col = iota(shape, 1).astype(F32)
        here = (mine >> self.bits) == block
        found = (
            jnp.min(jnp.where(here, col, self.big), axis=1, keepdims=True),
            jnp.max(jnp.where(here, col, -1.0), axis=1, keepdims=True),
        )
        live = self.live_of(block)
        slot = (mine & (slots - 1)).astype(F32)
        done = 0.0
        for which in range(2):
            rows = self.rows(other, which)
            hot = found[which] == col
            self.place_ref[rows, :] = hot.astype(BF16)
            slot_of = jnp.sum(jnp.where(hot, slot, 0.0), axis=1, keepdims=True)
            self.to_pos_ref[rows, :] = jnp.where(hot & (slot_of < live), 1.0, 0.0).astype(BF16)
            done = done + slot_of[:GROUP]
        return jnp.broadcast_to(done, (GROUP, LANES))

    def weights(self):
        weight = padded(self.weight_ref[...], LANES, self.slots).T
        self.weight_parts_ref[...] = jnp.concatenate(split2(weight), axis=1)

    def place_weights(self):
        both = dot(self.to_slot_ref[...], self.weight_parts_ref[...])
        self.wp_ref[...] = both[:, :LANES] + both[:, LANES:]

    def observations(self):
        lane, time = iota((LANES, self.width), 0) - OBS_LANE, iota((LANES, self.width), 1)
        comp = time // STEPS
        turned = (lane == comp * STEPS + (STEPS - 1 - (time - comp * STEPS))).astype(BF16)
        parts = [dot(turned, part).astype(BF16) for part in split2(self.observed_ref[...])]
        self.observed_parts_ref[...] = jnp.concatenate(parts, axis=0)

    def place_observations(self):
        parts = self.observed_parts_ref[...]
        both = lax.dot_general(self.place_ref[...], parts, (((1,), (1,)), ((), ())), preferred_element_type=F32)
        self.acc_ref[...] = both[:, :LANES] + both[:, LANES:]

    def seen(self):
        live = jnp.sum(self.to_pos_ref[...].astype(F32), axis=0, keepdims=True)
        self.seen_ref[...] = self.observed_ref[...] * live


class Stepper:
    def __init__(self, fields, load, store, factor, metric, wt_ref, wl_ref, ck_ref, t_ref, h_ref, lt_ref, lu_ref):
        self.fields, self.load, self.store, self.factor, self.metric = fields, load, store, factor, metric
        self.wt_ref, self.wl_ref, self.ck_ref = wt_ref, wl_ref, ck_ref
        self.t_ref, self.h_ref, self.lt_ref, self.lu_ref = t_ref, h_ref, lt_ref, lu_ref

    def split(self, item):
        halves = ([], [])
        for f in range(self.fields):
            x = jnp.concatenate([self.load(item.t, f, g) for g in item.groups], axis=0)
            hi, lo = split2(x)
            rows = slice(f * PAIR_ROWS, (f + 1) * PAIR_ROWS)
            self.lu_ref[item.slot, rows, :LANES] = hi
            self.lu_ref[item.slot, rows, LANES:] = lo
            hi32 = hi.astype(F32)
            lo32 = x - hi32
            for side in range(2):
                part = slice(side * GROUP, (side + 1) * GROUP)
                halves[side].append((hi32[part], lo32[part]))
        return halves

    def couple(self, item):
        columns = []
        for side in self.split(item):
            his, los = [p[0] for p in side], [p[1] for p in side]
            columns.append(jnp.concatenate(his + los + his, axis=0).astype(BF16))
        if item.lift_only:
            return
        size = 3 * self.fields * GROUP
        v = dot(self.ck_ref[:size, :size], jnp.concatenate(columns, axis=1))
        for k in range(AXES):
            scale = [self.metric(k, g) for g in item.groups]
            if item.after is not None:
                scale = [x + 0.0 * item.after for x in scale]
            parts = []
            for f in range(self.fields):
                base = (k * self.fields + f) * GROUP
                for side in range(2):
                    parts.append(v[base : base + GROUP, side * LANES : (side + 1) * LANES] * scale[side])
            for lane, part in zip(((0, 4), (1, 5), (2, 3))[k], split2(jnp.concatenate(parts, axis=0))):
                self.lt_ref[item.slot, :, lane * LANES : (lane + 1) * LANES] = part

    def apply(self, item):
        lu = self.lu_ref.at[item.slot]
        if not item.lift_only:
            both = dot(self.lt_ref[item.slot], self.wt_ref[...])
        lifted = dot(lu[...], self.wl_ref[: 2 * LANES, :]) + dot(lu[:, :LANES], self.wl_ref[2 * LANES :, :])
        for f in range(self.fields):
            for side, g in enumerate(item.groups):
                rows = slice(f * PAIR_ROWS + side * GROUP, f * PAIR_ROWS + (side + 1) * GROUP)
                faces = [lifted[rows, face * LANES : (face + 1) * LANES] for face in range(2)]
                if not item.lift_only:
                    total = both[rows, :LANES] + both[rows, LANES:]
                    self.t_ref[f, g : g + GROUP, :] = total - (faces[0] + faces[1])
                for face in range(2):
                    at = g + GROUP
                    self.h_ref[face, f, at : at + GROUP, :] = faces[face]

    def update(self, t, g):
        before, after = slice(g + GROUP - 1, g + 2 * GROUP - 1), slice(g + GROUP + 1, g + 2 * GROUP + 1)
        for f in range(self.fields):
            lift = self.h_ref[0, f, before, :] + self.h_ref[1, f, after, :]
            change = self.t_ref[f, g : g + GROUP, :] + lift
            if self.factor(g) is not None:
                change = self.factor(g) * change
            self.store(t, f, g, self.load(t, f, g) + change)

    def run(self, items, ready, after, mended=(set(), set())):
        ready = set(ready)
        product, lifted, done = set(), set(), set()
        wanted = {}
        for item in items:
            for g in item.groups:
                wanted.setdefault(item.t, {})[g] = item
        coupled = 0

        def couple_next(limit):
            nonlocal coupled
            while coupled < limit and all((items[coupled].t, g) in ready for g in items[coupled].groups):
                self.couple(items[coupled])
                coupled += 1

        for index, item in enumerate(items):
            couple_next(min(index + 2, len(items)))
            assert coupled > index
            self.apply(item)
            for g in item.groups:
                lifted.add((item.t, g))
                if not item.lift_only:
                    product.add((item.t, g))
            for t, groups in wanted.items():
                for g in groups:
                    if (t, g) in done or (t, g) not in product:
                        continue
                    if all(n not in groups or (t, n) in lifted for n in (g - GROUP, g + GROUP)):
                        self.update(t, g)
                        done.add((t, g))
                        ready.add((t + 1, g))
            if mended[1] <= ready:
                ready |= mended[0]
            after(index)


class Item:
    after = None

    def __init__(self, t, slot, groups, lift_only=False):
        self.t, self.slot, self.groups, self.lift_only = t, slot, groups, lift_only


def own_pair(t, j):
    first = HALO + PAIR_ROWS * j
    return Item(t, j, (first, first + GROUP))


def hold(refs, local):
    for ref, to in zip(refs, local):
        rows, cols = ref.shape
        to[:rows, :cols] = ref[...]
    return local


def early_kernel(own_ref, wt_ref, wl_ref, ck_ref, *refs):
    ins, past, outs = refs[:5], refs[5 : 5 + EARLY], refs[5 + EARLY : 11 + EARLY]
    t_ref, h_ref, lt_ref, lu_ref, *local = refs[11 + EARLY :]
    planes, elems, _ = own_ref.shape
    fields = planes - AXES
    rows = lambda g: slice(g - HALO, g - HALO + GROUP)

    def load(t, f, g):
        return own_ref[f, rows(g), :] if t == 0 else past[t - 1][f, rows(g), :]

    def store(t, f, g, value):
        past[t][f, rows(g), :] = value

    pad = slice(HALO, HALO + GROUP), slice(elems + HALO + GROUP, elems + HALO + 2 * GROUP)
    for rim in pad:
        h_ref[:, :, rim, :] = jnp.zeros((2, fields, GROUP, LANES), F32)
    stepper = Stepper(
        fields, load, store, lambda g: None, lambda k, g: own_ref[fields + k, rows(g), :],
        wt_ref, wl_ref, ck_ref, t_ref, h_ref, lt_ref, lu_ref,
    )
    pairs = elems // PAIR_ROWS
    order = sorted(range(pairs), key=lambda j: abs(2 * j + 1 - pairs))
    items = [own_pair(t, j) for t in range(EARLY) for j in order]
    pieces = list(Order(block_index(), ins, outs, local).pieces())
    at = {(len(items) - 4) * i // len(pieces): piece for i, piece in enumerate(pieces)}

    def beside(index):
        if index in at:
            items[index + 4].after = at[index]()

    stepper.run(items, {(0, g) for item in items for g in item.groups}, beside)


def scratch(fields, elems):
    rows = elems + 2 * HALO
    tile = fields * PAIR_ROWS
    slots = rows // PAIR_ROWS + 2
    return [
        VMEM((fields, rows, LANES), F32),
        VMEM((2, fields, rows + 2 * GROUP, LANES), F32),
        VMEM((slots, tile, 6 * LANES), BF16),
        VMEM((slots, tile, 2 * LANES), BF16),
    ]


def early(own, operators, ins):
    planes, elems, _ = own.shape
    fields = planes - AXES
    width, slots = ins[-1].shape
    vmem = pl.BlockSpec(memory_space=VMEM)
    return pl.pallas_call(
        early_kernel,
        in_specs=[vmem] * (1 + len(operators) + len(ins)),
        out_shape=tuple(jax.ShapeDtypeStruct((fields, elems, LANES), F32) for _ in range(EARLY))
        + (
            jax.ShapeDtypeStruct((slots, 2 * LANES), BF16),
            jax.ShapeDtypeStruct((slots, LANES), F32),
            jax.ShapeDtypeStruct((slots, LANES), F32),
            jax.ShapeDtypeStruct((slots, slots), BF16),
            jax.ShapeDtypeStruct((slots, slots), BF16),
            jax.ShapeDtypeStruct((width, slots), F32),
        ),
        scratch_shapes=scratch(fields, elems) + [VMEM((slots, slots), BF16)] * 3,
        compiler_params=pltpu.CompilerParams(vmem_limit_bytes=32 << 20),
        cost_estimate=pl.CostEstimate(flops=5_000_000_000, bytes_accessed=4_000_000, transcendentals=0),
        name="early",
    )(own, *operators, *ins)


def march_kernel(own_ref, near_ref, far_ref, *refs, last_block):
    past = (own_ref,) + refs[:EARLY]
    wt_ref, wl_ref, ck_ref, eh_ref, wp_ref, acc0_ref, keep_ref, give_ref, rev_ref = refs[EARLY : EARLY + 9]
    edge_ref, u_ref, m_ref, t_ref, h_ref, lt_ref, lu_ref, *local = refs[EARLY + 9 :]
    wt_ref, wl_ref, ck_ref = hold((wt_ref, wl_ref, ck_ref), local)
    planes, elems, _ = own_ref.shape
    fields = planes - AXES
    slots = eh_ref.shape[0]
    end = HALO + elems
    me = block_index()
    in_low = jnp.where(me == 0, 0.0, 1.0).astype(F32)
    in_high = jnp.where(me == last_block, 0.0, 1.0).astype(F32)
    skip = HALO - STEPS
    side_rows = HALO + GROUP
    low_rim, high_rim = [skip, skip + GROUP], [end - skip, end - skip + GROUP]
    low_groups, high_groups = list(range(0, side_rows, GROUP)), list(range(end - GROUP, end + HALO, GROUP))
    own_rows = lambda g: slice(g - HALO, g - HALO + GROUP)

    def rim_rows(g):
        at = g if g < HALO + GROUP else side_rows + g - (end - GROUP)
        return slice(at, at + GROUP)

    odd = me % 2 == 1
    low_edge = lambda edge: jnp.where(odd, near_ref[edge], far_ref[edge])
    high_edge = lambda edge: jnp.where(odd, far_ref[edge], near_ref[edge])
    spare = jnp.zeros((skip, LANES), F32)
    for f in range(fields):
        edge = slice(f * STEPS, (f + 1) * STEPS)
        low = jnp.where(me > 0, low_edge(edge), 0.0)
        high = jnp.where(me < last_block, high_edge(edge), 0.0)
        edge_ref[0, f, :side_rows, :] = jnp.concatenate([spare, low, own_ref[f, :GROUP, :]], axis=0)
        edge_ref[0, f, side_rows:, :] = jnp.concatenate([own_ref[f, elems - GROUP :, :], high, spare], axis=0)
    edge_ref[EARLY] = jnp.zeros(edge_ref.shape[1:], F32)
    edge = slice(fields * STEPS, (fields + 1) * STEPS)
    low_factors, high_factors = low_edge(edge), high_edge(edge)
    for k in range(AXES):
        lane = k * (LANES // AXES)
        spread = lambda x: jnp.broadcast_to(x[:, lane : lane + 1], (STEPS, LANES))
        own_low, own_high = own_ref[fields + k, :GROUP, :], own_ref[fields + k, elems - GROUP :, :]
        m_ref[k, :side_rows, :] = jnp.concatenate([spare, spread(low_factors), own_low], axis=0)
        m_ref[k, side_rows:, :] = jnp.concatenate([own_high, spread(high_factors), spare], axis=0)
    h_ref[:, :, :PAIR_ROWS, :] = jnp.zeros((2, fields, PAIR_ROWS, LANES), F32)
    h_ref[:, :, end + GROUP + HALO - GROUP :, :] = jnp.zeros((2, fields, PAIR_ROWS, LANES), F32)
    half = slots // 2
    keep_ref[...] = acc0_ref[:half]
    give_ref[...] = acc0_ref[half:]
    rev_ref[...] = jnp.zeros(rev_ref.shape, F32)

    def load(t, f, g):
        if t > EARLY:
            return u_ref[t % 2, f, g : g + GROUP, :]
        if t == EARLY and g in low_groups + high_groups or g in low_rim + high_rim:
            return edge_ref[t, f, rim_rows(g), :]
        return past[t][f, own_rows(g), :]

    def store(t, f, g, value):
        if t >= EARLY:
            u_ref[(t + 1) % 2, f, g : g + GROUP, :] = value
            return
        row = iota((GROUP, LANES), 0)
        if g == low_rim[1]:
            rest = past[t + 1][f, : GROUP - skip, :]
            value = jnp.where(row <= skip + t, value, jnp.concatenate([rest[:skip], rest], axis=0))
            if t == EARLY - 1:
                edge_ref[EARLY, f, side_rows - skip : side_rows, :] = past[t + 1][f, GROUP - skip : GROUP, :]
        if g == high_rim[0]:
            rest = past[t + 1][f, elems - (GROUP - skip) :, :]
            value = jnp.where(row >= GROUP - skip - 1 - t, value, jnp.concatenate([rest, rest[:skip]], axis=0))
            if t == EARLY - 1:
                at = elems - GROUP
                edge_ref[EARLY, f, side_rows : side_rows + skip, :] = past[t + 1][f, at : at + skip, :]
        edge_ref[t + 1, f, rim_rows(g), :] = value

    def metric(k, g):
        if g < HALO or g > end - GROUP:
            return m_ref[k, rim_rows(g), :]
        return own_ref[fields + k, own_rows(g), :]

    def factor(g):
        if g + GROUP <= HALO:
            return in_low
        if g >= end:
            return in_high
        if g < HALO:
            return jnp.where(iota((GROUP, LANES), 0) < HALO - g, in_low, 1.0)
        if g + GROUP > end:
            return jnp.where(iota((GROUP, LANES), 0) >= end - g, in_high, 1.0)
        return None

    def own_load(t, f, g):
        if t < EARLY and g in (HALO, end - GROUP):
            rest, row = past[t][f, own_rows(g), :], iota((GROUP, LANES), 0)
            mended = edge_ref[t, f, rim_rows(g), :]
            return jnp.where(row < t, mended, rest) if g == HALO else jnp.where(row >= GROUP - t, mended, rest)
        return load(t, f, g)

    def sample(t):
        field = lambda f: jnp.concatenate([own_load(t + 1, f, g) for g in range(HALO, end, GROUP)], axis=0)
        columns = []
        for c in range(COMPS):
            x = field(c) if c < 3 else (field(3) + field(4) + field(5)) / 3.0
            columns.append(jnp.concatenate(split2(x), axis=0))
        lane = iota((slots, LANES), 1)
        send = jnp.concatenate([keep_ref[...], give_ref[...]], axis=0)
        rev = rev_ref[...]
        for c in range(0, COMPS, 2):
            found = dot(eh_ref[...], jnp.concatenate(columns[c : c + 2], axis=1))
            for i in range(2):
                value = jnp.sum(found[:, i * LANES : (i + 1) * LANES] * wp_ref[...], axis=1, keepdims=True)
                send = jnp.where(lane == (c + i) * STEPS + t, value, send)
                rev = jnp.where(lane == OBS_LANE + (c + i) * STEPS + (STEPS - 1) - t, value, rev)
        keep_ref[...] = send[:half]
        give_ref[...] = send[half:]
        rev_ref[...] = rev

    pairs = elems // PAIR_ROWS
    order = sorted(range(pairs), key=lambda j: abs(2 * j + 1 - pairs))
    inner, outer = order[:-2], order[-2:]
    ring_rows = lambda ring: (HALO - GROUP * (ring + 1), end + GROUP * ring)
    items, samples = [], {}
    fill = -(-len(inner) // EARLY)
    for t in range(EARLY):
        items += [Item(t, pairs, (low_rim[1], high_rim[0])), Item(t, pairs + 1, (low_rim[0], high_rim[1]))]
        items += [own_pair(EARLY, j) for j in inner[t * fill : (t + 1) * fill]]
        if t >= 1:
            samples[len(items) - 1] = t - 1
    for t in range(EARLY, STEPS):
        items += [own_pair(t, j) for j in (outer if t == EARLY else order)]
        if t > EARLY:
            samples[len(items) - len(order) + 2] = t - 1
        for ring in range(HALO // GROUP):
            if ring * GROUP < STEPS - t:
                items.append(Item(t, pairs + ring, ring_rows(ring), lift_only=ring * GROUP >= STEPS - 1 - t))
        if t == EARLY:
            samples[len(items) - 2] = EARLY - 1
    ready = {(0, g) for g in low_rim + high_rim}
    ready |= {(EARLY, g) for g in range(HALO + GROUP, end - GROUP, GROUP)}
    mended = {(EARLY, g) for g in low_groups + high_groups}, {(EARLY, g) for g in low_rim + high_rim}
    stepper = Stepper(
        fields, load, store, factor, metric, wt_ref, wl_ref, ck_ref, t_ref, h_ref, lt_ref, lu_ref
    )
    stepper.run(items, ready, lambda index: sample(samples[index]) if index in samples else None, mended)
    sample(STEPS - 1)


def march(own, near, far, past, ops, last_block):
    eh = ops[3]
    planes, elems, _ = own.shape
    fields = planes - AXES
    slots = eh.shape[0]
    vmem = pl.BlockSpec(memory_space=VMEM)
    return pl.pallas_call(
        functools.partial(march_kernel, last_block=last_block),
        in_specs=[vmem] * (3 + EARLY + len(ops)),
        out_shape=(
            jax.ShapeDtypeStruct((slots // 2, LANES), F32),
            jax.ShapeDtypeStruct((slots // 2, LANES), F32),
            jax.ShapeDtypeStruct((slots, LANES), F32),
        ),
        scratch_shapes=[
            VMEM((EARLY + 1, fields, 2 * (HALO + GROUP), LANES), F32),
            VMEM((2, fields, elems + 2 * HALO, LANES), F32),
            VMEM((AXES, 2 * (HALO + GROUP), LANES), F32),
        ]
        + scratch(fields, elems)
        + [VMEM((6 * LANES, 2 * LANES), BF16), VMEM((3 * LANES, 2 * LANES), BF16), VMEM((2 * LANES, 2 * LANES), BF16)],
        compiler_params=pltpu.CompilerParams(vmem_limit_bytes=40 << 20),
        cost_estimate=pl.CostEstimate(flops=20_000_000_000, bytes_accessed=4_000_000, transcendentals=0),
        name="march",
    )(own, near, far, *past, *ops)


def pack_kernel(keep_ref, given_ref, out_ref):
    chips = keep_ref.shape[0] // 2
    for other, ref in enumerate((keep_ref, given_ref)):
        for which in range(2):
            out_ref[pl.ds(2 * other + which, chips, stride=4), :] = ref[which * chips : (which + 1) * chips, :]


def pack(keep, given):
    return pl.pallas_call(
        pack_kernel,
        out_shape=jax.ShapeDtypeStruct((2 * keep.shape[0], LANES), F32),
        compiler_params=pltpu.CompilerParams(vmem_limit_bytes=4 << 20),
        name="pack",
    )(keep, given)


def finish_kernel(
    got_ref, rev_ref, to_slot_ref, to_pos_ref, seen_ref, res_hbm, mis_hbm, adj_hbm, res_ref, mis_ref, adj_ref, sems
):
    width, slots = seen_ref.shape
    chips = slots // 4
    got = jnp.concatenate([got_ref[pl.ds(i, chips, stride=4), :] for i in range(4)], axis=0)
    lane = iota(got.shape, 1)
    turned = jnp.where(lane < OBS_LANE, got, rev_ref[...] - got).T

    def place(rows, onehot):
        found = dot(jnp.concatenate(split2(rows), axis=0), onehot)
        return found[:width] + found[width:]

    residual = place(turned[:width], to_pos_ref[...]) - seen_ref[...]
    res_ref[...] = residual
    mis_ref[...] = 0.5 * jnp.sum(residual * residual, axis=0, keepdims=True)
    adj_ref[...] = place(turned[OBS_LANE : OBS_LANE + width], to_slot_ref[...])
    pairs = ((res_ref, res_hbm), (adj_ref, adj_hbm), (mis_ref, mis_hbm))
    copies = [pltpu.make_async_copy(here, out, sems.at[i]) for i, (here, out) in enumerate(pairs)]
    for copy in copies:
        copy.start()
    for copy in copies:
        copy.wait()


def finish(got, rev, to_slot, to_pos, seen):
    width, slots = seen.shape
    vmem = pl.BlockSpec(memory_space=VMEM)
    hbm = pl.BlockSpec(memory_space=pltpu.HBM)
    shapes = ((width, slots), (1, slots), (width, slots))
    return pl.pallas_call(
        finish_kernel,
        in_specs=[vmem] * 5,
        out_specs=(hbm, hbm, hbm),
        out_shape=tuple(jax.ShapeDtypeStruct(shape, F32) for shape in shapes),
        scratch_shapes=[VMEM(shape, F32) for shape in shapes] + [pltpu.SemaphoreType.DMA((3,))],
        compiler_params=pltpu.CompilerParams(vmem_limit_bytes=8 << 20),
        name="finish",
    )(got, rev, to_slot, to_pos, seen)


def shards(
    initial,
    derivative,
    coupling,
    face_lift,
    metric,
    rec_element,
    rec_weight,
    live_counts,
    shot_order,
    observed,
):
    blocks = lax.axis_size(MX)
    slots = rec_element.shape[0]
    order, element, lives = (x.reshape(-1, LANES) for x in (shot_order, rec_element, live_counts))
    staged = (derivative, rec_weight, order, element, lives, observed.T)
    own, near, far, derivative, rec_weight, order, element, lives, observed = turn(initial, metric, staged)
    pairs = [(i, min(i + 1, blocks - 1) if i % 2 else max(i - 1, 0)) for i in range(blocks)]
    far = lax.ppermute(far, MX, pairs)
    near = lax.ppermute(near, MX, [(i, i ^ 1) for i in range(blocks)])
    ops = operators(derivative, coupling, face_lift)
    outs = early(own, ops, (lives, element, rec_weight, order, observed))
    past, eh, wp, acc0, to_slot, to_pos, seen = (outs[:EARLY],) + tuple(outs[EARLY:])
    keep, give, rev = march(own, near, far, past, (*ops, eh, wp, acc0), blocks - 1)
    given = lax.ppermute(give, MX, [(i, i ^ 1) for i in range(blocks)])
    rows = pack(keep, given).reshape(blocks // 2, 4, LANES)
    got = lax.all_to_all(rows, MX[:2], split_axis=0, concat_axis=0, tiled=True)
    residual, misfit, adjoint = finish(got.reshape(slots, LANES), rev, to_slot, to_pos, seen)
    return (residual.T, misfit.reshape(slots), adjoint.T)


def solution(mesh):
    split = Mesh(
        mesh.devices.reshape(mesh.shape["shots"], 8, 8, 2), ("shots", "mx_0", "mx_1", "mx_2")
    )
    in_specs = (
        P("shots", None, MX),
        P(),
        P(),
        P(),
        P(None, MX),
        P(MX),
        P(None, MX),
        P(),
        P(),
        P(SHOTS_MX, None),
    )
    out_specs = (P(SHOTS_MX, None), P(SHOTS_MX), P(SHOTS_MX, None))
    return jax.shard_map(
        shards, mesh=split, in_specs=in_specs, out_specs=out_specs, check_vma=False
    )
```

```python
import functools

import jax
import jax.numpy as jnp
from jax import lax
from jax.experimental import pallas as pl
from jax.experimental.pallas import tpu as pltpu
from jax.sharding import Mesh
from jax.sharding import PartitionSpec as P


STEPS = 12
EARLY = 3
DT = 0.5 / STEPS
AXES = 3
COMPS = 4
MX = ("mx_0", "mx_1", "mx_2")
SHOTS_MX = ("shots", "mx_0", "mx_1", "mx_2")
F32 = jnp.float32
BF16 = jnp.bfloat16
I32 = jnp.int32
LANES = 128
GROUP = 8
PAIR_ROWS = 2 * GROUP
HALO = 16
WHOLE = 32
OBS_LANE = 64
VMEM = pltpu.VMEM


def iota(shape, dim):
    return lax.broadcasted_iota(I32, shape, dim)


def split2(x):
    hi = x.astype(BF16)
    return hi, (x - hi.astype(F32)).astype(BF16)


def dot(a, b):
    return jnp.dot(a, b, preferred_element_type=F32)


def block_index():
    index = 0
    for axis in MX:
        index = index * lax.axis_size(axis) + lax.axis_index(axis)
    return index


def whole(rows):
    return -(-rows // WHOLE) * WHOLE


def padded(x, rows, cols):
    if x.shape[1] < cols:
        x = jnp.concatenate([x, jnp.zeros((x.shape[0], cols - x.shape[1]), x.dtype)], axis=1)
    if x.shape[0] < rows:
        x = jnp.concatenate([x, jnp.zeros((rows - x.shape[0], cols), x.dtype)], axis=0)
    return x


def turn_kernel(*refs):
    staged = (len(refs) - 10) // 2
    initial_hbm, metric_hbm = refs[:2]
    from_refs = refs[2 : 2 + staged]
    own_ref, near_ref, far_ref = refs[2 + staged : 5 + staged]
    to_refs = refs[5 + staged : 5 + 2 * staged]
    initial_ref, metric_ref, low_ref, high_ref, sems = refs[-5:]
    fields, _, elems = initial_ref.shape
    pairs = [(metric_hbm, metric_ref), (initial_hbm, initial_ref)]
    pairs += [(x, y if x.shape == y.shape else y.at[: x.shape[0]]) for x, y in zip(from_refs, to_refs)]
    copies = [pltpu.make_async_copy(x, y, sems.at[i]) for i, (x, y) in enumerate(pairs)]
    for copy in copies:
        copy.start()
    copies[0].wait()
    for k in range(metric_ref.shape[0]):
        own_ref[fields + k] = jnp.broadcast_to(metric_ref[k : k + 1, :], (LANES, elems)).T
    copies[1].wait()
    for f in range(fields):
        own_ref[f] = padded(initial_ref[f], LANES, elems).T
    third = iota((elems, LANES), 1) // (LANES // 3)
    factors = jnp.where(third == 0, own_ref[fields], jnp.where(third == 1, own_ref[fields + 1], own_ref[fields + 2]))
    for edge_ref, rows in ((low_ref, slice(0, STEPS)), (high_ref, slice(elems - STEPS, elems))):
        for f in range(fields):
            edge_ref[f * STEPS : (f + 1) * STEPS, :] = own_ref[f, rows, :]
        edge_ref[fields * STEPS : (fields + 1) * STEPS, :] = factors[rows]
        edge_ref[(fields + 1) * STEPS :, :] = jnp.zeros((edge_ref.shape[0] - (fields + 1) * STEPS, LANES), F32)
    odd = block_index() % 2 == 1
    near_ref[...] = jnp.where(odd, low_ref[...], high_ref[...])
    far_ref[...] = jnp.where(odd, high_ref[...], low_ref[...])
    for copy in copies[2:]:
        copy.wait()


def turn(initial, metric, staged):
    fields, _, elems = initial.shape
    planes = fields + metric.shape[0]
    edge = jax.ShapeDtypeStruct((whole((fields + 1) * STEPS), LANES), F32)
    hbm = pl.BlockSpec(memory_space=pltpu.HBM)
    return pl.pallas_call(
        turn_kernel,
        in_specs=[hbm] * (2 + len(staged)),
        out_shape=(jax.ShapeDtypeStruct((planes, elems, LANES), F32), edge, edge)
        + tuple(jax.ShapeDtypeStruct((whole(x.shape[0]),) + x.shape[1:] if x.shape[0] < GROUP and x.ndim == 2 else x.shape, x.dtype) for x in staged),
        scratch_shapes=[
            VMEM(initial.shape, F32),
            VMEM(metric.shape, F32),
            VMEM(edge.shape, F32),
            VMEM(edge.shape, F32),
            pltpu.SemaphoreType.DMA((2 + len(staged),)),
        ],
        compiler_params=pltpu.CompilerParams(vmem_limit_bytes=8 << 20),
        name="turn",
    )(*(pltpu.with_memory_space_constraint(x, pltpu.HBM) for x in (initial, metric, *staged)))


def operators_kernel(derivative_ref, coupling_ref, lift_ref, wt_ref, wl_ref, ck_ref):
    fields = coupling_ref.shape[1]
    dh, dl = zip(*(split2(padded(DT * derivative_ref[k], LANES, LANES).T) for k in range(AXES)))
    zero = jnp.zeros((LANES, LANES), BF16)
    for row, (left, right) in enumerate(
        [(dh[0], dl[0]), (dh[1], dl[1]), (dh[2], dl[2]), (dh[2], zero), (dh[0], zero), (dh[1], zero)]
    ):
        wt_ref[row * LANES : (row + 1) * LANES, :] = jnp.concatenate([left, right], axis=1)
    l0h, l0l = split2(padded(DT * lift_ref[0], LANES, LANES).T)
    l1h, l1l = split2(padded(DT * lift_ref[1], LANES, LANES).T)
    for row, (left, right) in enumerate([(l0h, l1h), (l0h, l1h), (l0l, l1l)]):
        wl_ref[row * LANES : (row + 1) * LANES, :] = jnp.concatenate([left, right], axis=1)
    rows, cols = AXES * fields * GROUP, fields * GROUP
    spread_cols = (iota((fields, cols), 0) == iota((fields, cols), 1) // GROUP).astype(BF16)
    by_row = [coupling_ref[k, g : g + 1, :] for k in range(AXES) for g in range(fields)]
    by_row = jnp.concatenate([jnp.broadcast_to(x, (GROUP, fields)) for x in by_row], axis=0)
    hi, lo = split2(by_row)
    full = dot(hi, spread_cols) + dot(lo, spread_cols)
    full = jnp.where(iota((rows, cols), 0) % GROUP == iota((rows, cols), 1) % GROUP, full, 0.0)
    full_hi = full.astype(BF16).astype(F32)
    spread = padded(jnp.concatenate([full_hi, full_hi, full - full_hi], axis=1), *ck_ref.shape)
    ck_ref[...] = spread.astype(BF16)


def operators(derivative, coupling, face_lift):
    fields = coupling.shape[1]
    block = AXES * fields * GROUP
    return pl.pallas_call(
        operators_kernel,
        out_shape=(
            jax.ShapeDtypeStruct((6 * LANES, 2 * LANES), BF16),
            jax.ShapeDtypeStruct((3 * LANES, 2 * LANES), BF16),
            jax.ShapeDtypeStruct((whole(block), 2 * LANES), BF16),
        ),
        compiler_params=pltpu.CompilerParams(vmem_limit_bytes=8 << 20),
        cost_estimate=pl.CostEstimate(flops=1_000_000_000, bytes_accessed=1_000_000, transcendentals=0),
        name="operators",
    )(derivative, coupling, face_lift)


class Order:
    def __init__(self, me, ins, outs, local):
        self.me = me
        self.lives_ref, self.element_ref, self.weight_ref, self.order_ref, self.observed_ref = ins
        self.eh_ref, self.wp_ref, self.acc_ref, self.to_slot_ref, self.to_pos_ref, self.seen_ref = outs
        self.place_ref, self.weight_parts_ref, self.observed_parts_ref = local
        self.width, self.slots = self.observed_ref.shape
        self.chips = self.slots // 4
        self.big = float(self.slots * self.slots)
        self.bits = self.slots.bit_length() - 1
        assert self.slots == 1 << self.bits
        self.odd = me & 1

    def pieces(self):
        yield from (functools.partial(self.slot_rows, 0), self.weights, functools.partial(self.slot_rows, 1))
        yield from (self.observations, functools.partial(self.position_rows, 0), self.place_weights)
        yield from (functools.partial(self.position_rows, 1), self.seen, self.place_observations)

    def rows(self, other, which):
        start = (2 * other + which) * self.chips
        return slice(start, start + self.chips)

    def across(self, ref):
        return jnp.concatenate([ref[0:1, :], ref[1:2, :]], axis=1)

    def live_of(self, block):
        lives = self.lives_ref[:1, :]
        there = block == iota((block.shape[0], lives.shape[1]), 1)
        return jnp.sum(jnp.where(there, lives.astype(F32), 0.0), axis=1, keepdims=True)

    def slot_rows(self, other):
        slots, chips = self.slots, self.chips
        first, last = None, None
        for half in range(2):
            core = [self.order_ref[pl.ds(2 * core + half, chips, stride=4), :] for core in range(2)]
            order = jnp.where(self.odd == 1 - other, core[1], core[0])
            key = (((half * LANES + iota(order.shape, 1)) << self.bits) + (order & (slots - 1))).astype(F32)
            mine = (order >> self.bits) == self.me
            low, high = jnp.where(mine, key, self.big), jnp.where(mine, key, -1.0)
            first = low if first is None else jnp.minimum(first, low)
            last = high if last is None else jnp.maximum(last, high)
        found = jnp.min(first, axis=1, keepdims=True), jnp.max(last, axis=1, keepdims=True)
        live_slot = iota((1, slots), 1).astype(F32) < self.live_of(jnp.full((1, 1), self.me, I32))
        element = self.across(self.element_ref).astype(F32)
        done = 0.0
        for which in range(2):
            rows = self.rows(other, which)
            hot = (found[which].astype(I32) & (slots - 1)) == iota((chips, slots), 1)
            self.to_slot_ref[rows, :] = jnp.where(hot & live_slot, 1.0, 0.0).astype(BF16)
            element_of = jnp.sum(jnp.where(hot, element, 0.0), axis=1, keepdims=True)
            hit = (element_of.astype(I32) == iota((chips, LANES), 1)).astype(BF16)
            self.eh_ref[rows, :] = jnp.concatenate([hit, hit], axis=1)
            done = done + element_of[:GROUP]
        return jnp.broadcast_to(done, (GROUP, LANES))

    def position_rows(self, other):
        slots, shape = self.slots, (self.chips, self.slots)
        mine = self.order_ref[pl.ds(2 * self.me, 2), :]
        mine = jnp.concatenate([mine[0:1], mine[1:2]], axis=1)
        block = 2 * iota((self.chips, 1), 0) + jnp.where(self.odd == 1 - other, 1, 0)
        col = iota(shape, 1).astype(F32)
        here = (mine >> self.bits) == block
        found = (
            jnp.min(jnp.where(here, col, self.big), axis=1, keepdims=True),
            jnp.max(jnp.where(here, col, -1.0), axis=1, keepdims=True),
        )
        live = self.live_of(block)
        slot = (mine & (slots - 1)).astype(F32)
        done = 0.0
        for which in range(2):
            rows = self.rows(other, which)
            hot = found[which] == col
            self.place_ref[rows, :] = hot.astype(BF16)
            slot_of = jnp.sum(jnp.where(hot, slot, 0.0), axis=1, keepdims=True)
            self.to_pos_ref[rows, :] = jnp.where(hot & (slot_of < live), 1.0, 0.0).astype(BF16)
            done = done + slot_of[:GROUP]
        return jnp.broadcast_to(done, (GROUP, LANES))

    def weights(self):
        weight = padded(self.weight_ref[...], LANES, self.slots).T
        self.weight_parts_ref[...] = jnp.concatenate(split2(weight), axis=1)

    def place_weights(self):
        both = dot(self.to_slot_ref[...], self.weight_parts_ref[...])
        self.wp_ref[...] = both[:, :LANES] + both[:, LANES:]

    def observations(self):
        lane, time = iota((LANES, self.width), 0) - OBS_LANE, iota((LANES, self.width), 1)
        comp = time // STEPS
        turned = (lane == comp * STEPS + (STEPS - 1 - (time - comp * STEPS))).astype(BF16)
        parts = [dot(turned, part).astype(BF16) for part in split2(self.observed_ref[...])]
        self.observed_parts_ref[...] = jnp.concatenate(parts, axis=0)

    def place_observations(self):
        parts = self.observed_parts_ref[...]
        both = lax.dot_general(self.place_ref[...], parts, (((1,), (1,)), ((), ())), preferred_element_type=F32)
        self.acc_ref[...] = both[:, :LANES] + both[:, LANES:]

    def seen(self):
        live = jnp.sum(self.to_pos_ref[...].astype(F32), axis=0, keepdims=True)
        self.seen_ref[...] = self.observed_ref[...] * live


class Stepper:
    def __init__(self, fields, load, store, factor, metric, wt_ref, wl_ref, ck_ref, t_ref, h_ref, lt_ref, lu_ref):
        self.fields, self.load, self.store, self.factor, self.metric = fields, load, store, factor, metric
        self.wt_ref, self.wl_ref, self.ck_ref = wt_ref, wl_ref, ck_ref
        self.t_ref, self.h_ref, self.lt_ref, self.lu_ref = t_ref, h_ref, lt_ref, lu_ref

    def split(self, item):
        halves = ([], [])
        for f in range(self.fields):
            x = jnp.concatenate([self.load(item.t, f, g) for g in item.groups], axis=0)
            hi, lo = split2(x)
            rows = slice(f * PAIR_ROWS, (f + 1) * PAIR_ROWS)
            self.lu_ref[item.slot, rows, :LANES] = hi
            self.lu_ref[item.slot, rows, LANES:] = lo
            hi32 = hi.astype(F32)
            lo32 = x - hi32
            for side in range(2):
                part = slice(side * GROUP, (side + 1) * GROUP)
                halves[side].append((hi32[part], lo32[part]))
        return halves

    def couple(self, item):
        columns = []
        for side in self.split(item):
            his, los = [p[0] for p in side], [p[1] for p in side]
            columns.append(jnp.concatenate(his + los + his, axis=0).astype(BF16))
        if item.lift_only:
            return
        size = 3 * self.fields * GROUP
        v = dot(self.ck_ref[:size, :size], jnp.concatenate(columns, axis=1))
        for k in range(AXES):
            scale = [self.metric(k, g) for g in item.groups]
            if item.after is not None:
                scale = [x + 0.0 * item.after for x in scale]
            parts = []
            for f in range(self.fields):
                base = (k * self.fields + f) * GROUP
                for side in range(2):
                    parts.append(v[base : base + GROUP, side * LANES : (side + 1) * LANES] * scale[side])
            for lane, part in zip(((0, 4), (1, 5), (2, 3))[k], split2(jnp.concatenate(parts, axis=0))):
                self.lt_ref[item.slot, :, lane * LANES : (lane + 1) * LANES] = part

    def apply(self, item):
        lu = self.lu_ref.at[item.slot]
        if not item.lift_only:
            both = dot(self.lt_ref[item.slot], self.wt_ref[...])
        lifted = dot(lu[...], self.wl_ref[: 2 * LANES, :]) + dot(lu[:, :LANES], self.wl_ref[2 * LANES :, :])
        for f in range(self.fields):
            for side, g in enumerate(item.groups):
                rows = slice(f * PAIR_ROWS + side * GROUP, f * PAIR_ROWS + (side + 1) * GROUP)
                faces = [lifted[rows, face * LANES : (face + 1) * LANES] for face in range(2)]
                if not item.lift_only:
                    total = both[rows, :LANES] + both[rows, LANES:]
                    self.t_ref[f, g : g + GROUP, :] = total - (faces[0] + faces[1])
                for face in range(2):
                    at = g + GROUP
                    self.h_ref[face, f, at : at + GROUP, :] = faces[face]

    def update(self, t, g):
        before, after = slice(g + GROUP - 1, g + 2 * GROUP - 1), slice(g + GROUP + 1, g + 2 * GROUP + 1)
        for f in range(self.fields):
            lift = self.h_ref[0, f, before, :] + self.h_ref[1, f, after, :]
            change = self.t_ref[f, g : g + GROUP, :] + lift
            if self.factor(g) is not None:
                change = self.factor(g) * change
            self.store(t, f, g, self.load(t, f, g) + change)

    def run(self, items, ready, after, mended=(set(), set())):
        ready = set(ready)
        product, lifted, done = set(), set(), set()
        wanted = {}
        for item in items:
            for g in item.groups:
                wanted.setdefault(item.t, {})[g] = item
        coupled = 0

        def couple_next(limit):
            nonlocal coupled
            while coupled < limit and all((items[coupled].t, g) in ready for g in items[coupled].groups):
                self.couple(items[coupled])
                coupled += 1

        for index, item in enumerate(items):
            couple_next(min(index + 2, len(items)))
            assert coupled > index
            self.apply(item)
            for g in item.groups:
                lifted.add((item.t, g))
                if not item.lift_only:
                    product.add((item.t, g))
            for t, groups in wanted.items():
                for g in groups:
                    if (t, g) in done or (t, g) not in product:
                        continue
                    if all(n not in groups or (t, n) in lifted for n in (g - GROUP, g + GROUP)):
                        self.update(t, g)
                        done.add((t, g))
                        ready.add((t + 1, g))
            if mended[1] <= ready:
                ready |= mended[0]
            after(index)


class Item:
    after = None

    def __init__(self, t, slot, groups, lift_only=False):
        self.t, self.slot, self.groups, self.lift_only = t, slot, groups, lift_only


def own_pair(t, j):
    first = HALO + PAIR_ROWS * j
    return Item(t, j, (first, first + GROUP))


def hold(refs, local):
    for ref, to in zip(refs, local):
        rows, cols = ref.shape
        to[:rows, :cols] = ref[...]
    return local


def early_kernel(own_ref, wt_ref, wl_ref, ck_ref, *refs):
    ins, past, outs = refs[:5], refs[5 : 5 + EARLY], refs[5 + EARLY : 11 + EARLY]
    t_ref, h_ref, lt_ref, lu_ref, *local = refs[11 + EARLY :]
    planes, elems, _ = own_ref.shape
    fields = planes - AXES
    rows = lambda g: slice(g - HALO, g - HALO + GROUP)

    def load(t, f, g):
        return own_ref[f, rows(g), :] if t == 0 else past[t - 1][f, rows(g), :]

    def store(t, f, g, value):
        past[t][f, rows(g), :] = value

    pad = slice(HALO, HALO + GROUP), slice(elems + HALO + GROUP, elems + HALO + 2 * GROUP)
    for rim in pad:
        h_ref[:, :, rim, :] = jnp.zeros((2, fields, GROUP, LANES), F32)
    stepper = Stepper(
        fields, load, store, lambda g: None, lambda k, g: own_ref[fields + k, rows(g), :],
        wt_ref, wl_ref, ck_ref, t_ref, h_ref, lt_ref, lu_ref,
    )
    pairs = elems // PAIR_ROWS
    order = sorted(range(pairs), key=lambda j: abs(2 * j + 1 - pairs))
    items = [own_pair(t, j) for t in range(EARLY) for j in order]
    pieces = list(Order(block_index(), ins, outs, local).pieces())
    at = {(len(items) - 4) * i // len(pieces): piece for i, piece in enumerate(pieces)}

    def beside(index):
        if index in at:
            items[index + 4].after = at[index]()

    stepper.run(items, {(0, g) for item in items for g in item.groups}, beside)


def scratch(fields, elems):
    rows = elems + 2 * HALO
    tile = fields * PAIR_ROWS
    slots = rows // PAIR_ROWS + 2
    return [
        VMEM((fields, rows, LANES), F32),
        VMEM((2, fields, rows + 2 * GROUP, LANES), F32),
        VMEM((slots, tile, 6 * LANES), BF16),
        VMEM((slots, tile, 2 * LANES), BF16),
    ]


def early(own, operators, ins):
    planes, elems, _ = own.shape
    fields = planes - AXES
    width, slots = ins[-1].shape
    vmem = pl.BlockSpec(memory_space=VMEM)
    return pl.pallas_call(
        early_kernel,
        in_specs=[vmem] * (1 + len(operators) + len(ins)),
        out_shape=tuple(jax.ShapeDtypeStruct((fields, elems, LANES), F32) for _ in range(EARLY))
        + (
            jax.ShapeDtypeStruct((slots, 2 * LANES), BF16),
            jax.ShapeDtypeStruct((slots, LANES), F32),
            jax.ShapeDtypeStruct((slots, LANES), F32),
            jax.ShapeDtypeStruct((slots, slots), BF16),
            jax.ShapeDtypeStruct((slots, slots), BF16),
            jax.ShapeDtypeStruct((width, slots), F32),
        ),
        scratch_shapes=scratch(fields, elems) + [VMEM((slots, slots), BF16)] * 3,
        compiler_params=pltpu.CompilerParams(vmem_limit_bytes=32 << 20),
        cost_estimate=pl.CostEstimate(flops=5_000_000_000, bytes_accessed=4_000_000, transcendentals=0),
        name="early",
    )(own, *operators, *ins)


def march_kernel(own_ref, near_ref, far_ref, *refs, last_block):
    past = (own_ref,) + refs[:EARLY]
    wt_ref, wl_ref, ck_ref, eh_ref, wp_ref, acc0_ref, keep_ref, give_ref, rev_ref = refs[EARLY : EARLY + 9]
    edge_ref, u_ref, m_ref, t_ref, h_ref, lt_ref, lu_ref, *local = refs[EARLY + 9 :]
    wt_ref, wl_ref, ck_ref = hold((wt_ref, wl_ref, ck_ref), local)
    planes, elems, _ = own_ref.shape
    fields = planes - AXES
    slots = eh_ref.shape[0]
    end = HALO + elems
    me = block_index()
    in_low = jnp.where(me == 0, 0.0, 1.0).astype(F32)
    in_high = jnp.where(me == last_block, 0.0, 1.0).astype(F32)
    skip = HALO - STEPS
    side_rows = HALO + GROUP
    low_rim, high_rim = [skip, skip + GROUP], [end - skip, end - skip + GROUP]
    low_groups, high_groups = list(range(0, side_rows, GROUP)), list(range(end - GROUP, end + HALO, GROUP))
    own_rows = lambda g: slice(g - HALO, g - HALO + GROUP)

    def rim_rows(g):
        at = g if g < HALO + GROUP else side_rows + g - (end - GROUP)
        return slice(at, at + GROUP)

    odd = me % 2 == 1
    low_edge = lambda edge: jnp.where(odd, near_ref[edge], far_ref[edge])
    high_edge = lambda edge: jnp.where(odd, far_ref[edge], near_ref[edge])
    spare = jnp.zeros((skip, LANES), F32)
    for f in range(fields):
        edge = slice(f * STEPS, (f + 1) * STEPS)
        low = jnp.where(me > 0, low_edge(edge), 0.0)
        high = jnp.where(me < last_block, high_edge(edge), 0.0)
        edge_ref[0, f, :side_rows, :] = jnp.concatenate([spare, low, own_ref[f, :GROUP, :]], axis=0)
        edge_ref[0, f, side_rows:, :] = jnp.concatenate([own_ref[f, elems - GROUP :, :], high, spare], axis=0)
    edge_ref[EARLY] = jnp.zeros(edge_ref.shape[1:], F32)
    edge = slice(fields * STEPS, (fields + 1) * STEPS)
    low_factors, high_factors = low_edge(edge), high_edge(edge)
    for k in range(AXES):
        lane = k * (LANES // AXES)
        spread = lambda x: jnp.broadcast_to(x[:, lane : lane + 1], (STEPS, LANES))
        own_low, own_high = own_ref[fields + k, :GROUP, :], own_ref[fields + k, elems - GROUP :, :]
        m_ref[k, :side_rows, :] = jnp.concatenate([spare, spread(low_factors), own_low], axis=0)
        m_ref[k, side_rows:, :] = jnp.concatenate([own_high, spread(high_factors), spare], axis=0)
    h_ref[:, :, :PAIR_ROWS, :] = jnp.zeros((2, fields, PAIR_ROWS, LANES), F32)
    h_ref[:, :, end + GROUP + HALO - GROUP :, :] = jnp.zeros((2, fields, PAIR_ROWS, LANES), F32)
    half = slots // 2
    keep_ref[...] = acc0_ref[:half]
    give_ref[...] = acc0_ref[half:]
    rev_ref[...] = jnp.zeros(rev_ref.shape, F32)

    def load(t, f, g):
        if t > EARLY:
            return u_ref[t % 2, f, g : g + GROUP, :]
        if t == EARLY and g in low_groups + high_groups or g in low_rim + high_rim:
            return edge_ref[t, f, rim_rows(g), :]
        return past[t][f, own_rows(g), :]

    def store(t, f, g, value):
        if t >= EARLY:
            u_ref[(t + 1) % 2, f, g : g + GROUP, :] = value
            return
        row = iota((GROUP, LANES), 0)
        if g == low_rim[1]:
            rest = past[t + 1][f, : GROUP - skip, :]
            value = jnp.where(row <= skip + t, value, jnp.concatenate([rest[:skip], rest], axis=0))
            if t == EARLY - 1:
                edge_ref[EARLY, f, side_rows - skip : side_rows, :] = past[t + 1][f, GROUP - skip : GROUP, :]
        if g == high_rim[0]:
            rest = past[t + 1][f, elems - (GROUP - skip) :, :]
            value = jnp.where(row >= GROUP - skip - 1 - t, value, jnp.concatenate([rest, rest[:skip]], axis=0))
            if t == EARLY - 1:
                at = elems - GROUP
                edge_ref[EARLY, f, side_rows : side_rows + skip, :] = past[t + 1][f, at : at + skip, :]
        edge_ref[t + 1, f, rim_rows(g), :] = value

    def metric(k, g):
        if g < HALO or g > end - GROUP:
            return m_ref[k, rim_rows(g), :]
        return own_ref[fields + k, own_rows(g), :]

    def factor(g):
        if g + GROUP <= HALO:
            return in_low
        if g >= end:
            return in_high
        if g < HALO:
            return jnp.where(iota((GROUP, LANES), 0) < HALO - g, in_low, 1.0)
        if g + GROUP > end:
            return jnp.where(iota((GROUP, LANES), 0) >= end - g, in_high, 1.0)
        return None

    def own_load(t, f, g):
        if t < EARLY and g in (HALO, end - GROUP):
            rest, row = past[t][f, own_rows(g), :], iota((GROUP, LANES), 0)
            mended = edge_ref[t, f, rim_rows(g), :]
            return jnp.where(row < t, mended, rest) if g == HALO else jnp.where(row >= GROUP - t, mended, rest)
        return load(t, f, g)

    def sample(t):
        field = lambda f: jnp.concatenate([own_load(t + 1, f, g) for g in range(HALO, end, GROUP)], axis=0)
        columns = []
        for c in range(COMPS):
            x = field(c) if c < 3 else (field(3) + field(4) + field(5)) / 3.0
            columns.append(jnp.concatenate(split2(x), axis=0))
        lane = iota((slots, LANES), 1)
        send = jnp.concatenate([keep_ref[...], give_ref[...]], axis=0)
        rev = rev_ref[...]
        for c in range(0, COMPS, 2):
            found = dot(eh_ref[...], jnp.concatenate(columns[c : c + 2], axis=1))
            for i in range(2):
                value = jnp.sum(found[:, i * LANES : (i + 1) * LANES] * wp_ref[...], axis=1, keepdims=True)
                send = jnp.where(lane == (c + i) * STEPS + t, value, send)
                rev = jnp.where(lane == OBS_LANE + (c + i) * STEPS + (STEPS - 1) - t, value, rev)
        keep_ref[...] = send[:half]
        give_ref[...] = send[half:]
        rev_ref[...] = rev

    pairs = elems // PAIR_ROWS
    order = sorted(range(pairs), key=lambda j: abs(2 * j + 1 - pairs))
    inner, outer = order[:-2], order[-2:]
    ring_rows = lambda ring: (HALO - GROUP * (ring + 1), end + GROUP * ring)
    items, samples = [], {}
    fill = -(-len(inner) // EARLY)
    for t in range(EARLY):
        items += [Item(t, pairs, (low_rim[1], high_rim[0])), Item(t, pairs + 1, (low_rim[0], high_rim[1]))]
        items += [own_pair(EARLY, j) for j in inner[t * fill : (t + 1) * fill]]
        if t >= 1:
            samples[len(items) - 1] = t - 1
    for t in range(EARLY, STEPS):
        items += [own_pair(t, j) for j in (outer if t == EARLY else order)]
        if t > EARLY:
            samples[len(items) - len(order) + 2] = t - 1
        for ring in range(HALO // GROUP):
            if ring * GROUP < STEPS - t:
                items.append(Item(t, pairs + ring, ring_rows(ring), lift_only=ring * GROUP >= STEPS - 1 - t))
        if t == EARLY:
            samples[len(items) - 3] = EARLY - 1
    ready = {(0, g) for g in low_rim + high_rim}
    ready |= {(EARLY, g) for g in range(HALO + GROUP, end - GROUP, GROUP)}
    mended = {(EARLY, g) for g in low_groups + high_groups}, {(EARLY, g) for g in low_rim + high_rim}
    stepper = Stepper(
        fields, load, store, factor, metric, wt_ref, wl_ref, ck_ref, t_ref, h_ref, lt_ref, lu_ref
    )
    stepper.run(items, ready, lambda index: sample(samples[index]) if index in samples else None, mended)
    sample(STEPS - 1)


def march(own, near, far, past, ops, last_block):
    eh = ops[3]
    planes, elems, _ = own.shape
    fields = planes - AXES
    slots = eh.shape[0]
    vmem = pl.BlockSpec(memory_space=VMEM)
    return pl.pallas_call(
        functools.partial(march_kernel, last_block=last_block),
        in_specs=[vmem] * (3 + EARLY + len(ops)),
        out_shape=(
            jax.ShapeDtypeStruct((slots // 2, LANES), F32),
            jax.ShapeDtypeStruct((slots // 2, LANES), F32),
            jax.ShapeDtypeStruct((slots, LANES), F32),
        ),
        scratch_shapes=[
            VMEM((EARLY + 1, fields, 2 * (HALO + GROUP), LANES), F32),
            VMEM((2, fields, elems + 2 * HALO, LANES), F32),
            VMEM((AXES, 2 * (HALO + GROUP), LANES), F32),
        ]
        + scratch(fields, elems)
        + [VMEM((6 * LANES, 2 * LANES), BF16), VMEM((3 * LANES, 2 * LANES), BF16), VMEM((2 * LANES, 2 * LANES), BF16)],
        compiler_params=pltpu.CompilerParams(vmem_limit_bytes=40 << 20),
        cost_estimate=pl.CostEstimate(flops=20_000_000_000, bytes_accessed=4_000_000, transcendentals=0),
        name="march",
    )(own, near, far, *past, *ops)


def pack_kernel(keep_ref, given_ref, out_ref):
    chips = keep_ref.shape[0] // 2
    for other, ref in enumerate((keep_ref, given_ref)):
        for which in range(2):
            out_ref[pl.ds(2 * other + which, chips, stride=4), :] = ref[which * chips : (which + 1) * chips, :]


def pack(keep, given):
    return pl.pallas_call(
        pack_kernel,
        out_shape=jax.ShapeDtypeStruct((2 * keep.shape[0], LANES), F32),
        compiler_params=pltpu.CompilerParams(vmem_limit_bytes=4 << 20),
        name="pack",
    )(keep, given)


def finish_kernel(
    got_ref, rev_ref, to_slot_ref, to_pos_ref, seen_ref, res_hbm, mis_hbm, adj_hbm, res_ref, mis_ref, adj_ref, sems
):
    width, slots = seen_ref.shape
    chips = slots // 4
    got = jnp.concatenate([got_ref[pl.ds(i, chips, stride=4), :] for i in range(4)], axis=0)
    lane = iota(got.shape, 1)
    turned = jnp.where(lane < OBS_LANE, got, rev_ref[...] - got).T

    def place(rows, onehot):
        found = dot(jnp.concatenate(split2(rows), axis=0), onehot)
        return found[:width] + found[width:]

    residual = place(turned[:width], to_pos_ref[...]) - seen_ref[...]
    res_ref[...] = residual
    mis_ref[...] = 0.5 * jnp.sum(residual * residual, axis=0, keepdims=True)
    adj_ref[...] = place(turned[OBS_LANE : OBS_LANE + width], to_slot_ref[...])
    pairs = ((res_ref, res_hbm), (adj_ref, adj_hbm), (mis_ref, mis_hbm))
    copies = [pltpu.make_async_copy(here, out, sems.at[i]) for i, (here, out) in enumerate(pairs)]
    for copy in copies:
        copy.start()
    for copy in copies:
        copy.wait()


def finish(got, rev, to_slot, to_pos, seen):
    width, slots = seen.shape
    vmem = pl.BlockSpec(memory_space=VMEM)
    hbm = pl.BlockSpec(memory_space=pltpu.HBM)
    shapes = ((width, slots), (1, slots), (width, slots))
    return pl.pallas_call(
        finish_kernel,
        in_specs=[vmem] * 5,
        out_specs=(hbm, hbm, hbm),
        out_shape=tuple(jax.ShapeDtypeStruct(shape, F32) for shape in shapes),
        scratch_shapes=[VMEM(shape, F32) for shape in shapes] + [pltpu.SemaphoreType.DMA((3,))],
        compiler_params=pltpu.CompilerParams(vmem_limit_bytes=8 << 20),
        name="finish",
    )(got, rev, to_slot, to_pos, seen)


def shards(
    initial,
    derivative,
    coupling,
    face_lift,
    metric,
    rec_element,
    rec_weight,
    live_counts,
    shot_order,
    observed,
):
    blocks = lax.axis_size(MX)
    slots = rec_element.shape[0]
    order, element, lives = (x.reshape(-1, LANES) for x in (shot_order, rec_element, live_counts))
    staged = (derivative, rec_weight, order, element, lives, observed.T)
    own, near, far, derivative, rec_weight, order, element, lives, observed = turn(initial, metric, staged)
    pairs = [(i, min(i + 1, blocks - 1) if i % 2 else max(i - 1, 0)) for i in range(blocks)]
    far = lax.ppermute(far, MX, pairs)
    near = lax.ppermute(near, MX, [(i, i ^ 1) for i in range(blocks)])
    ops = operators(derivative, coupling, face_lift)
    outs = early(own, ops, (lives, element, rec_weight, order, observed))
    past, eh, wp, acc0, to_slot, to_pos, seen = (outs[:EARLY],) + tuple(outs[EARLY:])
    keep, give, rev = march(own, near, far, past, (*ops, eh, wp, acc0), blocks - 1)
    given = lax.ppermute(give, MX, [(i, i ^ 1) for i in range(blocks)])
    rows = pack(keep, given).reshape(blocks // 2, 4, LANES)
    got = lax.all_to_all(rows, MX[:2], split_axis=0, concat_axis=0, tiled=True)
    residual, misfit, adjoint = finish(got.reshape(slots, LANES), rev, to_slot, to_pos, seen)
    return (residual.T, misfit.reshape(slots), adjoint.T)


def solution(mesh):
    split = Mesh(
        mesh.devices.reshape(mesh.shape["shots"], 8, 8, 2), ("shots", "mx_0", "mx_1", "mx_2")
    )
    in_specs = (
        P("shots", None, MX),
        P(),
        P(),
        P(),
        P(None, MX),
        P(MX),
        P(None, MX),
        P(),
        P(),
        P(SHOTS_MX, None),
    )
    out_specs = (P(SHOTS_MX, None), P(SHOTS_MX), P(SHOTS_MX, None))
    return jax.shard_map(
        shards, mesh=split, in_specs=in_specs, out_specs=out_specs, check_vma=False
    )
```
